128 devices in a mesh: bx: 4 (over z_hi, core), by: 8 (over z_lo, x), bz: 4 (over y).
Axes of the slice: x: 4, y: 4, z: 4 (z_hi: 2, z_lo: 2; z = z_hi * 2 + z_lo), core: 2. Of those that a mesh axis runs over, the one named last changes fastest.
Arguments:
- estimate: float32 [64, 128, 512], P('bx', 'by', 'bz'), may hold values from 0.2 to 5
- observed: float32 [8, 64, 128, 512], P(None, 'bx', 'by', 'bz'), may hold values from 0.3 to 180, as said below
- coverage: int32 [8, 4, 8, 4], P(None, 'bx', 'by', 'bz'), may hold values from 0 to 1, as said below
- psf_taps: float32 [8, 3, 17], replicated, may hold values from 0.05 to 1
Outputs:
- refined: float32 [64, 128, 512], P('bx', 'by', 'bz')
The draws below stay inside these ranges and needn't reach their ends.
Inputs may be any that keep to these rules, and one draw needn't show every extreme that they name: `coverage`: each block is covered by 2 to 8 views; in every draw some block is covered by all 8. `observed`: positive.
All inputs are finite; a program needn't handle non-finite values.
Results may differ from the reference program's by a relative error of at most 0.0001.
Values sent between devices are 32-bit elements; how exact they have to be, the bound alone decides.
A program may use at most 64 MiB of HBM per device.

```python
import math
import jax
import jax.numpy as jnp
from jax import lax

V = 8
R = 8
CX = 16
CY = 16
CZ = 128
NX = 64
NY = 128
NZ = 512
N_BX = 4
N_BY = 8
N_BZ = 4


def draw_observed(key, part):
    first, second = jax.random.split(key, 2)
    blocks_x = NX // CX
    blocks_y = NY // CY
    blocks_z = NZ // CZ
    coarse = jnp.exp(jax.random.uniform(first, (blocks_x, blocks_y, blocks_z), jnp.float32, 0.0, jnp.log(10.0)))
    ramp = 1.0 + 2.0 * jnp.arange(blocks_y, dtype=jnp.float32) / max(blocks_y - 1, 1)
    coarse = coarse * ramp[None, :, None]
    grown = jnp.repeat(jnp.repeat(jnp.repeat(coarse, CX, axis=0), CY, axis=1), CZ, axis=2)
    voxel = jnp.exp(jax.random.uniform(second, (V, NX, NY, NZ), jnp.float32, jnp.log(0.3), jnp.log(3.0)))
    values = voxel * grown[None]
    return values.astype(jnp.float32)


def draw_coverage(key, part):
    blocks = NX // CX * (NY // CY) * (NZ // CZ)
    first, second, third = jax.random.split(jax.random.fold_in(key, 7), 3)
    counts = jax.random.randint(first, (blocks,), 2, V + 1)
    fullest = jax.random.randint(second, (), 0, blocks)
    counts = counts.at[fullest].set(V)
    ranks = jax.vmap(lambda each: jax.random.permutation(each, V))(jax.random.split(third, blocks))
    covered = (ranks < counts[:, None]).astype(jnp.int32)
    return covered.T.reshape(V, NX // CX, NY // CY, NZ // CZ)


def levels(key, dims, cuts, least, high):
    def one(position, shards_of):
        steps = jax.random.uniform(jax.random.fold_in(jax.random.fold_in(key, 6), position), (shards_of,), jnp.float32, least / len(cuts), high / len(cuts))
        return jnp.repeat(jnp.exp(steps), dims[position] // shards_of).reshape((-1,) + (1,) * (len(dims) - position - 1))

    factor_of = one(*cuts[0])
    for cut in cuts[1:]:
        factor_of = factor_of * one(*cut)
    return factor_of


def setup_inputs(seed: int = 0) -> dict:
    key_list = jax.random.split(jax.random.key(seed), 5)
    return {
        "estimate": jnp.clip(jnp.exp(math.log(5.0) - 3.218876 * jax.random.uniform(key_list[0], (NX, NY, NZ), jnp.float32) ** levels(key_list[0], (NX, NY, NZ), ((0, 4), (1, 8), (2, 4)), -0.2, 0.2)), 0.2, 5.0),
        "observed": draw_observed(jax.random.fold_in(key_list[4], 71), 0),
        "coverage": draw_coverage(jax.random.fold_in(key_list[4], 71), 0),
        "psf_taps": jnp.clip(jnp.exp(jax.random.uniform(key_list[3], (V, 3, 2 * R + 1), jnp.float32, math.log(0.05), math.log(1.0))), 0.05, 1.0),
    }


def blur_axis(field, taps_row, axis):
    moved = jnp.moveaxis(field, axis, -1)
    shape = moved.shape
    flat = moved.reshape(-1, 1, shape[-1])
    kernel = taps_row.reshape(1, 1, -1)
    width = (taps_row.shape[0] - 1) // 2
    result = lax.conv_general_dilated(flat, kernel, (1,), [(width, width)], precision=lax.Precision.HIGHEST)
    return jnp.moveaxis(result.reshape(shape), -1, axis)


def blur_volume(field, kernels):
    result = field
    for axis in range(3):
        result = blur_axis(result, kernels[axis], axis)
    return result


def spread(block_values):
    grown = jnp.broadcast_to(block_values[:, None, :, None, :, None], (N_BX, CX, N_BY, CY, N_BZ, CZ))
    return grown.reshape(NX, NY, NZ)


def reference(estimate, observed, coverage, psf_taps):
    taps = psf_taps / jnp.sum(psf_taps, axis=2, keepdims=True)
    weights = coverage.astype(jnp.float32)
    count = spread(jnp.sum(weights, axis=0))
    summed = jnp.zeros((NX, NY, NZ), jnp.float32)
    target_field = jnp.zeros((NX, NY, NZ), jnp.float32)
    for view in range(V):
        blurred = blur_volume(estimate, taps[view])
        ratio = observed[view] / blurred
        back = blur_volume(ratio, taps[view][:, ::-1])
        weight_full = spread(weights[view])
        summed = summed + weight_full * back
        target_field = target_field + weight_full * observed[view]
    updated = estimate * (summed / count)
    target = jnp.sum(target_field / count)
    total = jnp.sum(updated)
    return updated * (target / total)
```

```python
import functools

import jax
import jax.numpy as jnp
from jax import lax
from jax.experimental import pallas as pl
from jax.experimental.pallas import tpu as pltpu
from jax.sharding import PartitionSpec as P

MESH = pl.DeviceIdType.MESH
F32 = jnp.float32
BF16 = jnp.bfloat16
V, R, T = 8, 8, 17
CX, CY, CZ = 16, 16, 128
EX, EY = CX + 2 * R, CY + 2 * R
LINES = (("bz", 4), ("by", 8), ("bx", 4))


def split(f):
    hi = f.astype(BF16)
    lo = (f - hi.astype(F32)).astype(BF16)
    return hi, lo


def dot(a, b):
    return jnp.dot(a, b, preferred_element_type=F32)


def stack4(f):
    hi, lo = split(f)
    return jnp.concatenate([hi, lo, hi, lo], axis=0)


def flip_tiles(f):
    return jnp.concatenate([f[:128].T, f[128:].T], axis=1)


def kernel(
    est, obs, cov, taps_s, taps_v, out,
    e_buf, o_buf, y_buf, g_buf, r_buf, x_buf, p_buf, rx_buf, ry_buf,
    sf_buf, hf_buf, sb_buf, hb_buf, w_buf, t_buf,
    zf_mat, zb_mat, yf_mat, yb_mat, red_own, red_in,
    load_sem, y_send, y_recv, x_send, x_recv, w_send, w_recv,
    zf_send, zf_recv, zb_send, zb_recv, rx_send, rx_recv, ry_send, ry_recv,
    red_send, red_recv,
):
    ids = {name: lax.axis_index(name) for name, _ in LINES}
    sizes = dict(LINES)

    barrier = pltpu.get_barrier_semaphore()
    for name, n in LINES:
        for d in range(1, n):
            pl.semaphore_signal(
                barrier, inc=1, device_id={name: lax.rem(ids[name] + d, n)}, device_id_type=MESH
            )
    load_e = pltpu.make_async_copy(est, e_buf.at[pl.ds(R, CX), pl.ds(R, CY)], load_sem.at[0])
    load_o = pltpu.make_async_copy(obs, o_buf, load_sem.at[1])
    load_e.start()
    load_o.start()

    def has(name, side):
        return ids[name] > 0 if side == 0 else ids[name] < sizes[name] - 1

    def peer(name, side):
        return {name: ids[name] - 1 if side == 0 else ids[name] + 1}

    def remote(src, dst, send, recv, name, side):
        return pltpu.make_async_remote_copy(
            src_ref=src, dst_ref=dst, send_sem=send, recv_sem=recv,
            device_id=peer(name, side), device_id_type=MESH,
        )

    edge = (pl.ds(0, R), pl.ds(EX - R, R))
    inner = (pl.ds(R, R), pl.ds(CX, R))

    def y_copy(side):
        return remote(
            e_buf.at[pl.ds(R, CX), inner[side]], e_buf.at[pl.ds(R, CX), edge[1 - side]],
            y_send.at[side], y_recv.at[1 - side], "by", side,
        )

    def yw_copy(side):
        return remote(
            w_buf.at[1, 1], w_buf.at[1, 2 - 2 * side],
            w_send.at[0, side], w_recv.at[0, 1 - side], "by", side,
        )

    def x_copy(side):
        return remote(
            e_buf.at[inner[side]], e_buf.at[edge[1 - side]],
            x_send.at[side], x_recv.at[1 - side], "bx", side,
        )

    def xw_copy(side):
        return remote(
            w_buf.at[1], w_buf.at[2 - 2 * side],
            w_send.at[1, side], w_recv.at[1, 1 - side], "bx", side,
        )

    def zf_copy(v, side):
        return remote(
            sf_buf.at[v, pl.ds(R - R * side, R)], hf_buf.at[v, pl.ds(R * side, R)],
            zf_send.at[v, side], zf_recv.at[v, 1 - side], "bz", side,
        )

    def zb_copy(v, side):
        return remote(
            sb_buf.at[v, pl.ds(R - R * side, R)], hb_buf.at[v, pl.ds(R * side, R)],
            zb_send.at[v, side], zb_recv.at[v, 1 - side], "bz", side,
        )

    def rx_copy(side):
        return remote(
            p_buf.at[edge[side]], rx_buf.at[1 - side],
            rx_send.at[side], rx_recv.at[1 - side], "bx", side,
        )

    def ry_copy(side):
        return remote(
            p_buf.at[pl.ds(R, CX), edge[side]], ry_buf.at[1 - side],
            ry_send.at[side], ry_recv.at[1 - side], "by", side,
        )

    def start(copies, name):
        for side in (0, 1):
            @pl.when(has(name, side))
            def _():
                for c in copies:
                    c(side).start()

    def finish(copies, name):
        for side in (0, 1):
            @pl.when(has(name, side))
            def _():
                for c in copies:
                    c(side).wait_send()
                    c(1 - side).wait_recv()

    for side in (0, 1):
        @pl.when(jnp.logical_not(has("by", side)))
        def _():
            e_buf[R:R + CX, edge[side], :] = jnp.zeros((CX, R, CZ), F32)
            w_buf[1, 2 * side] = jnp.zeros((V, CZ), F32)
            ry_buf[side] = jnp.zeros((CX, R, CZ), F32)

        @pl.when(jnp.logical_not(has("bx", side)))
        def _():
            e_buf[edge[side]] = jnp.zeros((R, EY, CZ), F32)
            w_buf[2 * side] = jnp.zeros((3, V, CZ), F32)
            rx_buf[side] = jnp.zeros((R, EY, CZ), F32)

        @pl.when(jnp.logical_not(has("bz", side)))
        def _():
            rows = pl.ds(R - R * side, R)
            hf_buf[:, rows, :] = jnp.zeros((V, R, CX * CY), F32)
            hb_buf[:, rows, :] = jnp.zeros((V, R, CX * CY), F32)

    row8 = lax.broadcasted_iota(jnp.int32, (V, CZ), 0)
    weight = jnp.zeros((V, CZ), F32)
    for v in range(V):
        weight = weight + jnp.where(row8 == v, cov[v, 0, 0, 0].astype(F32), 0.0)
    w_buf[1, 1] = weight

    load_e.wait()
    pl.semaphore_wait(barrier, sum(n - 1 for _, n in LINES))
    start((y_copy, yw_copy), "by")

    t_buf[...] = jnp.zeros_like(t_buf)
    t_buf[:, 0:3, 0:T] = taps_v[...]

    lane = lax.broadcasted_iota(jnp.int32, (128, 128), 1)
    row = lax.broadcasted_iota(jnp.int32, (128, 128), 0)
    near = jnp.abs(row - lane) <= R
    band = lax.broadcasted_iota(jnp.int32, (CY, 128), 1)
    zf_mat[...] = jnp.zeros_like(zf_mat)
    zb_mat[...] = jnp.zeros_like(zb_mat)

    def build(v, carry):
        sums = jnp.sum(t_buf[v], axis=1, keepdims=True)
        ty = t_buf[v, 1:2, :] / sums[1:2]
        tz = t_buf[v, 2:3, :] / (sums[2:3] * sums[0:1])
        ty = ty + pltpu.roll(ty, 32, 1)
        ty = ty + pltpu.roll(ty, 64, 1)
        q = pltpu.roll(jnp.broadcast_to(ty, (CY, 128)), 0, 1, stride=1, stride_axis=0)
        q_hi, q_lo = split(q)
        zero = jnp.zeros_like(q_hi)
        for x in range(2):
            mine = (band // 32) % 2 == x
            yf_mat[v, x * CY:(x + 1) * CY, 0:128] = jnp.where(mine, q_hi, zero)
            yf_mat[v, x * CY:(x + 1) * CY, 128:256] = jnp.where(mine, q_lo, zero)
        q4 = jnp.concatenate(
            [jnp.where(band // 32 == x % 4, q, 0.0) for x in range(8)], axis=0
        ).T
        b_hi, b_lo = split(q4)
        yb_mat[v, :, 0:128] = b_hi
        yb_mat[v, :, 128:256] = b_lo

        ring = pltpu.roll(jnp.broadcast_to(tz, (128, 128)), 128 - R, 1, stride=1, stride_axis=0)
        for mat, full in ((zb_mat, ring), (zf_mat, ring.T)):
            m_hi, m_lo = split(jnp.where(near, full, 0.0))
            mat[v, 0:128, 0:128] = m_hi
            mat[v, 0:128, 128:256] = m_lo
            far = jnp.where(near, 0.0, full)
            far = jnp.concatenate([far[0:R], far[128 - R:128]], axis=0)
            f_hi, f_lo = split(far)
            rows = pl.ds(pl.multiple_of(128 + 2 * R * v, 2 * R), 2 * R)
            mat[v, rows, 0:128] = f_hi
            mat[v, rows, 128:256] = f_lo
        return carry

    lax.fori_loop(0, V, build, 0)

    finish((y_copy, yw_copy), "by")
    start((x_copy, xw_copy), "bx")

    def forward_y(x0):
        data = jnp.concatenate(
            [stack4(e_buf[pl.ds(x0 + 2 * h, 2)].reshape(2 * EY, CZ)) for h in range(2)], axis=1
        )
        full = dot(yf_mat[...].reshape(V * 2 * CY, 256), data)
        for h in range(2):
            y_buf[:, pl.ds(x0 + 2 * h, 2)] = full[:, h * CZ:(h + 1) * CZ].reshape(V, 2, CY, CZ)

    for x0 in range(R, R + CX, 4):
        forward_y(x0)

    load_o.wait()
    seen = jnp.zeros((8, CZ), F32)
    for v in range(V):
        seen = seen + w_buf[1, 1, v:v + 1, :] * jnp.sum(o_buf[v].reshape(CX * CY // 8, 8, CZ), axis=0)
    count_own = jnp.sum(w_buf[1, 1], axis=0, keepdims=True)
    red_own[0] = seen / count_own

    finish((x_copy, xw_copy), "bx")
    for x0 in (0, 4, EX - 8, EX - 4):
        forward_y(x0)

    def forward_x(v, carry):
        t = [jnp.full((8, CZ), taps_s[v, 0, k], F32) for k in range(T)]
        for h in range(CY // 8):
            ys = pl.ds(8 * h, 8)
            acc = [None] * CX
            for xi in range(EX):
                val = y_buf[v, xi, ys, :]
                for xo in range(max(0, xi - T + 1), min(CX, xi + 1)):
                    term = t[xi - xo] * val
                    acc[xo] = term if acc[xo] is None else acc[xo] + term
                if xi >= T - 1:
                    g_buf[v, xi - T + 1, ys, :] = acc[xi - T + 1]
        flipped = flip_tiles(g_buf[v].reshape(CX * CY, CZ))
        sf_buf[v, 0:R] = flipped[CZ - R:]
        sf_buf[v, R:2 * R] = flipped[:R]
        start((functools.partial(zf_copy, v),), "bz")
        return carry

    lax.fori_loop(0, V, forward_x, 0)

    def halo_rows(h_buf):
        flat = h_buf[...].reshape(V * 2 * R, CX * CY)
        return split(jnp.concatenate([flat[:, :128].T, flat[:, 128:].T], axis=0))

    def z_apply(f, halo, mat, v):
        hi, lo = split(f)
        both = dot(jnp.concatenate([hi, halo[0]], axis=1), mat[v])
        rest = dot(jnp.concatenate([lo, halo[1]], axis=1), mat[v, :, 0:128])
        return both[:, :128] + both[:, 128:] + rest

    for v in range(V):
        finish((functools.partial(zf_copy, v),), "bz")
    halo = halo_rows(hf_buf)
    for v in range(V):
        blurred = z_apply(g_buf[v].reshape(CX * CY, CZ), halo, zf_mat, v)
        ratio = o_buf[v].reshape(CX * CY, CZ) / blurred
        r_buf[v] = ratio.reshape(CX, CY, CZ)
        flipped = flip_tiles(ratio)
        sb_buf[v, 0:R] = flipped[CZ - R:]
        sb_buf[v, R:2 * R] = flipped[:R]
        start((functools.partial(zb_copy, v),), "bz")

    for v in range(V):
        finish((functools.partial(zb_copy, v),), "bz")
    halo = halo_rows(hb_buf)
    for v in range(V):
        f = r_buf[v].reshape(CX * CY, CZ)
        g_buf[v] = z_apply(f, halo, zb_mat, v).reshape(CX, CY, CZ)

    def backward_x(v, carry):
        t = [jnp.full((8, CZ), taps_s[v, 0, k], F32) for k in range(T)]
        for h in range(CY // 8):
            ys = pl.ds(8 * h, 8)
            val = [g_buf[v, xi, ys, :] for xi in range(CX)]
            for xo in range(EX):
                acc = None
                for xi in range(max(0, xo - T + 1), min(CX, xo + 1)):
                    term = t[xo - xi] * val[xi]
                    acc = term if acc is None else acc + term
                x_buf[v, xo, ys, :] = acc
        return carry

    lax.fori_loop(0, V, backward_x, 0)

    def backward_y(x0, xb):
        def one(v, acc):
            data = jnp.concatenate(
                [stack4(x_buf[v, pl.ds(x0 + 4 * h, 4)].reshape(4 * CY, CZ)) for h in range(2)], axis=1
            )
            full = dot(yb_mat[v], data)
            new = []
            for h in range(2):
                part = full[:, h * CZ:(h + 1) * CZ].reshape(4, EY, CZ)
                for x in range(4):
                    for t in range(4):
                        w = w_buf[xb, (0, 1, 1, 2)[t], pl.ds(v, 1), :]
                        new.append(w * part[x, 8 * t:8 * t + 8])
            return tuple(a + b for a, b in zip(acc, new))

        acc = lax.fori_loop(0, V, one, tuple(jnp.zeros((8, CZ), F32) for _ in range(32)))
        for x in range(8):
            for t in range(4):
                p_buf[x0 + x, 8 * t:8 * t + 8, :] = acc[4 * x + t]

    backward_y(0, 0)
    backward_y(EX - 8, 2)
    start((rx_copy,), "bx")
    backward_y(R, 1)
    backward_y(2 * R, 1)

    total = jnp.zeros((8, CZ), F32)
    for xb, xs in ((0, range(0, R)), (1, range(R, R + CX)), (2, range(R + CX, EX))):
        for yb, ys in ((0, (0,)), (1, (1, 2)), (2, (3,))):
            count = jnp.maximum(jnp.sum(w_buf[xb, yb], axis=0, keepdims=True), 1.0)
            part = jnp.zeros((8, CZ), F32)
            for x in xs:
                for t in ys:
                    part = part + e_buf[x, 8 * t:8 * t + 8, :] * p_buf[x, 8 * t:8 * t + 8, :]
            total = total + part / count
    red_own[1] = total
    red_own[0] = jnp.where(
        row8 == 0, jnp.sum(red_own[0], axis=0, keepdims=True),
        jnp.where(row8 == 1, jnp.sum(total, axis=0, keepdims=True), 0.0),
    )

    def red_copy(stage, d):
        name, n = LINES[stage]
        return pltpu.make_async_remote_copy(
            src_ref=red_own.at[0 if stage == 0 else stage + 1], dst_ref=red_in.at[stage, d],
            send_sem=red_send.at[stage, d], recv_sem=red_recv.at[stage, d],
            device_id={name: lax.rem(ids[name] + d, n)}, device_id_type=MESH,
        )

    def red_start(stage):
        for d in range(1, LINES[stage][1]):
            red_copy(stage, d).start()

    def red_finish(stage):
        total = red_own[0 if stage == 0 else stage + 1]
        for d in range(1, LINES[stage][1]):
            red_copy(stage, d).wait()
            total = total + red_in[stage, d]
        red_own[stage + 2] = total

    red_start(0)
    red_finish(0)
    red_start(1)

    finish((rx_copy,), "bx")
    p_buf[R:2 * R] = p_buf[R:2 * R] + rx_buf[0]
    p_buf[2 * R:3 * R] = p_buf[2 * R:3 * R] + rx_buf[1]
    start((ry_copy,), "by")
    red_finish(1)
    red_start(2)
    red_finish(2)
    final = red_own[4]
    scale = jnp.sum(final[0:1], axis=1, keepdims=True) / (
        jnp.sum(final[1:2], axis=1, keepdims=True) * count_own[:, 0:1]
    )
    finish((ry_copy,), "by")
    for h in range(2):
        ys = slice(R + 8 * h, R + 8 * h + 8)
        summed = p_buf[R:R + CX, ys, :] + ry_buf[h]
        out[:, 8 * h:8 * h + 8, :] = e_buf[R:R + CX, ys, :] * summed * scale.reshape(1, 1, 1)


def on_device(estimate, observed, coverage, psf_taps):
    dma = pltpu.SemaphoreType.DMA
    return pl.pallas_call(
        kernel,
        out_shape=jax.ShapeDtypeStruct((CX, CY, CZ), F32),
        in_specs=[
            pl.BlockSpec(memory_space=pl.ANY),
            pl.BlockSpec(memory_space=pl.ANY),
            pl.BlockSpec(memory_space=pltpu.SMEM),
            pl.BlockSpec(memory_space=pltpu.SMEM),
            pl.BlockSpec(memory_space=pltpu.VMEM),
        ],
        out_specs=pl.BlockSpec(memory_space=pltpu.VMEM),
        scratch_shapes=[
            pltpu.VMEM((EX, EY, CZ), F32),
            pltpu.VMEM((V, CX, CY, CZ), F32),
            pltpu.VMEM((V, EX, CY, CZ), F32),
            pltpu.VMEM((V, CX, CY, CZ), F32),
            pltpu.VMEM((V, CX, CY, CZ), F32),
            pltpu.VMEM((V, EX, CY, CZ), F32),
            pltpu.VMEM((EX, EY, CZ), F32),
            pltpu.VMEM((2, R, EY, CZ), F32),
            pltpu.VMEM((2, CX, R, CZ), F32),
            pltpu.VMEM((V, 2 * R, CX * CY), F32),
            pltpu.VMEM((V, 2 * R, CX * CY), F32),
            pltpu.VMEM((V, 2 * R, CX * CY), F32),
            pltpu.VMEM((V, 2 * R, CX * CY), F32),
            pltpu.VMEM((3, 3, V, CZ), F32),
            pltpu.VMEM((V, 8, 128), F32),
            pltpu.VMEM((V, 256, 256), BF16),
            pltpu.VMEM((V, 256, 256), BF16),
            pltpu.VMEM((V, 2 * CY, 256), BF16),
            pltpu.VMEM((V, 128, 256), BF16),
            pltpu.VMEM((5, 8, CZ), F32),
            pltpu.VMEM((3, 8, 8, CZ), F32),
            dma((2,)), dma((2,)), dma((2,)), dma((2,)), dma((2,)), dma((2, 2)), dma((2, 2)),
            dma((V, 2)), dma((V, 2)), dma((V, 2)), dma((V, 2)), dma((2,)), dma((2,)), dma((2,)), dma((2,)),
            dma((3, 8)), dma((3, 8)),
        ],
        compiler_params=pltpu.CompilerParams(
            collective_id=0, has_side_effects=True, vmem_limit_bytes=48 * 1024 * 1024
        ),
    )(estimate, observed, coverage, psf_taps, psf_taps)


def solution(mesh):
    block = P("bx", "by", "bz")
    views = P(None, "bx", "by", "bz")
    return jax.shard_map(
        on_device, mesh=mesh, in_specs=(block, views, views, P()), out_specs=block, check_vma=False
    )
```

```python
import functools

import jax
import jax.numpy as jnp
from jax import lax
from jax.experimental import pallas as pl
from jax.experimental.pallas import tpu as pltpu
from jax.sharding import PartitionSpec as P

MESH = pl.DeviceIdType.MESH
F32 = jnp.float32
BF16 = jnp.bfloat16
V, R, T = 8, 8, 17
CX, CY, CZ = 16, 16, 128
EX, EY = CX + 2 * R, CY + 2 * R
G = 4
LINES = (("bz", 4), ("by", 8), ("bx", 4))


def split(f):
    hi = f.astype(BF16)
    lo = (f - hi.astype(F32)).astype(BF16)
    return hi, lo


def dot(a, b):
    return jnp.dot(a, b, preferred_element_type=F32)


def stack4(f):
    hi, lo = split(f)
    return jnp.concatenate([hi, lo, hi, lo], axis=0)


def kernel(
    est, obs, cov, taps, out,
    e_buf, o_buf, y_buf, g_buf, r_buf, x_buf, p_buf, rx_buf, ry_buf,
    sf_buf, hf_buf, sb_buf, hb_buf, w_buf, c_buf, k_buf, t_buf,
    zf_mat, zb_mat, yf_mat, yb_mat, red_own, red_in,
    load_sem, y_send, y_recv, x_send, x_recv, w_send, w_recv,
    zf_send, zf_recv, zb_send, zb_recv, rx_send, rx_recv, ry_send, ry_recv,
    red_send, red_recv,
):
    ids = {name: lax.axis_index(name) for name, _ in LINES}
    sizes = dict(LINES)

    barrier = pltpu.get_barrier_semaphore()
    for name, n in LINES:
        for d in range(1, n):
            pl.semaphore_signal(
                barrier, inc=1, device_id={name: lax.rem(ids[name] + d, n)}, device_id_type=MESH
            )
    load_e = pltpu.make_async_copy(est, e_buf.at[pl.ds(R, CX), pl.ds(R, CY)], load_sem.at[0])
    load_c = pltpu.make_async_copy(cov, c_buf, load_sem.at[1])
    load_t = pltpu.make_async_copy(taps, k_buf, load_sem.at[2])
    load_o = pltpu.make_async_copy(obs, o_buf, load_sem.at[3])
    for load in (load_e, load_c, load_t, load_o):
        load.start()

    def has(name, side):
        return ids[name] > 0 if side == 0 else ids[name] < sizes[name] - 1

    def peer(name, side):
        return {name: ids[name] - 1 if side == 0 else ids[name] + 1}

    def remote(src, dst, send, recv, name, side):
        return pltpu.make_async_remote_copy(
            src_ref=src, dst_ref=dst, send_sem=send, recv_sem=recv,
            device_id=peer(name, side), device_id_type=MESH,
        )

    edge = (pl.ds(0, R), pl.ds(EX - R, R))
    inner = (pl.ds(R, R), pl.ds(CX, R))
    own = pl.ds(R, CX)
    y_parts = (own, edge[0], edge[1])

    def y_copy(side):
        return remote(
            e_buf.at[own, inner[side]], e_buf.at[own, edge[1 - side]],
            y_send.at[side], y_recv.at[1 - side], "by", side,
        )

    def yw_copy(side):
        return remote(
            w_buf.at[1, 1], w_buf.at[1, 2 - 2 * side],
            w_send.at[0, side], w_recv.at[0, 1 - side], "by", side,
        )

    def x_copy(part, side):
        return remote(
            e_buf.at[inner[side], y_parts[part]], e_buf.at[edge[1 - side], y_parts[part]],
            x_send.at[part, side], x_recv.at[part, 1 - side], "bx", side,
        )

    def xw_copy(side):
        return remote(
            w_buf.at[1], w_buf.at[2 - 2 * side],
            w_send.at[1, side], w_recv.at[1, 1 - side], "bx", side,
        )

    def z_copy(s_buf, h_buf, send, recv, g, side):
        views = pl.ds(G * g, G)
        return remote(
            s_buf.at[views, pl.ds(R - R * side, R)], h_buf.at[views, pl.ds(R * side, R)],
            send.at[g, side], recv.at[g, 1 - side], "bz", side,
        )

    def rx_copy(part, side):
        return remote(
            p_buf.at[edge[side], y_parts[part]], rx_buf.at[1 - side, :, y_parts[part]],
            rx_send.at[part, side], rx_recv.at[part, 1 - side], "bx", side,
        )

    def ry_copy(side):
        return remote(
            p_buf.at[own, edge[side]], ry_buf.at[1 - side],
            ry_send.at[side], ry_recv.at[1 - side], "by", side,
        )

    def start(copies, name):
        for side in (0, 1):
            @pl.when(has(name, side))
            def _():
                for c in copies:
                    c(side).start()

    def finish(copies, name):
        for side in (0, 1):
            @pl.when(has(name, side))
            def _():
                for c in copies:
                    c(1 - side).wait_recv()
                    c(side).wait_send()

    part = functools.partial
    x_first = (part(x_copy, 0),)
    x_second = (part(x_copy, 1), part(x_copy, 2), xw_copy)

    for side in (0, 1):
        @pl.when(jnp.logical_not(has("by", side)))
        def _():
            e_buf[R:R + CX, edge[side], :] = jnp.zeros((CX, R, CZ), F32)
            w_buf[1, 2 * side] = jnp.zeros((V, CZ), F32)
            ry_buf[side] = jnp.zeros((CX, R, CZ), F32)

        @pl.when(jnp.logical_not(has("bx", side)))
        def _():
            e_buf[edge[side]] = jnp.zeros((R, EY, CZ), F32)
            w_buf[2 * side] = jnp.zeros((3, V, CZ), F32)
            rx_buf[side] = jnp.zeros((R, EY, CZ), F32)

        @pl.when(jnp.logical_not(has("bz", side)))
        def _():
            rows = pl.ds(R - R * side, R)
            hf_buf[:, rows, :] = jnp.zeros((V, R, CX * CY), F32)
            hb_buf[:, rows, :] = jnp.zeros((V, R, CX * CY), F32)

    row8 = lax.broadcasted_iota(jnp.int32, (V, CZ), 0)
    lane8 = lax.broadcasted_iota(jnp.int32, (V, CZ), 1)
    load_c.wait()
    flags = jnp.broadcast_to(c_buf[...].astype(F32), (V, V))
    picked = jnp.where(row8[:, :V] == lane8[:, :V], flags, 0.0)
    w_buf[1, 1] = jnp.broadcast_to(jnp.sum(picked, axis=1, keepdims=True), (V, CZ))
    load_e.wait()
    pl.semaphore_wait(barrier, sum(n - 1 for _, n in LINES))
    start((y_copy, yw_copy), "by")
    start(x_first, "bx")

    load_t.wait()
    t_buf[...] = jnp.zeros_like(t_buf)
    for d in range(3):
        t_buf[d, :, 0:T] = k_buf[d]
    taps_x, taps_y, taps_z = (
        t_buf[d] / jnp.sum(t_buf[d], axis=1, keepdims=True) for d in range(3)
    )
    taps_y = taps_y + pltpu.roll(taps_y, 32, 1)
    taps_y = taps_y + pltpu.roll(taps_y, 64, 1)
    band = lax.broadcasted_iota(jnp.int32, (CY, 128), 1)
    bands = []
    for v in range(V):
        q = pltpu.roll(
            jnp.broadcast_to(taps_y[v:v + 1], (CY, 128)), 0, 1, stride=1, stride_axis=0
        )
        bands.append(q)
        q_hi, q_lo = split(q)
        zero = jnp.zeros_like(q_hi)
        for x in range(2):
            mine = (band // 32) % 2 == x
            yf_mat[v, x * CY:(x + 1) * CY, 0:128] = jnp.where(mine, q_hi, zero)
            yf_mat[v, x * CY:(x + 1) * CY, 128:256] = jnp.where(mine, q_lo, zero)
    for k in range(T):
        t_buf[3 + k] = jnp.broadcast_to(taps_x[:, k:k + 1], (V, CZ))

    finish((y_copy, yw_copy), "by")
    start(x_second, "bx")

    def forward_y(x0):
        data = jnp.concatenate(
            [stack4(e_buf[pl.ds(x0 + 2 * h, 2)].reshape(2 * EY, CZ)) for h in range(2)], axis=1
        )
        full = dot(yf_mat[...].reshape(V * 2 * CY, 256), data)
        for h in range(2):
            y_buf[:, pl.ds(x0 + 2 * h, 2)] = full[:, h * CZ:(h + 1) * CZ].reshape(V, 2, CY, CZ)

    for x0 in range(R, R + CX, 4):
        forward_y(x0)

    def x_taps(v):
        return [jnp.broadcast_to(t_buf[3 + k, pl.ds(v, 1), :], (8, CZ)) for k in range(T)]

    def forward_x(inputs, first, v, carry):
        t = x_taps(v)
        for h in range(CY // 8):
            ys = pl.ds(8 * h, 8)
            acc = [None if first else g_buf[v, xo, ys, :] for xo in range(CX)]
            for xi in inputs:
                val = y_buf[v, xi, ys, :]
                for xo in range(max(0, xi - T + 1), min(CX, xi + 1)):
                    term = t[xi - xo] * val
                    acc[xo] = term if acc[xo] is None else acc[xo] + term
            for xo in range(CX):
                g_buf[v, xo, ys, :] = acc[xo]
        return carry

    lax.fori_loop(0, V, part(forward_x, range(R, R + CX), True), 0)

    lane = lax.broadcasted_iota(jnp.int32, (128, 128), 1)
    row = lax.broadcasted_iota(jnp.int32, (128, 128), 0)
    near = jnp.abs(row - lane) <= R
    for mat in (zf_mat, zb_mat):
        mat[:, 128:192, :] = jnp.zeros((V, 64, 256), BF16)
    for v in range(V):
        ring = pltpu.roll(
            jnp.broadcast_to(taps_z[v:v + 1], (128, 128)), 128 - R, 1, stride=1, stride_axis=0
        )
        for mat, full in ((zb_mat, ring), (zf_mat, ring.T)):
            m_hi, m_lo = split(jnp.where(near, full, 0.0))
            mat[v, 0:128, 0:128] = m_hi
            mat[v, 0:128, 128:256] = m_lo
            far = jnp.where(near, 0.0, full)
            far = jnp.concatenate([far[0:R], far[128 - R:128]], axis=0)
            f_hi, f_lo = split(far)
            at = 128 + 2 * R * (v % G)
            mat[v, at:at + 2 * R, 0:128] = f_hi
            mat[v, at:at + 2 * R, 128:256] = f_lo

    load_o.wait()
    seen = jnp.zeros((8, CZ), F32)
    for v in range(V):
        seen = seen + w_buf[1, 1, v:v + 1, :] * jnp.sum(o_buf[v].reshape(CX * CY // 8, 8, CZ), axis=0)
    count_own = jnp.sum(w_buf[1, 1], axis=0, keepdims=True)
    red_own[1] = seen / count_own

    finish(x_first + x_second, "bx")
    for x0 in (0, 4, EX - 8, EX - 4):
        forward_y(x0)

    def send_edges(fields, s_buf, h_buf, send, recv, g):
        for v, f in zip(range(G * g, G * g + G), fields):
            for h in range(2):
                flipped = f[128 * h:128 * h + 128].T
                s_buf[v, 0:R, 128 * h:128 * h + 128] = flipped[CZ - R:]
                s_buf[v, R:2 * R, 128 * h:128 * h + 128] = flipped[:R]
        start((part(z_copy, s_buf, h_buf, send, recv, g),), "bz")

    def halo_rows(h_buf, g):
        flat = h_buf[G * g:G * g + G].reshape(G * 2 * R, CX * CY)
        return split(jnp.concatenate([flat[:, :128].T, flat[:, 128:].T], axis=0))

    def z_apply(f, halo, mat, v):
        hi, lo = split(f)
        both = dot(jnp.concatenate([hi, halo[0]], axis=1), mat[v])
        rest = dot(jnp.concatenate([lo, halo[1]], axis=1), mat[v, :, 0:128])
        return both[:, :128] + both[:, 128:] + rest

    forward = (sf_buf, hf_buf, zf_send, zf_recv)
    backward = (sb_buf, hb_buf, zb_send, zb_recv)
    halo_planes = tuple(range(R)) + tuple(range(R + CX, EX))
    for g in range(V // G):
        lax.fori_loop(G * g, G * g + G, part(forward_x, halo_planes, False), 0)
        send_edges(
            [g_buf[v].reshape(CX * CY, CZ) for v in range(G * g, G * g + G)], *forward, g
        )

    for v in range(V):
        q4 = jnp.concatenate(
            [jnp.where(band // 32 == i // 2, bands[v], 0.0) for i in range(8)], axis=0
        ).T
        both = split(q4)
        for xb in range(3):
            w = [jnp.broadcast_to(w_buf[xb, yb, v:v + 1, :], (8, CZ)) for yb in (0, 1, 1, 2)]
            w = jnp.concatenate(w * 4, axis=0).astype(BF16)
            for i in range(2):
                yb_mat[xb, v, :, 128 * i:128 * i + 128] = both[i] * w

    for g in range(V // G):
        finish((part(z_copy, *forward, g),), "bz")
        halo = halo_rows(hf_buf, g)
        ratios = []
        for v in range(G * g, G * g + G):
            blurred = z_apply(g_buf[v].reshape(CX * CY, CZ), halo, zf_mat, v)
            ratio = o_buf[v].reshape(CX * CY, CZ) / blurred
            r_buf[v] = ratio.reshape(CX, CY, CZ)
            ratios.append(ratio)
        send_edges(ratios, *backward, g)

    def backward_x(outputs, v, carry):
        t = x_taps(v)
        for xo in outputs:
            accs = []
            for h in range(CY // 8):
                ys = pl.ds(8 * h, 8)
                acc = None
                for xi in range(max(0, xo - T + 1), min(CX, xo + 1)):
                    term = t[xo - xi] * g_buf[v, xi, ys, :]
                    acc = term if acc is None else acc + term
                accs.append(acc)
            hi, lo = split(jnp.concatenate(accs, axis=0))
            x_buf[v, xo, 0:CY, :] = hi
            x_buf[v, xo, CY:2 * CY, :] = lo
        return carry

    for g in range(V // G):
        finish((part(z_copy, *backward, g),), "bz")
        halo = halo_rows(hb_buf, g)
        for v in range(G * g, G * g + G):
            f = r_buf[v].reshape(CX * CY, CZ)
            g_buf[v] = z_apply(f, halo, zb_mat, v).reshape(CX, CY, CZ)
        lax.fori_loop(G * g, G * g + G, part(backward_x, halo_planes), 0)

    def backward_y(x0, xb):
        full = None
        for v in range(V):
            data = []
            for h in range(2):
                planes = x_buf[v, x0 + 4 * h:x0 + 4 * h + 4].reshape(128, CZ)
                data.append(jnp.concatenate([planes, planes], axis=0))
            term = dot(yb_mat[xb, v], jnp.concatenate(data, axis=1))
            full = term if full is None else full + term
        for h in range(2):
            p_buf[x0 + 4 * h:x0 + 4 * h + 4] = full[:, h * CZ:(h + 1) * CZ].reshape(4, EY, CZ)

    backward_y(0, 0)
    backward_y(EX - 8, 2)
    rx_edges = (part(rx_copy, 1), part(rx_copy, 2))
    rx_own = (part(rx_copy, 0),)
    start(rx_edges + rx_own, "bx")
    lax.fori_loop(0, V, part(backward_x, range(R, R + CX)), 0)
    backward_y(R, 1)
    backward_y(2 * R, 1)

    total = jnp.zeros((8, CZ), F32)
    for xb, xs in ((0, range(0, R)), (1, range(R, R + CX)), (2, range(R + CX, EX))):
        for yb, ys in ((0, (0,)), (1, (1, 2)), (2, (3,))):
            count = jnp.maximum(jnp.sum(w_buf[xb, yb], axis=0, keepdims=True), 1.0)
            term = jnp.zeros((8, CZ), F32)
            for x in xs:
                for t in ys:
                    term = term + e_buf[x, 8 * t:8 * t + 8, :] * p_buf[x, 8 * t:8 * t + 8, :]
            total = total + term / count
    red_own[0] = jnp.where(
        row8 == 0, jnp.sum(red_own[1], axis=0, keepdims=True),
        jnp.where(row8 == 1, jnp.sum(total, axis=0, keepdims=True), 0.0),
    )

    def red_copy(stage, d):
        name, n = LINES[stage]
        return pltpu.make_async_remote_copy(
            src_ref=red_own.at[0 if stage == 0 else stage + 1], dst_ref=red_in.at[stage, d],
            send_sem=red_send.at[stage, d], recv_sem=red_recv.at[stage, d],
            device_id={name: lax.rem(ids[name] + d, n)}, device_id_type=MESH,
        )

    def red_start(stage):
        for d in range(1, LINES[stage][1]):
            red_copy(stage, d).start()

    def red_finish(stage):
        total = red_own[0 if stage == 0 else stage + 1]
        for d in range(1, LINES[stage][1]):
            red_copy(stage, d).wait()
            total = total + red_in[stage, d]
        red_own[stage + 2] = total

    red_start(0)
    red_finish(0)
    red_start(1)

    finish(rx_edges, "bx")
    for t in (0, 3):
        ys = slice(8 * t, 8 * t + 8)
        p_buf[R:2 * R, ys] = p_buf[R:2 * R, ys] + rx_buf[0, :, ys]
        p_buf[2 * R:3 * R, ys] = p_buf[2 * R:3 * R, ys] + rx_buf[1, :, ys]
    start((ry_copy,), "by")
    red_finish(1)
    red_start(2)
    red_finish(2)
    final = red_own[4]
    scale = jnp.sum(final[0:1], axis=1, keepdims=True) / (
        jnp.sum(final[1:2], axis=1, keepdims=True) * count_own[:, 0:1]
    )
    finish(rx_own, "bx")
    finish((ry_copy,), "by")
    for s in range(2):
        xs = slice(R + 8 * s, R + 8 * s + 8)
        for h in range(2):
            ys = slice(R + 8 * h, R + 8 * h + 8)
            summed = p_buf[xs, ys, :] + rx_buf[s, :, ys] + ry_buf[h, 8 * s:8 * s + 8]
            out[8 * s:8 * s + 8, 8 * h:8 * h + 8, :] = e_buf[xs, ys, :] * summed * scale.reshape(1, 1, 1)


def on_device(estimate, observed, coverage, psf_taps):
    dma = pltpu.SemaphoreType.DMA
    arrays = (estimate, observed, coverage.reshape(1, V), jnp.transpose(psf_taps, (1, 0, 2)))
    return pl.pallas_call(
        kernel,
        out_shape=jax.ShapeDtypeStruct((CX, CY, CZ), F32),
        in_specs=[pl.BlockSpec(memory_space=pltpu.HBM)] * 4,
        out_specs=pl.BlockSpec(memory_space=pltpu.VMEM),
        scratch_shapes=[
            pltpu.VMEM((EX, EY, CZ), F32),
            pltpu.VMEM((V, CX, CY, CZ), F32),
            pltpu.VMEM((V, EX, CY, CZ), F32),
            pltpu.VMEM((V, CX, CY, CZ), F32),
            pltpu.VMEM((V, CX, CY, CZ), F32),
            pltpu.VMEM((V, EX, 2 * CY, CZ), BF16),
            pltpu.VMEM((EX, EY, CZ), F32),
            pltpu.VMEM((2, R, EY, CZ), F32),
            pltpu.VMEM((2, CX, R, CZ), F32),
            pltpu.VMEM((V, 2 * R, CX * CY), F32),
            pltpu.VMEM((V, 2 * R, CX * CY), F32),
            pltpu.VMEM((V, 2 * R, CX * CY), F32),
            pltpu.VMEM((V, 2 * R, CX * CY), F32),
            pltpu.VMEM((3, 3, V, CZ), F32),
            pltpu.VMEM((1, V), jnp.int32),
            pltpu.VMEM((3, V, T), F32),
            pltpu.VMEM((3 + T, V, CZ), F32),
            pltpu.VMEM((V, 192, 256), BF16),
            pltpu.VMEM((V, 192, 256), BF16),
            pltpu.VMEM((V, 2 * CY, 256), BF16),
            pltpu.VMEM((3, V, 128, 256), BF16),
            pltpu.VMEM((5, 8, CZ), F32),
            pltpu.VMEM((3, 8, 8, CZ), F32),
            dma((4,)), dma((2,)), dma((2,)), dma((3, 2)), dma((3, 2)), dma((2, 2)), dma((2, 2)),
            dma((2, 2)), dma((2, 2)), dma((2, 2)), dma((2, 2)), dma((3, 2)), dma((3, 2)), dma((2,)), dma((2,)),
            dma((3, 8)), dma((3, 8)),
        ],
        compiler_params=pltpu.CompilerParams(
            collective_id=0, has_side_effects=True, vmem_limit_bytes=48 * 1024 * 1024
        ),
    )(*[pltpu.with_memory_space_constraint(a, pltpu.HBM) for a in arrays])


def solution(mesh):
    block = P("bx", "by", "bz")
    views = P(None, "bx", "by", "bz")
    return jax.shard_map(
        on_device, mesh=mesh, in_specs=(block, views, views, P()), out_specs=block, check_vma=False
    )
```

```python
import functools

import jax
import jax.numpy as jnp
from jax import lax
from jax.experimental import pallas as pl
from jax.experimental.pallas import tpu as pltpu
from jax.sharding import PartitionSpec as P

MESH = pl.DeviceIdType.MESH
F32 = jnp.float32
BF16 = jnp.bfloat16
V, R, T = 8, 8, 17
CX, CY, CZ = 16, 16, 128
EX, EY = CX + 2 * R, CY + 2 * R
G = 4
LINES = (("bz", 4), ("by", 8), ("bx", 4))
STAGES = (8, 16)


def split(f):
    hi = f.astype(BF16)
    lo = (f - hi.astype(F32)).astype(BF16)
    return hi, lo


def dot(a, b):
    return jnp.dot(a, b, preferred_element_type=F32)


def stack4(f):
    hi, lo = split(f)
    return jnp.concatenate([hi, lo, hi, lo], axis=0)


def kernel(
    est, obs, cov, taps, out,
    e_buf, o_buf, y_buf, g_buf, r_buf, x_buf, p_buf, rx_buf, ry_buf,
    sf_buf, hf_buf, sb_buf, hb_buf, w_buf, c_buf, k_buf, t_buf,
    zf_mat, zb_mat, yf_mat, yw_mat, yb_mat, b_buf, seen_buf, red_own, red_in,
    load_sem, y_send, y_recv, x_send, x_recv, w_send, w_recv,
    zf_send, zf_recv, zb_send, zb_recv, rx_send, rx_recv, ry_send, ry_recv,
    red_send, red_recv, met_sem,
):
    ids = {name: lax.axis_index(name) for name, _ in LINES}
    sizes = dict(LINES)

    barrier = pltpu.get_barrier_semaphore()
    for name, n in LINES:
        for d in range(1, n):
            pl.semaphore_signal(
                barrier, inc=1, device_id={name: lax.rem(ids[name] + d, n)}, device_id_type=MESH
            )
    load_e = pltpu.make_async_copy(est, e_buf.at[pl.ds(R, CX), pl.ds(R, CY)], load_sem.at[0])
    load_c = pltpu.make_async_copy(cov, c_buf, load_sem.at[1])
    load_t = pltpu.make_async_copy(taps, k_buf, load_sem.at[2])
    load_o = pltpu.make_async_copy(obs, o_buf, load_sem.at[3])
    for load in (load_e, load_c, load_t, load_o):
        load.start()

    def has(name, side):
        return ids[name] > 0 if side == 0 else ids[name] < sizes[name] - 1

    def peer(name, side):
        return {name: ids[name] - 1 if side == 0 else ids[name] + 1}

    def remote(src, dst, send, recv, name, side):
        return pltpu.make_async_remote_copy(
            src_ref=src, dst_ref=dst, send_sem=send, recv_sem=recv,
            device_id=peer(name, side), device_id_type=MESH,
        )

    edge = (pl.ds(0, R), pl.ds(EX - R, R))
    inner = (pl.ds(R, R), pl.ds(CX, R))
    own = pl.ds(R, CX)
    y_parts = (own, edge[0], edge[1])

    def y_copy(side):
        return remote(
            e_buf.at[own, inner[side]], e_buf.at[own, edge[1 - side]],
            y_send.at[side], y_recv.at[1 - side], "by", side,
        )

    def yw_copy(side):
        return remote(
            w_buf.at[1, 1], w_buf.at[1, 2 - 2 * side],
            w_send.at[0, side], w_recv.at[0, 1 - side], "by", side,
        )

    def x_copy(part, side):
        return remote(
            e_buf.at[inner[side], y_parts[part]], e_buf.at[edge[1 - side], y_parts[part]],
            x_send.at[part, side], x_recv.at[part, 1 - side], "bx", side,
        )

    def xw_copy(side):
        return remote(
            w_buf.at[1], w_buf.at[2 - 2 * side],
            w_send.at[1, side], w_recv.at[1, 1 - side], "bx", side,
        )

    def z_copy(s_buf, h_buf, send, recv, g, side):
        views = pl.ds(G * g, G)
        return remote(
            s_buf.at[views, pl.ds(R - R * side, R)], h_buf.at[views, pl.ds(R * side, R)],
            send.at[g, side], recv.at[g, 1 - side], "bz", side,
        )

    def rx_copy(part, side):
        return remote(
            p_buf.at[edge[side], y_parts[part]], rx_buf.at[1 - side, :, y_parts[part]],
            rx_send.at[part, side], rx_recv.at[part, 1 - side], "bx", side,
        )

    def ry_copy(side):
        return remote(
            p_buf.at[own, edge[side]], ry_buf.at[1 - side],
            ry_send.at[side], ry_recv.at[1 - side], "by", side,
        )

    def start(copies, name):
        for side in (0, 1):
            @pl.when(has(name, side))
            def _():
                for c in copies:
                    c(side).start()

    def finish(copies, name):
        for side in (0, 1):
            @pl.when(has(name, side))
            def _():
                for c in copies:
                    c(1 - side).wait_recv()
                    sent[name, side].append(c)

    sent = {(name, side): [] for name, _ in LINES for side in (0, 1)}
    part = functools.partial
    x_first = (part(x_copy, 0),)
    x_second = (part(x_copy, 1), part(x_copy, 2), xw_copy)

    for side in (0, 1):
        @pl.when(jnp.logical_not(has("by", side)))
        def _():
            e_buf[R:R + CX, edge[side], :] = jnp.zeros((CX, R, CZ), F32)
            w_buf[1, 2 * side] = jnp.zeros((V, CZ), F32)
            ry_buf[side] = jnp.zeros((CX, R, CZ), F32)

        @pl.when(jnp.logical_not(has("bx", side)))
        def _():
            e_buf[edge[side]] = jnp.zeros((R, EY, CZ), F32)
            w_buf[2 * side] = jnp.zeros((3, V, CZ), F32)
            rx_buf[side] = jnp.zeros((R, EY, CZ), F32)

        @pl.when(jnp.logical_not(has("bz", side)))
        def _():
            rows = pl.ds(R - R * side, R)
            hf_buf[:, rows, :] = jnp.zeros((V, R, CX * CY), F32)
            hb_buf[:, rows, :] = jnp.zeros((V, R, CX * CY), F32)

    row8 = lax.broadcasted_iota(jnp.int32, (V, CZ), 0)
    lane8 = lax.broadcasted_iota(jnp.int32, (V, CZ), 1)
    load_c.wait()
    flags = jnp.broadcast_to(c_buf[...].astype(F32), (V, V))
    picked = jnp.where(row8[:, :V] == lane8[:, :V], flags, 0.0)
    w_buf[1, 1] = jnp.broadcast_to(jnp.sum(picked, axis=1, keepdims=True), (V, CZ))
    load_e.wait()
    pl.semaphore_wait(barrier, sum(n - 1 for _, n in LINES))
    for name, n in LINES:
        for d in range(1, n):
            pl.semaphore_signal(
                met_sem, inc=1, device_id={name: lax.rem(ids[name] + d, n)}, device_id_type=MESH
            )
    start((y_copy, yw_copy), "by")
    start(x_first, "bx")

    load_t.wait()
    t_buf[...] = jnp.zeros_like(t_buf)
    for d in range(3):
        t_buf[d, :, 0:T] = k_buf[d]
    taps_x, taps_y, taps_z = (
        t_buf[d] / jnp.sum(t_buf[d], axis=1, keepdims=True) for d in range(3)
    )
    taps_y = taps_y + pltpu.roll(taps_y, 32, 1)
    taps_y = taps_y + pltpu.roll(taps_y, 64, 1)
    band = lax.broadcasted_iota(jnp.int32, (CY, 128), 1)
    bands = []
    for v in range(V):
        q = pltpu.roll(
            jnp.broadcast_to(taps_y[v:v + 1], (CY, 128)), 0, 1, stride=1, stride_axis=0
        )
        bands.append(q)
        q_hi, q_lo = split(q)
        zero = jnp.zeros_like(q_hi)
        for x in range(2):
            mine = (band // 32) % 2 == x
            yf_mat[v, x * CY:(x + 1) * CY, 0:128] = jnp.where(mine, q_hi, zero)
            yf_mat[v, x * CY:(x + 1) * CY, 128:256] = jnp.where(mine, q_lo, zero)
    for k in range(T):
        t_buf[3 + k] = jnp.broadcast_to(taps_x[:, k:k + 1], (V, CZ))

    finish((y_copy, yw_copy), "by")
    start(x_second, "bx")

    def forward_y(x0, source=e_buf, mat=yf_mat):
        data = jnp.concatenate(
            [stack4(source[pl.ds(x0 + 2 * h, 2)].reshape(2 * EY, CZ)) for h in range(2)], axis=1
        )
        full = dot(mat[...].reshape(V * 2 * CY, 256), data)
        for h in range(2):
            y_buf[:, pl.ds(x0 + 2 * h, 2)] = full[:, h * CZ:(h + 1) * CZ].reshape(V, 2, CY, CZ)

    for x0 in range(R, R + CX, 4):
        forward_y(x0)

    def x_taps(v):
        return [jnp.broadcast_to(t_buf[3 + k, pl.ds(v, 1), :], (8, CZ)) for k in range(T)]

    def forward_x(inputs, first, g_buf, v, carry):
        t = x_taps(v)
        for h in range(CY // 8):
            ys = pl.ds(8 * h, 8)
            acc = [None if first else g_buf[v, xo, ys, :] for xo in range(CX)]
            for xi in inputs:
                val = y_buf[v, xi, ys, :]
                for xo in range(max(0, xi - T + 1), min(CX, xi + 1)):
                    term = t[xi - xo] * val
                    acc[xo] = term if acc[xo] is None else acc[xo] + term
            for xo in range(CX):
                g_buf[v, xo, ys, :] = acc[xo]
        return carry

    lax.fori_loop(0, V, part(forward_x, range(R, R + CX), True, g_buf), 0)

    lane = lax.broadcasted_iota(jnp.int32, (128, 128), 1)
    row = lax.broadcasted_iota(jnp.int32, (128, 128), 0)
    near = jnp.abs(row - lane) <= R
    for mat in (zf_mat, zb_mat):
        mat[:, 128:192, :] = jnp.zeros((V, 64, 256), BF16)
    for v in range(V):
        ring = pltpu.roll(
            jnp.broadcast_to(taps_z[v:v + 1], (128, 128)), 128 - R, 1, stride=1, stride_axis=0
        )
        for mat, full in ((zb_mat, ring), (zf_mat, ring.T)):
            m_hi, m_lo = split(jnp.where(near, full, 0.0))
            mat[v, 0:128, 0:128] = m_hi
            mat[v, 0:128, 128:256] = m_lo
            far = jnp.where(near, 0.0, full)
            far = jnp.concatenate([far[0:R], far[128 - R:128]], axis=0)
            f_hi, f_lo = split(far)
            at = 128 + 2 * R * (v % G)
            mat[v, at:at + 2 * R, 0:128] = f_hi
            mat[v, at:at + 2 * R, 128:256] = f_lo

    load_o.wait()
    seen = jnp.zeros((8, CZ), F32)
    for v in range(V):
        seen = seen + w_buf[1, 1, v:v + 1, :] * jnp.sum(o_buf[v].reshape(CX * CY // 8, 8, CZ), axis=0)
    count_own = jnp.sum(w_buf[1, 1], axis=0, keepdims=True)
    seen_buf[...] = seen / count_own

    finish(x_first + x_second, "bx")
    for x0 in (0, 4, EX - 8, EX - 4):
        forward_y(x0)

    def send_edges(fields, s_buf, h_buf, send, recv, g):
        for v, f in zip(range(G * g, G * g + G), fields):
            for h in range(2):
                flipped = f[128 * h:128 * h + 128].T
                s_buf[v, 0:R, 128 * h:128 * h + 128] = flipped[CZ - R:]
                s_buf[v, R:2 * R, 128 * h:128 * h + 128] = flipped[:R]
        start((part(z_copy, s_buf, h_buf, send, recv, g),), "bz")

    def halo_rows(h_buf, g):
        flat = h_buf[G * g:G * g + G].reshape(G * 2 * R, CX * CY)
        return split(jnp.concatenate([flat[:, :128].T, flat[:, 128:].T], axis=0))

    def z_apply(f, halo, mat, v):
        hi, lo = split(f)
        both = dot(jnp.concatenate([hi, halo[0]], axis=1), mat[v])
        rest = dot(jnp.concatenate([lo, halo[1]], axis=1), mat[v, :, 0:128])
        return both[:, :128] + both[:, 128:] + rest

    forward = (sf_buf, hf_buf, zf_send, zf_recv)
    backward = (sb_buf, hb_buf, zb_send, zb_recv)
    halo_planes = tuple(range(R)) + tuple(range(R + CX, EX))
    for g in range(V // G):
        lax.fori_loop(G * g, G * g + G, part(forward_x, halo_planes, False, g_buf), 0)
        send_edges(
            [g_buf[v].reshape(CX * CY, CZ) for v in range(G * g, G * g + G)], *forward, g
        )

    for v in range(V):
        q4 = jnp.concatenate(
            [jnp.where(band // 32 == i // 2, bands[v], 0.0) for i in range(8)], axis=0
        ).T
        both = split(q4)
        for xb in range(3):
            w = [jnp.broadcast_to(w_buf[xb, yb, v:v + 1, :], (8, CZ)) for yb in (0, 1, 1, 2)]
            w = jnp.concatenate(w * 4, axis=0).astype(BF16)
            for i in range(2):
                yb_mat[xb, v, :, 128 * i:128 * i + 128] = both[i] * w

    third = (band % 32)[:8]
    for xb, xs in ((0, (0, R)), (1, (R, R + CX)), (2, (R + CX, EX))):
        for yb, ys in ((0, (0, R)), (1, (R, R + CY)), (2, (R + CY, EY))):
            count = jnp.maximum(jnp.sum(w_buf[xb, yb], axis=0, keepdims=True), 1.0)
            p_buf[xs[0]:xs[1], ys[0]:ys[1]] = e_buf[xs[0]:xs[1], ys[0]:ys[1]] * (1.0 / count)
        w = jnp.where(third < R, w_buf[xb, 0], jnp.where(third < R + CY, w_buf[xb, 1], w_buf[xb, 2]))
        for v in range(V):
            wide = jnp.broadcast_to(w[v:v + 1], (2 * CY, CZ)).astype(BF16)
            for i in range(2):
                cols = slice(128 * i, 128 * i + 128)
                yw_mat[xb, v, :, cols] = yf_mat[v, :, cols] * wide
    for x0 in range(0, EX, 4):
        forward_y(x0, p_buf, yw_mat.at[0 if x0 < R else 1 if x0 < R + CX else 2])

    for g in range(V // G):
        finish((part(z_copy, *forward, g),), "bz")
        halo = halo_rows(hf_buf, g)
        ratios = []
        for v in range(G * g, G * g + G):
            blurred = z_apply(g_buf[v].reshape(CX * CY, CZ), halo, zf_mat, v)
            ratio = o_buf[v].reshape(CX * CY, CZ) / blurred
            r_buf[v] = ratio.reshape(CX, CY, CZ)
            ratios.append(ratio)
        send_edges(ratios, *backward, g)

    def backward_x(outputs, v, carry):
        t = x_taps(v)
        for xo in outputs:
            accs = []
            for h in range(CY // 8):
                ys = pl.ds(8 * h, 8)
                acc = None
                for xi in range(max(0, xo - T + 1), min(CX, xo + 1)):
                    term = t[xo - xi] * g_buf[v, xi, ys, :]
                    acc = term if acc is None else acc + term
                accs.append(acc)
            hi, lo = split(jnp.concatenate(accs, axis=0))
            x_buf[v, xo, 0:CY, :] = hi
            x_buf[v, xo, CY:2 * CY, :] = lo
        return carry

    lax.fori_loop(0, V, part(forward_x, range(EX), True, b_buf), 0)

    total = jnp.zeros((8, CZ), F32)
    for g in range(V // G):
        finish((part(z_copy, *backward, g),), "bz")
        halo = halo_rows(hb_buf, g)
        for v in range(G * g, G * g + G):
            f = z_apply(r_buf[v].reshape(CX * CY, CZ), halo, zb_mat, v)
            g_buf[v] = f.reshape(CX, CY, CZ)
            weighed = f * b_buf[v].reshape(CX * CY, CZ)
            total = total + jnp.sum(weighed.reshape(CX * CY // 8, 8, CZ), axis=0)

    lane1 = lax.broadcasted_iota(jnp.int32, (1, CZ), 1)

    def summed(f):
        return jnp.sum(jnp.sum(f, axis=0, keepdims=True), axis=1, keepdims=True)

    red_own[0] = jnp.where(lane1 < CZ // 2, summed(seen_buf[...]), summed(total))

    by_hi, by_lo = lax.div(ids["by"], 4), lax.rem(ids["by"], 4)

    def red_peer(stage, d):
        if stage == 0:
            return {
                "bx": lax.rem(ids["bx"] + d % 4, 4),
                "by": lax.rem(by_hi + d // 4, 2) * 4 + by_lo,
            }
        return {
            "bz": lax.rem(ids["bz"] + d % 4, 4),
            "by": by_hi * 4 + lax.rem(by_lo + d // 4, 4),
        }

    def red_copy(stage, d):
        return pltpu.make_async_remote_copy(
            src_ref=red_own.at[stage], dst_ref=red_in.at[stage, d],
            send_sem=red_send.at[stage], recv_sem=red_recv.at[stage],
            device_id=red_peer(stage, d), device_id_type=MESH,
        )

    def red_start(stage):
        for d in range(1, STAGES[stage]):
            red_copy(stage, d).start()

    def red_all(stage):
        every = red_in.at[stage, pl.ds(1, STAGES[stage] - 1)]
        return pltpu.make_async_remote_copy(
            src_ref=every, dst_ref=every, send_sem=red_send.at[stage],
            recv_sem=red_recv.at[stage], device_id=red_peer(stage, 1), device_id_type=MESH,
        )

    def red_finish(stage):
        red_all(stage).wait_recv()
        total = red_own[stage]
        for d in range(1, STAGES[stage]):
            total = total + red_in[stage, d]
        return total

    pl.semaphore_wait(met_sem, sum(n - 1 for _, n in LINES))
    red_start(0)
    lax.fori_loop(0, V, part(backward_x, halo_planes), 0)

    def backward_y(x0, xb):
        full = None
        for v in range(V):
            data = []
            for h in range(2):
                planes = x_buf[v, x0 + 4 * h:x0 + 4 * h + 4].reshape(128, CZ)
                data.append(jnp.concatenate([planes, planes], axis=0))
            term = dot(yb_mat[xb, v], jnp.concatenate(data, axis=1))
            full = term if full is None else full + term
        for h in range(2):
            p_buf[x0 + 4 * h:x0 + 4 * h + 4] = full[:, h * CZ:(h + 1) * CZ].reshape(4, EY, CZ)

    backward_y(0, 0)
    backward_y(EX - 8, 2)
    rx_edges = (part(rx_copy, 1), part(rx_copy, 2))
    rx_own = (part(rx_copy, 0),)
    start(rx_edges + rx_own, "bx")
    lax.fori_loop(0, V, part(backward_x, range(R, R + CX)), 0)
    red_own[1] = red_finish(0)
    red_start(1)
    backward_y(R, 1)
    backward_y(2 * R, 1)

    finish(rx_edges, "bx")
    for t in (0, 3):
        ys = slice(8 * t, 8 * t + 8)
        p_buf[R:2 * R, ys] = p_buf[R:2 * R, ys] + rx_buf[0, :, ys]
        p_buf[2 * R:3 * R, ys] = p_buf[2 * R:3 * R, ys] + rx_buf[1, :, ys]
    start((ry_copy,), "by")
    finish(rx_own, "bx")
    finish((ry_copy,), "by")
    for s in range(2):
        xs = slice(R + 8 * s, R + 8 * s + 8)
        for h in range(2):
            ys = slice(R + 8 * h, R + 8 * h + 8)
            summed = p_buf[xs, ys, :] + rx_buf[s, :, ys] + ry_buf[h, 8 * s:8 * s + 8]
            out[8 * s:8 * s + 8, 8 * h:8 * h + 8, :] = e_buf[xs, ys, :] * summed
    for name, _ in LINES:
        for side in (0, 1):
            @pl.when(has(name, side))
            def _():
                for c in sent[name, side]:
                    c(side).wait_send()
    red_all(0).wait_send()
    red_all(1).wait_send()
    final = red_finish(1)
    scale = final[:, 0:1] / (final[:, CZ // 2:CZ // 2 + 1] * count_own[:, 0:1])
    out[...] = out[...] * scale.reshape(1, 1, 1)


def on_device(estimate, observed, coverage, psf_taps):
    dma = pltpu.SemaphoreType.DMA
    arrays = (estimate, observed, coverage.reshape(1, V), jnp.transpose(psf_taps, (1, 0, 2)))
    return pl.pallas_call(
        kernel,
        out_shape=jax.ShapeDtypeStruct((CX, CY, CZ), F32),
        in_specs=[pl.BlockSpec(memory_space=pltpu.HBM)] * 4,
        out_specs=pl.BlockSpec(memory_space=pltpu.VMEM),
        scratch_shapes=[
            pltpu.VMEM((EX, EY, CZ), F32),
            pltpu.VMEM((V, CX, CY, CZ), F32),
            pltpu.VMEM((V, EX, CY, CZ), F32),
            pltpu.VMEM((V, CX, CY, CZ), F32),
            pltpu.VMEM((V, CX, CY, CZ), F32),
            pltpu.VMEM((V, EX, 2 * CY, CZ), BF16),
            pltpu.VMEM((EX, EY, CZ), F32),
            pltpu.VMEM((2, R, EY, CZ), F32),
            pltpu.VMEM((2, CX, R, CZ), F32),
            pltpu.VMEM((V, 2 * R, CX * CY), F32),
            pltpu.VMEM((V, 2 * R, CX * CY), F32),
            pltpu.VMEM((V, 2 * R, CX * CY), F32),
            pltpu.VMEM((V, 2 * R, CX * CY), F32),
            pltpu.VMEM((3, 3, V, CZ), F32),
            pltpu.VMEM((1, V), jnp.int32),
            pltpu.VMEM((3, V, T), F32),
            pltpu.VMEM((3 + T, V, CZ), F32),
            pltpu.VMEM((V, 192, 256), BF16),
            pltpu.VMEM((V, 192, 256), BF16),
            pltpu.VMEM((V, 2 * CY, 256), BF16),
            pltpu.VMEM((3, V, 2 * CY, 256), BF16),
            pltpu.VMEM((3, V, 128, 256), BF16),
            pltpu.VMEM((V, CX, CY, CZ), F32),
            pltpu.VMEM((8, CZ), F32),
            pltpu.VMEM((2, 1, CZ), F32),
            pltpu.VMEM((2, 16, 1, CZ), F32),
            dma((4,)), dma((2,)), dma((2,)), dma((3, 2)), dma((3, 2)), dma((2, 2)), dma((2, 2)),
            dma((2, 2)), dma((2, 2)), dma((2, 2)), dma((2, 2)), dma((3, 2)), dma((3, 2)), dma((2,)), dma((2,)),
            dma((2,)), dma((2,)), pltpu.SemaphoreType.REGULAR,
        ],
        compiler_params=pltpu.CompilerParams(
            collective_id=0, has_side_effects=True, vmem_limit_bytes=48 * 1024 * 1024
        ),
    )(*[pltpu.with_memory_space_constraint(a, pltpu.HBM) for a in arrays])


def solution(mesh):
    block = P("bx", "by", "bz")
    views = P(None, "bx", "by", "bz")
    return jax.shard_map(
        on_device, mesh=mesh, in_specs=(block, views, views, P()), out_specs=block, check_vma=False
    )
```

```python
import functools

import jax
import jax.numpy as jnp
from jax import lax
from jax.experimental import pallas as pl
from jax.experimental.pallas import tpu as pltpu
from jax.sharding import PartitionSpec as P

MESH = pl.DeviceIdType.MESH
F32 = jnp.float32
BF16 = jnp.bfloat16
V, R, T = 8, 8, 17
CX, CY, CZ = 16, 16, 128
EX, EY = CX + 2 * R, CY + 2 * R
G = 4
LINES = (("bz", 4), ("by", 8), ("bx", 4))
STAGES = (8, 16)
SIDES = tuple((x, y) for x in (-1, 0, 1) for y in (-1, 0, 1) if x or y)
ROUNDS = (
    (("bz", 1), ("by", 1), ("bx", 1)),
    (("bz", 1), ("by", 1), ("bx", 1)),
    (("bz", 2), ("by", 2), ("bx", 2)),
    (("bz", 2), ("by", 4), ("bx", 2)),
)


def split(f):
    hi = f.astype(BF16)
    lo = (f - hi.astype(F32)).astype(BF16)
    return hi, lo


def dot(a, b):
    return jnp.dot(a, b, preferred_element_type=F32)


def stack4(f):
    hi, lo = split(f)
    return jnp.concatenate([hi, lo, hi, lo], axis=0)


def kernel(
    est, obs, cov, taps, out,
    e_buf, o_buf, y_buf, m_buf, g_buf, r_buf, x_buf, p_buf, rp_buf,
    zt_buf, h_buf, ht_buf, sb_buf, hb_buf, c_buf, k_buf, t_buf, l_buf,
    zf_mat, zb_mat, yf_mat, yw_mat, yb_mat, b_buf, seen_buf, red_own, red_in,
    load_sem, e_send, e_recv, f_send, f_recv, h_send, h_recv,
    zb_send, zb_recv, p_send, p_recv, red_send, red_recv, met_sem,
):
    ids = {name: lax.axis_index(name) for name, _ in LINES}
    sizes = dict(LINES)

    def at(dx, dy, dz=0):
        return {
            name: lax.rem(ids[name] + d + sizes[name], sizes[name])
            for name, d in (("bx", dx), ("by", dy), ("bz", dz)) if d
        }

    barrier = pltpu.get_barrier_semaphore()

    def has(name, d):
        return ids[name] + d >= 0 if d < 0 else ids[name] + d < sizes[name]

    def meet(sem, steps):
        for name, size in steps:
            for d in (-size, size):
                @pl.when(has(name, d))
                def _():
                    pl.semaphore_signal(
                        sem, inc=1, device_id={name: ids[name] + d}, device_id_type=MESH
                    )

    def met(sem, steps):
        heard = 0
        for name, size in steps:
            for d in (-size, size):
                heard = heard + jnp.where(has(name, d), 1, 0)
        pl.semaphore_wait(sem, heard)

    meet(barrier, ROUNDS[0])
    load_e = pltpu.make_async_copy(est, e_buf.at[pl.ds(R, CX), pl.ds(R, CY)], load_sem.at[0])
    load_c = pltpu.make_async_copy(cov, c_buf, load_sem.at[1])
    load_t = pltpu.make_async_copy(taps, k_buf, load_sem.at[2])
    load_o = pltpu.make_async_copy(obs, o_buf, load_sem.at[3])
    for load in (load_e, load_c, load_t, load_o):
        load.start()

    def both(dx, dy):
        if dx and dy:
            return jnp.logical_and(has("bx", dx), has("by", dy))
        return has("bx", dx) if dx else has("by", dy)

    def remote(src, dst, send, recv, device):
        return pltpu.make_async_remote_copy(
            src_ref=src, dst_ref=dst, send_sem=send, recv_sem=recv,
            device_id=device, device_id_type=MESH,
        )

    own = pl.ds(R, CX)
    edge = {-1: pl.ds(0, R), 0: own, 1: pl.ds(EX - R, R)}
    inner = {-1: pl.ds(R, R), 0: own, 1: pl.ds(CX, R)}

    def slot(dx, dy):
        return 3 * (dx + 1) + dy + 1

    def e_copy(dx, dy):
        return remote(
            e_buf.at[inner[dx], inner[dy]], e_buf.at[edge[-dx], edge[-dy]],
            e_send.at[slot(dx, dy)], e_recv.at[slot(-dx, -dy)], at(dx, dy),
        )

    def p_copy(dx, dy):
        return remote(
            p_buf.at[edge[dx], edge[dy]], rp_buf.at[edge[-dx], edge[-dy]],
            p_send.at[slot(dx, dy)], p_recv.at[slot(-dx, -dy)], at(dx, dy),
        )

    rows = {-1: pl.ds(R, R), 1: pl.ds(0, R)}

    def face_copy(dz):
        return remote(
            zt_buf.at[:, rows[dz]], h_buf.at[pl.ds(1, 2), 1, rows[-dz]],
            f_send.at[(1 + dz) // 2], f_recv.at[(1 - dz) // 2], at(0, 0, dz),
        )

    def h_copy(dx, dy):
        src = {-1: pl.ds(1, 1), 0: pl.ds(1, 2), 1: pl.ds(2, 1)}[dx]
        dst = {-1: pl.ds(3, 1), 0: pl.ds(1, 2), 1: pl.ds(0, 1)}[dx]
        return remote(
            h_buf.at[src, 1], h_buf.at[dst, 1 - dy],
            h_send.at[slot(dx, dy)], h_recv.at[slot(-dx, -dy)], at(dx, dy),
        )

    def weight(xb, yb):
        return h_buf[(0, 1, 3)[xb], yb, 2 * R:]

    def z_copy(g, dz):
        views = pl.ds(G * g, G)
        side = (dz + 1) // 2
        return remote(
            sb_buf.at[views, rows[dz]], hb_buf.at[views, rows[-dz]],
            zb_send.at[g, side], zb_recv.at[g, 1 - side], at(0, 0, dz),
        )

    part = functools.partial

    for d in (-1, 1):
        @pl.when(jnp.logical_not(has("by", d)))
        def _():
            e_buf[:, edge[d], :] = jnp.zeros((EX, R, CZ), F32)
            rp_buf[:, edge[d], :] = jnp.zeros((EX, R, CZ), F32)
            h_buf[:, 1 + d] = jnp.zeros((4, 3 * R, CZ), F32)

        @pl.when(jnp.logical_not(has("bx", d)))
        def _():
            e_buf[edge[d]] = jnp.zeros((R, EY, CZ), F32)
            rp_buf[edge[d]] = jnp.zeros((R, EY, CZ), F32)
            h_buf[3 * (1 + d) // 2] = jnp.zeros((3, 3 * R, CZ), F32)

        @pl.when(jnp.logical_not(has("bz", d)))
        def _():
            hb_buf[:, rows[d], :] = jnp.zeros((V, R, CX * CY), F32)
            h_buf[1:3, 1, rows[d], :] = jnp.zeros((2, R, CZ), F32)

    row8 = lax.broadcasted_iota(jnp.int32, (V, CZ), 0)
    lane8 = lax.broadcasted_iota(jnp.int32, (V, CZ), 1)
    load_c.wait()
    flags = jnp.broadcast_to(c_buf[...].astype(F32), (V, V))
    picked = jnp.where(row8[:, :V] == lane8[:, :V], flags, 0.0)
    for b in (1, 2):
        h_buf[b, 1, 2 * R:] = jnp.broadcast_to(jnp.sum(picked, axis=1, keepdims=True), (V, CZ))
    load_e.wait()
    planes = e_buf[own, own].reshape(CX * CY, CZ)
    for h in range(2):
        flipped = planes[128 * h:128 * h + 128].T
        zt_buf[h, 0:R] = flipped[CZ - R:]
        zt_buf[h, R:2 * R] = flipped[:R]
    met(barrier, ROUNDS[0])
    meet(met_sem.at[0], ROUNDS[1])
    for d in (-1, 1):
        @pl.when(has("bz", d))
        def _():
            face_copy(d).start()
    for d in (-1, 1):
        @pl.when(has("bx", d))
        def _():
            e_copy(d, 0).start()
    for d in (-1, 1):
        @pl.when(has("by", d))
        def _():
            e_copy(0, d).start()

    load_t.wait()
    t_buf[...] = jnp.zeros_like(t_buf)
    for d in range(3):
        t_buf[d, 0:V, 0:T] = k_buf[d]
    taps_x, taps_y, taps_z = (
        t_buf[d, 0:V] / jnp.sum(t_buf[d, 0:V], axis=1, keepdims=True) for d in range(3)
    )
    for k, table in enumerate((taps_x, taps_y)):
        wide = jnp.concatenate(
            [jnp.broadcast_to(table[v:v + 1], (2 * R, CZ)) for v in range(V)], axis=0
        ).T
        l_buf[k] = wide[:4 * R]
    taps_y = taps_y + pltpu.roll(taps_y, 32, 1)
    taps_y = taps_y + pltpu.roll(taps_y, 64, 1)
    band = lax.broadcasted_iota(jnp.int32, (CY, 128), 1)
    bands = []
    for v in range(V):
        q = pltpu.roll(
            jnp.broadcast_to(taps_y[v:v + 1], (CY, 128)), 0, 1, stride=1, stride_axis=0
        )
        bands.append(q)
        q_hi, q_lo = split(q)
        zero = jnp.zeros_like(q_hi)
        for x in range(2):
            mine = (band // 32) % 2 == x
            yf_mat[v, x * CY:(x + 1) * CY, 0:128] = jnp.where(mine, q_hi, zero)
            yf_mat[v, x * CY:(x + 1) * CY, 128:256] = jnp.where(mine, q_lo, zero)
    for k in range(T):
        t_buf[3 + k, 0:V] = jnp.broadcast_to(taps_x[:, k:k + 1], (V, CZ))
        t_buf[3 + k, V:2 * V] = jnp.broadcast_to(l_buf[0, k:k + 1], (V, CZ))

    lane = lax.broadcasted_iota(jnp.int32, (128, 128), 1)
    row = lax.broadcasted_iota(jnp.int32, (128, 128), 0)
    near = jnp.abs(row - lane) <= R
    zf_mat[:, 128:256, :] = jnp.zeros((V, 128, 256), BF16)
    zb_mat[:, 128:192, :] = jnp.zeros((V, 64, 256), BF16)
    for v in range(V):
        ring = pltpu.roll(
            jnp.broadcast_to(taps_z[v:v + 1], (128, 128)), 128 - R, 1, stride=1, stride_axis=0
        )
        for mat, full in ((zb_mat, ring), (zf_mat, ring.T)):
            m_hi, m_lo = split(jnp.where(near, full, 0.0))
            mat[v, 0:128, 0:128] = m_hi
            mat[v, 0:128, 128:256] = m_lo
            far = jnp.where(near, 0.0, full)
            far = jnp.concatenate([far[0:R], far[128 - R:128]], axis=0)
            f_hi, f_lo = split(far)
            top = 128 + 2 * R * (v if mat is zf_mat else v % G)
            mat[v, top:top + 2 * R, 0:128] = f_hi
            mat[v, top:top + 2 * R, 128:256] = f_lo

    load_o.wait()
    seen = jnp.zeros((8, CZ), F32)
    for v in range(V):
        seen = seen + weight(1, 1)[v:v + 1] * jnp.sum(o_buf[v].reshape(CX * CY // 8, 8, CZ), axis=0)
    count_own = jnp.sum(weight(1, 1), axis=0, keepdims=True)
    seen_buf[...] = seen / count_own

    met(met_sem.at[0], ROUNDS[1])
    meet(met_sem.at[1], ROUNDS[2])
    for dx in (-1, 1):
        for dy in (-1, 1):
            @pl.when(both(dx, dy))
            def _():
                e_copy(dx, dy).start()
    for d in (-1, 1):
        @pl.when(has("bz", d))
        def _():
            face_copy(-d).wait_recv()
    for dx, dy in SIDES:
        @pl.when(both(dx, dy))
        def _():
            h_copy(dx, dy).start()
    for d in (-1, 1):
        @pl.when(has("by", d))
        def _():
            e_copy(0, -d).wait_recv()

    def forward_y(x0, source=e_buf, mat=yf_mat, to=y_buf):
        data = jnp.concatenate(
            [stack4(source[pl.ds(x0 + 2 * h, 2)].reshape(2 * EY, CZ)) for h in range(2)], axis=1
        )
        full = dot(mat[...].reshape(V * 2 * CY, 256), data)
        for h in range(2):
            to[0:V, pl.ds(x0 + 2 * h, 2)] = full[:, h * CZ:(h + 1) * CZ].reshape(V, 2, CY, CZ)

    for x0 in range(R, R + CX, 4):
        forward_y(x0)

    def x_taps(v):
        return [jnp.broadcast_to(t_buf[3 + k, pl.ds(v, 1), :], (8, CZ)) for k in range(T)]

    def forward_x(inputs, first, y_buf, g_buf, v, carry):
        t = x_taps(v)
        for h in range(CY // 8):
            ys = pl.ds(8 * h, 8)
            acc = [None if first else g_buf[v, xo, ys, :] for xo in range(CX)]
            for xi in inputs:
                val = y_buf[v, xi, ys, :]
                for xo in range(max(0, xi - T + 1), min(CX, xi + 1)):
                    term = t[xi - xo] * val
                    acc[xo] = term if acc[xo] is None else acc[xo] + term
            for xo in range(CX):
                g_buf[v, xo, ys, :] = acc[xo]
        return carry

    def halo_y(b):
        for yb, rows, ys in ((0, slice(R, CY), slice(0, R)), (1, slice(0, CY), slice(R, R + CY)),
                             (2, slice(0, R), slice(R + CY, EY))):
            tile = jnp.concatenate([h_buf[b, yb, :2 * R]] * V, axis=0).T.reshape(R, CY, CZ)
            ht_buf[R * b:R * b + R, ys] = tile[:, rows]

        t = [jnp.broadcast_to(l_buf[1, k:k + 1, :], (8, CZ)) for k in range(T)]
        for x in range(R * b, R * b + R):
            for h in range(2):
                acc = None
                for k in range(T):
                    term = t[k] * ht_buf[x, 8 * h + k:8 * h + k + 8, :]
                    acc = term if acc is None else acc + term
                y_buf[V, x, 8 * h:8 * h + 8, :] = acc

    third = (band % 32)[:8]
    spans = ((0, R), (R, R + CX), (R + CX, EX))

    def mask(xb):
        xs = slice(*spans[xb])
        for yb in range(3):
            ys = slice(*spans[yb])
            count = jnp.maximum(jnp.sum(weight(xb, yb), axis=0, keepdims=True), 1.0)
            p_buf[xs, ys] = e_buf[xs, ys] * (1.0 / count)
        w = jnp.where(third < R, weight(xb, 0), jnp.where(third < R + CY, weight(xb, 1), weight(xb, 2)))
        for v in range(V):
            wide = jnp.broadcast_to(w[v:v + 1], (2 * CY, CZ)).astype(BF16)
            for i in range(2):
                cols = slice(128 * i, 128 * i + 128)
                yw_mat[xb, v, :, cols] = yf_mat[v, :, cols] * wide

    own_planes = range(R, R + CX)
    lax.fori_loop(0, V, part(forward_x, own_planes, True, y_buf, g_buf), 0)
    met(met_sem.at[1], ROUNDS[2])
    meet(met_sem.at[2], ROUNDS[3])
    for d in (-1, 1):
        @pl.when(has("by", d))
        def _():
            h_copy(0, -d).wait_recv()
    halo_y(1)
    halo_y(2)
    forward_x(own_planes, True, y_buf, g_buf, V, 0)
    mask(1)
    for x0 in range(R, R + CX, 4):
        forward_y(x0, p_buf, yw_mat.at[1], m_buf)
    for dx, dy in SIDES:
        if dx:
            @pl.when(both(dx, dy))
            def _():
                e_copy(-dx, -dy).wait_recv()
                h_copy(-dx, -dy).wait_recv()
    for x0 in (0, 4, EX - 8, EX - 4):
        forward_y(x0)
    halo_y(0)
    halo_y(3)
    halo_planes = tuple(range(R)) + tuple(range(R + CX, EX))
    lax.fori_loop(0, V + 1, part(forward_x, halo_planes, False, y_buf, g_buf), 0)

    def send_edges(fields, g):
        for v, f in zip(range(G * g, G * g + G), fields):
            for h in range(2):
                flipped = f[128 * h:128 * h + 128].T
                sb_buf[v, 0:R, 128 * h:128 * h + 128] = flipped[CZ - R:]
                sb_buf[v, R:2 * R, 128 * h:128 * h + 128] = flipped[:R]
        for d in (-1, 1):
            @pl.when(has("bz", d))
            def _():
                z_copy(g, d).start()

    def halo_rows(g):
        flat = hb_buf[G * g:G * g + G].reshape(G * 2 * R, CX * CY)
        return split(jnp.concatenate([flat[:, :128].T, flat[:, 128:].T], axis=0))

    def z_apply(f, halo, mat, v):
        hi, lo = split(f)
        both = dot(jnp.concatenate([hi, halo[0]], axis=1), mat[v])
        rest = dot(jnp.concatenate([lo, halo[1]], axis=1), mat[v, :, 0:128])
        return both[:, :128] + both[:, 128:] + rest

    halo = split(g_buf[V].reshape(CX * CY, CZ))
    for g in range(V // G):
        ratios = []
        for v in range(G * g, G * g + G):
            blurred = z_apply(g_buf[v].reshape(CX * CY, CZ), halo, zf_mat, v)
            ratio = o_buf[v].reshape(CX * CY, CZ) / blurred
            r_buf[v] = ratio.reshape(CX, CY, CZ)
            ratios.append(ratio)
        send_edges(ratios, g)

    for xb, x0s in ((0, (0, 4)), (2, (EX - 8, EX - 4))):
        mask(xb)
        for x0 in x0s:
            forward_y(x0, p_buf, yw_mat.at[xb], m_buf)
    lax.fori_loop(0, V, part(forward_x, range(EX), True, m_buf, b_buf), 0)

    for v in range(V):
        q4 = jnp.concatenate(
            [jnp.where(band // 32 == i // 2, bands[v], 0.0) for i in range(8)], axis=0
        ).T
        pair = split(q4)
        for xb in range(3):
            w = [jnp.broadcast_to(weight(xb, yb)[v:v + 1], (8, CZ)) for yb in (0, 1, 1, 2)]
            w = jnp.concatenate(w * 4, axis=0).astype(BF16)
            for i in range(2):
                yb_mat[xb, v, :, 128 * i:128 * i + 128] = pair[i] * w

    def backward_x(outputs, v, carry):
        t = x_taps(v)
        for xo in outputs:
            accs = []
            for h in range(CY // 8):
                ys = pl.ds(8 * h, 8)
                acc = None
                for xi in range(max(0, xo - T + 1), min(CX, xo + 1)):
                    term = t[xo - xi] * g_buf[v, xi, ys, :]
                    acc = term if acc is None else acc + term
                accs.append(acc)
            hi, lo = split(jnp.concatenate(accs, axis=0))
            x_buf[v, xo, 0:CY, :] = hi
            x_buf[v, xo, CY:2 * CY, :] = lo
        return carry

    total = jnp.zeros((8, CZ), F32)
    for g in range(V // G):
        for d in (-1, 1):
            @pl.when(has("bz", d))
            def _():
                z_copy(g, -d).wait_recv()
        halo = halo_rows(g)
        for v in range(G * g, G * g + G):
            f = z_apply(r_buf[v].reshape(CX * CY, CZ), halo, zb_mat, v)
            g_buf[v] = f.reshape(CX, CY, CZ)
            weighed = f * b_buf[v].reshape(CX * CY, CZ)
            total = total + jnp.sum(weighed.reshape(CX * CY // 8, 8, CZ), axis=0)

    lane1 = lax.broadcasted_iota(jnp.int32, (1, CZ), 1)

    def summed(f):
        return jnp.sum(jnp.sum(f, axis=0, keepdims=True), axis=1, keepdims=True)

    red_own[0] = jnp.where(lane1 < CZ // 2, summed(seen_buf[...]), summed(total))

    by_hi, by_lo = lax.div(ids["by"], 4), lax.rem(ids["by"], 4)

    def red_peer(stage, d):
        if stage == 0:
            return {
                "bx": lax.rem(ids["bx"] + d % 4, 4),
                "by": lax.rem(by_hi + d // 4, 2) * 4 + by_lo,
            }
        return {
            "bz": lax.rem(ids["bz"] + d % 4, 4),
            "by": by_hi * 4 + lax.rem(by_lo + d // 4, 4),
        }

    def red_copy(stage, d):
        return pltpu.make_async_remote_copy(
            src_ref=red_own.at[stage], dst_ref=red_in.at[stage, d],
            send_sem=red_send.at[stage], recv_sem=red_recv.at[stage],
            device_id=red_peer(stage, d), device_id_type=MESH,
        )

    def red_start(stage):
        for d in range(1, STAGES[stage]):
            red_copy(stage, d).start()

    def red_all(stage):
        every = red_in.at[stage, pl.ds(1, STAGES[stage] - 1)]
        return pltpu.make_async_remote_copy(
            src_ref=every, dst_ref=every, send_sem=red_send.at[stage],
            recv_sem=red_recv.at[stage], device_id=red_peer(stage, 1), device_id_type=MESH,
        )

    def red_finish(stage):
        red_all(stage).wait_recv()
        total = red_own[stage]
        for d in range(1, STAGES[stage]):
            total = total + red_in[stage, d]
        return total

    met(met_sem.at[2], ROUNDS[3])
    red_start(0)
    lax.fori_loop(0, V, part(backward_x, halo_planes), 0)

    def backward_y(x0, xb):
        full = None
        for v in range(V):
            data = []
            for h in range(2):
                planes = x_buf[v, x0 + 4 * h:x0 + 4 * h + 4].reshape(128, CZ)
                data.append(jnp.concatenate([planes, planes], axis=0))
            term = dot(yb_mat[xb, v], jnp.concatenate(data, axis=1))
            full = term if full is None else full + term
        for h in range(2):
            p_buf[x0 + 4 * h:x0 + 4 * h + 4] = full[:, h * CZ:(h + 1) * CZ].reshape(4, EY, CZ)

    backward_y(0, 0)
    backward_y(EX - 8, 2)
    for dx in (-1, 1):
        @pl.when(has("bx", dx))
        def _():
            p_copy(dx, 0).start()
        for dy in (-1, 1):
            @pl.when(both(dx, dy))
            def _():
                p_copy(dx, dy).start()
    lax.fori_loop(0, V, part(backward_x, range(R, R + CX)), 0)
    backward_y(R, 1)
    backward_y(2 * R, 1)
    for d in (-1, 1):
        @pl.when(has("by", d))
        def _():
            p_copy(0, d).start()
    red_own[1] = red_finish(0)
    red_start(1)
    for dx, dy in SIDES:
        @pl.when(both(dx, dy))
        def _():
            p_copy(-dx, -dy).wait_recv()
    for s in range(2):
        xs, xe = slice(R + 8 * s, R + 8 * s + 8), edge[2 * s - 1]
        for h in range(2):
            ys, ye = slice(R + 8 * h, R + 8 * h + 8), edge[2 * h - 1]
            summed = p_buf[xs, ys] + rp_buf[xe, ys] + rp_buf[xs, ye] + rp_buf[xe, ye]
            out[8 * s:8 * s + 8, 8 * h:8 * h + 8, :] = e_buf[xs, ys, :] * summed
    for dx, dy in SIDES:
        @pl.when(both(dx, dy))
        def _():
            e_copy(dx, dy).wait_send()
            p_copy(dx, dy).wait_send()
            h_copy(dx, dy).wait_send()
    for d in (-1, 1):
        @pl.when(has("bz", d))
        def _():
            face_copy(d).wait_send()
            for g in range(V // G):
                z_copy(g, d).wait_send()
    red_all(0).wait_send()
    red_all(1).wait_send()
    final = red_finish(1)
    scale = final[:, 0:1] / (final[:, CZ // 2:CZ // 2 + 1] * count_own[:, 0:1])
    out[...] = out[...] * scale.reshape(1, 1, 1)


def on_device(estimate, observed, coverage, psf_taps):
    dma = pltpu.SemaphoreType.DMA
    arrays = (estimate, observed, coverage.reshape(1, V), jnp.transpose(psf_taps, (1, 0, 2)))
    return pl.pallas_call(
        kernel,
        out_shape=jax.ShapeDtypeStruct((CX, CY, CZ), F32),
        in_specs=[pl.BlockSpec(memory_space=pltpu.HBM)] * 4,
        out_specs=pl.BlockSpec(memory_space=pltpu.VMEM),
        scratch_shapes=[
            pltpu.VMEM((EX, EY, CZ), F32),
            pltpu.VMEM((V, CX, CY, CZ), F32),
            pltpu.VMEM((V + 1, EX, CY, CZ), F32),
            pltpu.VMEM((V, EX, CY, CZ), F32),
            pltpu.VMEM((V + 1, CX, CY, CZ), F32),
            pltpu.VMEM((V, CX, CY, CZ), F32),
            pltpu.VMEM((V, EX, 2 * CY, CZ), BF16),
            pltpu.VMEM((EX, EY, CZ), F32),
            pltpu.VMEM((EX, EY, CZ), F32),
            pltpu.VMEM((2, 2 * R, CZ), F32),
            pltpu.VMEM((4, 3, 3 * R, CZ), F32),
            pltpu.VMEM((EX, EY, CZ), F32),
            pltpu.VMEM((V, 2 * R, CX * CY), F32),
            pltpu.VMEM((V, 2 * R, CX * CY), F32),
            pltpu.VMEM((1, V), jnp.int32),
            pltpu.VMEM((3, V, T), F32),
            pltpu.VMEM((3 + T, 2 * V, CZ), F32),
            pltpu.VMEM((2, 4 * R, CZ), F32),
            pltpu.VMEM((V, 256, 256), BF16),
            pltpu.VMEM((V, 192, 256), BF16),
            pltpu.VMEM((V, 2 * CY, 256), BF16),
            pltpu.VMEM((3, V, 2 * CY, 256), BF16),
            pltpu.VMEM((3, V, 128, 256), BF16),
            pltpu.VMEM((V, CX, CY, CZ), F32),
            pltpu.VMEM((8, CZ), F32),
            pltpu.VMEM((2, 1, CZ), F32),
            pltpu.VMEM((2, 16, 1, CZ), F32),
            dma((4,)), dma((9,)), dma((9,)), dma((2,)), dma((2,)), dma((9,)), dma((9,)),
            dma((2, 2)), dma((2, 2)), dma((9,)), dma((9,)), dma((2,)), dma((2,)),
            pltpu.SemaphoreType.REGULAR((3,)),
        ],
        compiler_params=pltpu.CompilerParams(
            collective_id=0, has_side_effects=True, vmem_limit_bytes=48 * 1024 * 1024
        ),
    )(*[pltpu.with_memory_space_constraint(a, pltpu.HBM) for a in arrays])


def solution(mesh):
    block = P("bx", "by", "bz")
    views = P(None, "bx", "by", "bz")
    return jax.shard_map(
        on_device, mesh=mesh, in_specs=(block, views, views, P()), out_specs=block, check_vma=False
    )
```

```python
import functools

import jax
import jax.numpy as jnp
from jax import lax
from jax.experimental import pallas as pl
from jax.experimental.pallas import tpu as pltpu
from jax.sharding import PartitionSpec as P

MESH = pl.DeviceIdType.MESH
F32 = jnp.float32
BF16 = jnp.bfloat16
V, R, T = 8, 8, 17
CX, CY, CZ = 16, 16, 128
EX, EY = CX + 2 * R, CY + 2 * R
G = 4
LINES = (("bz", 4), ("by", 8), ("bx", 4))
STAGES = (8, 16)
SIDES = tuple((x, y) for x in (-1, 0, 1) for y in (-1, 0, 1) if x or y)
ROUNDS = (
    (("bz", 1), ("by", 1), ("bx", 1)),
    (("bz", 1), ("by", 1), ("bx", 1)),
    (("bz", 2), ("by", 2), ("bx", 2)),
    (("bz", 2), ("by", 4), ("bx", 2)),
)


def split(f):
    hi = f.astype(BF16)
    lo = (f - hi.astype(F32)).astype(BF16)
    return hi, lo


def dot(a, b):
    return jnp.dot(a, b, preferred_element_type=F32)


def stack4(f):
    hi, lo = split(f)
    return jnp.concatenate([hi, lo, hi, lo], axis=0)


def kernel(
    est, obs, cov, taps, out,
    e_buf, o_buf, y_buf, m_buf, g_buf, r_buf, x_buf, p_buf, rp_buf, tp_buf,
    zt_buf, share_buf, h_buf, ht_buf, sb_buf, hb_buf, w_buf, c_buf, k_buf, t_buf, l_buf,
    zf_mat, zm_mat, zh_mat, yf_mat, yw_mat, yb_mat, b_buf, seen_buf, red_own, red_in,
    load_sem, e_send, e_recv, w_send, w_recv, f_send, f_recv, h_send, h_recv,
    zb_send, zb_recv, p_send, p_recv, red_send, red_recv, met_sem,
):
    ids = {name: lax.axis_index(name) for name, _ in LINES}
    sizes = dict(LINES)

    def at(dx, dy, dz=0):
        return {
            name: lax.rem(ids[name] + d + sizes[name], sizes[name])
            for name, d in (("bx", dx), ("by", dy), ("bz", dz)) if d
        }

    barrier = pltpu.get_barrier_semaphore()

    def has(name, d):
        return ids[name] + d >= 0 if d < 0 else ids[name] + d < sizes[name]

    def meet(sem, steps):
        for name, size in steps:
            for d in (-size, size):
                @pl.when(has(name, d))
                def _():
                    pl.semaphore_signal(
                        sem, inc=1, device_id={name: ids[name] + d}, device_id_type=MESH
                    )

    def met(sem, steps, heard=0):
        for name, size in steps:
            for d in (-size, size):
                heard = heard + jnp.where(has(name, d), 1, 0)
        pl.semaphore_wait(sem, heard)

    def twin(dx):
        return lax.rem(ids["bx"], 2) == (1 - dx) // 2

    def cross(dx):
        return jnp.logical_and(has("bx", dx), jnp.logical_not(twin(dx)))

    def cross_both(dx, dy):
        return jnp.logical_and(cross(dx), has("by", dy))

    corners = [(dx, dy) for dx in (-1, 1) for dy in (-1, 1)]
    meet(barrier, ROUNDS[0])
    greeted = 0
    for dx, dy in corners:
        near_by = jnp.logical_and(has("bx", dx), has("by", dy))
        greeted = greeted + jnp.where(near_by, 1, 0)

        @pl.when(near_by)
        def _():
            pl.semaphore_signal(barrier, inc=1, device_id=at(dx, dy), device_id_type=MESH)
    load_e = pltpu.make_async_copy(est, e_buf.at[pl.ds(R, CX), pl.ds(R, CY)], load_sem.at[0])
    load_c = pltpu.make_async_copy(cov, c_buf, load_sem.at[1])
    load_t = pltpu.make_async_copy(taps, k_buf, load_sem.at[2])
    load_o = pltpu.make_async_copy(obs, o_buf, load_sem.at[3])
    for load in (load_e, load_c, load_t, load_o):
        load.start()

    def both(dx, dy):
        if dx and dy:
            return jnp.logical_and(has("bx", dx), has("by", dy))
        return has("bx", dx) if dx else has("by", dy)

    def remote(src, dst, send, recv, device):
        return pltpu.make_async_remote_copy(
            src_ref=src, dst_ref=dst, send_sem=send, recv_sem=recv,
            device_id=device, device_id_type=MESH,
        )

    own = pl.ds(R, CX)
    edge = {-1: pl.ds(0, R), 0: own, 1: pl.ds(EX - R, R)}
    inner = {-1: pl.ds(R, R), 0: own, 1: pl.ds(CX, R)}

    def counted(act):
        ends = [
            jnp.logical_and(has(name, -1), has(name, 1)) for name in ("bx", "by")
        ]
        for nx in (1, 2):
            for ny in (1, 2):
                hit = [e if n == 2 else jnp.logical_not(e) for e, n in zip(ends, (nx, ny))]

                @pl.when(jnp.logical_and(*hit))
                def _():
                    act(nx, ny)

    def planes_of(buf, rows):
        width = 32 if rows % 32 == 0 else 24
        return buf.at[pl.ds(0, rows // width), pl.ds(0, width)]

    def group(ref, send, recv):
        return remote(ref, ref, send, recv, at(0, 0, 1))

    def e_copy(dx, dy):
        return remote(
            e_buf.at[inner[dx], inner[dy]], e_buf.at[edge[-dx], edge[-dy]],
            e_send.at[0], e_recv.at[0 if dx else (3 - dy) // 2], at(dx, dy),
        )

    def e_pass(dx, dy):
        return remote(
            e_buf.at[inner[dx], edge[dy]], e_buf.at[edge[-dx], edge[dy]],
            e_send.at[0], e_recv.at[0], at(dx, 0),
        )

    def p_copy(dx, dy):
        return remote(
            p_buf.at[edge[dx], edge[dy]], rp_buf.at[edge[-dx], edge[-dy]],
            p_send.at[0], p_recv.at[0], at(dx, dy),
        )

    def p_pass(dx):
        return remote(p_buf.at[edge[dx]], tp_buf, p_send.at[0], p_recv.at[1], at(dx, 0))

    rows = {-1: pl.ds(R, R), 1: pl.ds(0, R)}
    to_rows = {-1: pl.ds(R, R), 1: pl.ds(0, R)}

    def face_copy(dz):
        return remote(
            zt_buf.at[:, rows[dz]], h_buf.at[pl.ds(1, 2), 1, to_rows[dz]],
            f_send.at[(1 + dz) // 2], f_recv.at[(1 - dz) // 2], at(0, 0, dz),
        )

    def share_copy(dz):
        return remote(
            share_buf.at[2], share_buf.at[(1 - dz) // 2],
            f_send.at[2 + (1 + dz) // 2], f_recv.at[2 + (1 - dz) // 2], at(0, 0, dz),
        )

    def h_copy(dx, dy):
        src = {-1: pl.ds(1, 1), 0: pl.ds(1, 2), 1: pl.ds(2, 1)}[dx]
        dst = {-1: pl.ds(3, 1), 0: pl.ds(1, 2), 1: pl.ds(0, 1)}[dx]
        return remote(
            h_buf.at[src, 1], h_buf.at[dst, 1 - dy],
            h_send.at[0], h_recv.at[1 if dx else 0], at(dx, dy),
        )

    def w_copy(dx, dy):
        return remote(
            w_buf.at[1, 1], w_buf.at[1 - dx, 1 - dy],
            w_send.at[0], w_recv.at[1 if dx else 0], at(dx, dy),
        )

    def z_copy(g, dz):
        views = pl.ds(G * g, G)
        side = (dz + 1) // 2
        return remote(
            sb_buf.at[views, rows[dz]], hb_buf.at[views, rows[-dz]],
            zb_send.at[g, side], zb_recv.at[g, 1 - side], at(0, 0, dz),
        )

    part = functools.partial

    for d in (-1, 1):
        @pl.when(jnp.logical_not(has("by", d)))
        def _():
            e_buf[:, edge[d], :] = jnp.zeros((EX, R, CZ), F32)
            rp_buf[:, edge[d], :] = jnp.zeros((EX, R, CZ), F32)
            h_buf[:, 1 + d] = jnp.zeros((4, 3 * R, CZ), F32)
            w_buf[:, 1 + d] = jnp.zeros((3, V, CZ), F32)

        @pl.when(jnp.logical_not(has("bx", d)))
        def _():
            e_buf[edge[d]] = jnp.zeros((R, EY, CZ), F32)
            h_buf[3 * (1 + d) // 2] = jnp.zeros((3, 3 * R, CZ), F32)
            w_buf[1 + d] = jnp.zeros((3, V, CZ), F32)

        @pl.when(jnp.logical_not(cross(d)))
        def _():
            rp_buf[edge[d]] = jnp.zeros((R, EY, CZ), F32)

        @pl.when(jnp.logical_not(has("bz", d)))
        def _():
            hb_buf[:, rows[d], :] = jnp.zeros((V, R, CX * CY), F32)
            h_buf[1:3, 1, to_rows[-d], :] = jnp.zeros((2, R, CZ), F32)
            share_buf[(1 + d) // 2] = jnp.zeros((V, CZ), F32)

    row8 = lax.broadcasted_iota(jnp.int32, (V, CZ), 0)
    lane8 = lax.broadcasted_iota(jnp.int32, (V, CZ), 1)
    load_c.wait()
    flags = jnp.broadcast_to(c_buf[...].astype(F32), (V, V))
    picked = jnp.where(row8[:, :V] == lane8[:, :V], flags, 0.0)
    weight = jnp.broadcast_to(jnp.sum(picked, axis=1, keepdims=True), (V, CZ))
    w_buf[1, 1] = weight
    share_buf[2] = weight / jnp.sum(weight, axis=0, keepdims=True)
    load_e.wait()
    planes = e_buf[own, own].reshape(CX * CY, CZ)
    for h in range(2):
        flipped = planes[128 * h:128 * h + 128].T
        zt_buf[h, 0:R] = flipped[CZ - R:]
        zt_buf[h, R:2 * R] = flipped[:R]
    met(barrier, ROUNDS[0], greeted)
    meet(met_sem.at[0], ROUNDS[1])
    for d in (-1, 1):
        @pl.when(has("bz", d))
        def _():
            face_copy(d).start()
            share_copy(d).start()
    for dx, dy in SIDES:
        @pl.when(both(dx, dy))
        def _():
            w_copy(dx, dy).start()
    for d in (-1, 1):
        @pl.when(has("bx", d))
        def _():
            e_copy(d, 0).start()
    for d in (-1, 1):
        @pl.when(has("by", d))
        def _():
            e_copy(0, d).start()
    for dx, dy in corners:
        @pl.when(cross_both(dx, dy))
        def _():
            e_copy(dx, dy).start()

    load_t.wait()
    t_buf[...] = jnp.zeros_like(t_buf)
    for d in range(3):
        t_buf[d, 0:V, 0:T] = k_buf[d]
    taps_x, taps_y, taps_z = (
        t_buf[d, 0:V] / jnp.sum(t_buf[d, 0:V], axis=1, keepdims=True) for d in range(3)
    )
    for k, table in enumerate((taps_x, taps_y)):
        wide = jnp.concatenate(
            [jnp.broadcast_to(table[v:v + 1], (2 * R, CZ)) for v in range(V)], axis=0
        ).T
        l_buf[k] = wide[:4 * R]
    taps_y = taps_y + pltpu.roll(taps_y, 32, 1)
    taps_y = taps_y + pltpu.roll(taps_y, 64, 1)
    band = lax.broadcasted_iota(jnp.int32, (CY, 128), 1)
    bands = []
    for v in range(V):
        q = pltpu.roll(
            jnp.broadcast_to(taps_y[v:v + 1], (CY, 128)), 0, 1, stride=1, stride_axis=0
        )
        bands.append(q)
        q_hi, q_lo = split(q)
        zero = jnp.zeros_like(q_hi)
        for x in range(2):
            mine = (band // 32) % 2 == x
            yf_mat[v, x * CY:(x + 1) * CY, 0:128] = jnp.where(mine, q_hi, zero)
            yf_mat[v, x * CY:(x + 1) * CY, 128:256] = jnp.where(mine, q_lo, zero)
    for k in range(T):
        t_buf[3 + k, 0:V] = jnp.broadcast_to(taps_x[:, k:k + 1], (V, CZ))
        t_buf[3 + k, V:2 * V] = jnp.broadcast_to(l_buf[0, k:k + 1], (V, CZ))

    lane = lax.broadcasted_iota(jnp.int32, (128, 128), 1)
    row = lax.broadcasted_iota(jnp.int32, (128, 128), 0)
    near = jnp.abs(row - lane) <= R
    zf_mat[:, 128:256, :] = jnp.zeros((V, 128, 256), BF16)
    zh_mat[...] = jnp.zeros_like(zh_mat)
    for v in range(V):
        ring = pltpu.roll(
            jnp.broadcast_to(taps_z[v:v + 1], (128, 128)), 128 - R, 1, stride=1, stride_axis=0
        )
        ahead = ring.T
        m_hi, m_lo = split(jnp.where(near, ahead, 0.0))
        zf_mat[v, 0:128, 0:128] = m_hi
        zf_mat[v, 0:128, 128:256] = m_lo
        far = jnp.where(near, 0.0, ahead)
        f_hi, f_lo = split(jnp.concatenate([far[128 - R:128], far[0:R]], axis=0))
        top = 128 + 2 * R * v
        zf_mat[v, top:top + 2 * R, 0:128] = f_hi
        zf_mat[v, top:top + 2 * R, 128:256] = f_lo
        m_hi, m_lo = split(jnp.where(near, ring, 0.0))
        far = jnp.where(near, 0.0, ring)
        s_hi, s_lo = split(pltpu.roll(far, (2 * R * v + R) % 128, 1))
        for i in range(2):
            zm_mat[v, 128 * i:128 * i + 128, 0:128] = m_hi
            zm_mat[v, 128 * i:128 * i + 128, 128:256] = s_hi
        zm_mat[v, 256:384, 0:128] = m_lo
        zm_mat[v, 256:384, 128:256] = s_lo
        f_hi, f_lo = split(jnp.concatenate([far[0:R], far[128 - R:128]], axis=0))
        top = 2 * R * (v % G)
        zh_mat[v, top:top + 2 * R] = f_hi
        zh_mat[v, 64 + top:64 + top + 2 * R] = f_hi
        zh_mat[v, 128 + top:128 + top + 2 * R] = f_lo

    load_o.wait()
    seen = jnp.zeros((8, CZ), F32)
    for v in range(V):
        seen = seen + w_buf[1, 1, v:v + 1] * jnp.sum(o_buf[v].reshape(CX * CY // 8, 8, CZ), axis=0)
    count_own = jnp.sum(w_buf[1, 1], axis=0, keepdims=True)
    seen_buf[...] = seen / count_own

    for d in (-1, 1):
        @pl.when(has("bz", d))
        def _():
            face_copy(-d).wait_recv()
            share_copy(-d).wait_recv()
    for b in (1, 2):
        h_buf[b, 1, 2 * R:] = jnp.where(lane8 < CZ // 2, share_buf[0], share_buf[1])
    met(met_sem.at[0], ROUNDS[1])
    meet(met_sem.at[1], ROUNDS[2])
    for dx, dy in SIDES:
        @pl.when(both(dx, dy))
        def _():
            h_copy(dx, dy).start()
    for d in (-1, 1):
        @pl.when(has("by", d))
        def _():
            e_copy(0, -d).wait_recv()
            for dx in (-1, 1):
                @pl.when(twin(dx))
                def _():
                    e_pass(dx, d).start()

    def forward_y(x0, source=e_buf, mat=yf_mat, to=y_buf):
        data = jnp.concatenate(
            [stack4(source[pl.ds(x0 + 2 * h, 2)].reshape(2 * EY, CZ)) for h in range(2)], axis=1
        )
        full = dot(mat[...].reshape(V * 2 * CY, 256), data)
        for h in range(2):
            to[0:V, pl.ds(x0 + 2 * h, 2)] = full[:, h * CZ:(h + 1) * CZ].reshape(V, 2, CY, CZ)

    for x0 in range(R, R + CX, 4):
        forward_y(x0)

    def x_taps(v):
        return [jnp.broadcast_to(t_buf[3 + k, pl.ds(v, 1), :], (8, CZ)) for k in range(T)]

    def forward_x(inputs, first, y_buf, g_buf, v, carry):
        t = x_taps(v)
        for h in range(CY // 8):
            ys = pl.ds(8 * h, 8)
            acc = [None if first else g_buf[v, xo, ys, :] for xo in range(CX)]
            for xi in inputs:
                val = y_buf[v, xi, ys, :]
                for xo in range(max(0, xi - T + 1), min(CX, xi + 1)):
                    term = t[xi - xo] * val
                    acc[xo] = term if acc[xo] is None else acc[xo] + term
            for xo in range(CX):
                g_buf[v, xo, ys, :] = acc[xo]
        return carry

    y_spans = ((0, slice(R, CY), slice(0, R)), (1, slice(0, CY), slice(R, R + CY)),
               (2, slice(0, R), slice(R + CY, EY)))

    def halo_in(b):
        for yb, part_of, ys in y_spans:
            tile = jnp.concatenate([h_buf[b, yb, :2 * R]] * V, axis=0).T.reshape(R, CY, CZ)
            ht_buf[R * b:R * b + R, ys] = tile[:, part_of]

    def halo_share(b):
        for yb, _, ys in y_spans:
            tile = h_buf[b, yb, 2 * R:]
            before = jnp.broadcast_to(tile[:, 0:1], (V, CZ))
            after = jnp.broadcast_to(tile[:, CZ // 2:CZ // 2 + 1], (V, CZ))
            share = jnp.where(lane8 % (2 * R) < R, before, after)
            share = jnp.sum(jnp.where(lane8 // (2 * R) == row8, share, 0.0), axis=0, keepdims=True)
            at_x = slice(R * b, R * b + R)
            ht_buf[at_x, ys] = ht_buf[at_x, ys] * share

    def halo_y(b, to):
        t = [jnp.broadcast_to(l_buf[1, k:k + 1, :], (8, CZ)) for k in range(T)]
        for x in range(R * b, R * b + R):
            for h in range(2):
                acc = None
                for k in range(T):
                    term = t[k] * ht_buf[x, 8 * h + k:8 * h + k + 8, :]
                    acc = term if acc is None else acc + term
                to[V, x, 8 * h:8 * h + 8, :] = acc

    third = (band % 32)[:8]
    spans = ((0, R), (R, R + CX), (R + CX, EX))

    def mask(xb):
        xs = slice(*spans[xb])
        for yb in range(3):
            ys = slice(*spans[yb])
            count = jnp.maximum(jnp.sum(w_buf[xb, yb], axis=0, keepdims=True), 1.0)
            p_buf[xs, ys] = e_buf[xs, ys] * (1.0 / count)
        w = jnp.where(third < R, w_buf[xb, 0], jnp.where(third < R + CY, w_buf[xb, 1], w_buf[xb, 2]))
        for v in range(V):
            wide = jnp.broadcast_to(w[v:v + 1], (2 * CY, CZ)).astype(BF16)
            for i in range(2):
                cols = slice(128 * i, 128 * i + 128)
                yw_mat[xb, v, :, cols] = yf_mat[v, :, cols] * wide

    own_planes = range(R, R + CX)
    lax.fori_loop(0, V, part(forward_x, own_planes, True, y_buf, g_buf), 0)
    halo_planes = tuple(range(R)) + tuple(range(R + CX, EX))

    def masked_y(xb):
        mask(xb)
        for x0 in range(spans[xb][0], spans[xb][1], 4):
            forward_y(x0, p_buf, yw_mat.at[xb], m_buf)

    def w_arrivals(nx, ny):
        group(w_buf.at[0, pl.ds(0, ny)], w_send.at[0], w_recv.at[0]).wait_recv()

    counted(w_arrivals)
    masked_y(1)
    lax.fori_loop(0, V, part(forward_x, own_planes, True, m_buf, b_buf), 0)
    def x_arrivals(nx, ny):
        group(planes_of(e_buf, nx * (128 + 64 * ny)), e_send.at[0], e_recv.at[0]).wait_recv()
        tiles = w_buf.at[pl.ds(0, nx), pl.ds(0, 3)] if ny == 2 else w_buf.at[pl.ds(0, 2), pl.ds(0, nx)]
        group(tiles, w_send.at[0], w_recv.at[1]).wait_recv()

    counted(x_arrivals)
    for x0 in (0, 4, EX - 8, EX - 4):
        forward_y(x0)
    lax.fori_loop(0, V, part(forward_x, halo_planes, False, y_buf, g_buf), 0)
    masked_y(0)
    masked_y(2)
    lax.fori_loop(0, V, part(forward_x, halo_planes, False, m_buf, b_buf), 0)
    met(met_sem.at[1], ROUNDS[2])
    meet(met_sem.at[2], ROUNDS[3])

    def h_arrivals(nx, ny):
        group(h_buf.at[pl.ds(0, 2 * ny), 0], h_send.at[0], h_recv.at[0]).wait_recv()
        blocks = {2: pl.ds(0, nx), 1: pl.ds(0, 2 * nx)}[ny]
        cols = pl.ds(0, 3) if ny == 2 else 0
        group(h_buf.at[blocks, cols], h_send.at[0], h_recv.at[1]).wait_recv()

    counted(h_arrivals)
    for b in range(4):
        halo_in(b)
    for b in range(4):
        halo_y(b, y_buf)
    forward_x(range(EX), True, y_buf, g_buf, V, 0)

    def send_edges(fields, g):
        for v, f in zip(range(G * g, G * g + G), fields):
            for h in range(2):
                flipped = f[128 * h:128 * h + 128].T
                sb_buf[v, 0:R, 128 * h:128 * h + 128] = flipped[CZ - R:]
                sb_buf[v, R:2 * R, 128 * h:128 * h + 128] = flipped[:R]
        for d in (-1, 1):
            @pl.when(has("bz", d))
            def _():
                z_copy(g, d).start()

    def halo_rows(g):
        flat = hb_buf[G * g:G * g + G].reshape(G * 2 * R, CX * CY)
        hi = flat.astype(BF16).astype(F32)
        pair = jnp.concatenate([hi, flat - hi], axis=0)
        pair = jnp.concatenate([pair[:, :128].T, pair[:, 128:].T], axis=0).astype(BF16)
        return jnp.concatenate([pair, pair[:, :64]], axis=1)

    def z_apply(f, halo, mat, v):
        hi, lo = split(f)
        both = dot(jnp.concatenate([hi, halo[0]], axis=1), mat[v])
        rest = dot(jnp.concatenate([lo, halo[1]], axis=1), mat[v, :, 0:128])
        return both[:, :128] + both[:, 128:] + rest

    halo = split(g_buf[V].reshape(CX * CY, CZ))
    for g in range(V // G):
        ratios = []
        for v in range(G * g, G * g + G):
            blurred = z_apply(g_buf[v].reshape(CX * CY, CZ), halo, zf_mat, v)
            ratio = o_buf[v].reshape(CX * CY, CZ) / blurred
            r_buf[v] = ratio.reshape(CX, CY, CZ)
            ratios.append(ratio)
        send_edges(ratios, g)

    total = jnp.zeros((8, CZ), F32)
    outside = jnp.zeros((CX * CY, CZ), F32)
    for v in range(V):
        hi, lo = split(r_buf[v].reshape(CX * CY, CZ))
        f = dot(jnp.concatenate([hi, lo], axis=1), zm_mat[v, 0:256]) + dot(hi, zm_mat[v, 256:384])
        g_buf[v] = f[:, :128].reshape(CX, CY, CZ)
        outside = outside + f[:, 128:]
        weighed = f[:, :128] * b_buf[v].reshape(CX * CY, CZ)
        total = total + jnp.sum(weighed.reshape(CX * CY // 8, 8, CZ), axis=0)
    for b in range(4):
        halo_share(b)
    for b in range(4):
        halo_y(b, m_buf)
    forward_x(range(EX), True, m_buf, b_buf, V, 0)
    weighed = outside * b_buf[V].reshape(CX * CY, CZ)
    total = total + jnp.sum(weighed.reshape(CX * CY // 8, 8, CZ), axis=0)
    lane1 = lax.broadcasted_iota(jnp.int32, (1, CZ), 1)

    def summed(f):
        return jnp.sum(jnp.sum(f, axis=0, keepdims=True), axis=1, keepdims=True)

    red_own[0] = jnp.where(lane1 < CZ // 2, summed(seen_buf[...]), summed(total))

    by_hi, by_lo = lax.div(ids["by"], 4), lax.rem(ids["by"], 4)

    def red_peer(stage, d):
        if stage == 0:
            return {
                "bx": lax.rem(ids["bx"] + d % 4, 4),
                "by": lax.rem(by_hi + d // 4, 2) * 4 + by_lo,
            }
        return {
            "bz": lax.rem(ids["bz"] + d % 4, 4),
            "by": by_hi * 4 + lax.rem(by_lo + d // 4, 4),
        }

    def red_copy(stage, d):
        return pltpu.make_async_remote_copy(
            src_ref=red_own.at[stage], dst_ref=red_in.at[stage, d],
            send_sem=red_send.at[stage], recv_sem=red_recv.at[stage],
            device_id=red_peer(stage, d), device_id_type=MESH,
        )

    def red_start(stage):
        for d in range(1, STAGES[stage]):
            red_copy(stage, d).start()

    def red_all(stage):
        every = red_in.at[stage, pl.ds(1, STAGES[stage] - 1)]
        return pltpu.make_async_remote_copy(
            src_ref=every, dst_ref=every, send_sem=red_send.at[stage],
            recv_sem=red_recv.at[stage], device_id=red_peer(stage, 1), device_id_type=MESH,
        )

    def red_finish(stage):
        red_all(stage).wait_recv()
        total = red_own[stage]
        for d in range(1, STAGES[stage]):
            total = total + red_in[stage, d]
        return total

    met(met_sem.at[2], ROUNDS[3])
    red_start(0)
    for v in range(V):
        q4 = jnp.concatenate(
            [jnp.where(band // 32 == i // 2, bands[v], 0.0) for i in range(8)], axis=0
        ).T
        pair = split(q4)
        for xb in range(3):
            w = [jnp.broadcast_to(w_buf[xb, yb, v:v + 1], (8, CZ)) for yb in (0, 1, 1, 2)]
            w = jnp.concatenate(w * 4, axis=0).astype(BF16)
            for i in range(2):
                yb_mat[xb, v, :, 128 * i:128 * i + 128] = pair[i] * w

    def backward_x(outputs, v, carry):
        t = x_taps(v)
        for xo in outputs:
            accs = []
            for h in range(CY // 8):
                ys = pl.ds(8 * h, 8)
                acc = None
                for xi in range(max(0, xo - T + 1), min(CX, xo + 1)):
                    term = t[xo - xi] * g_buf[v, xi, ys, :]
                    acc = term if acc is None else acc + term
                accs.append(acc)
            hi, lo = split(jnp.concatenate(accs, axis=0))
            x_buf[v, xo, 0:CY, :] = hi
            x_buf[v, xo, CY:2 * CY, :] = lo
        return carry

    for g in range(V // G):
        for d in (-1, 1):
            @pl.when(has("bz", d))
            def _():
                z_copy(g, -d).wait_recv()
        halo = halo_rows(g)
        for v in range(G * g, G * g + G):
            g_buf[v] = g_buf[v] + dot(halo, zh_mat[v]).reshape(CX, CY, CZ)

    lax.fori_loop(0, V, part(backward_x, halo_planes), 0)

    def backward_y(x0, xb):
        full = None
        for v in range(V):
            data = []
            for h in range(2):
                planes = x_buf[v, x0 + 4 * h:x0 + 4 * h + 4].reshape(128, CZ)
                data.append(jnp.concatenate([planes, planes], axis=0))
            term = dot(yb_mat[xb, v], jnp.concatenate(data, axis=1))
            full = term if full is None else full + term
        for h in range(2):
            p_buf[x0 + 4 * h:x0 + 4 * h + 4] = full[:, h * CZ:(h + 1) * CZ].reshape(4, EY, CZ)

    backward_y(0, 0)
    backward_y(EX - 8, 2)
    for dx in (-1, 1):
        @pl.when(twin(dx))
        def _():
            p_pass(dx).start()

        @pl.when(cross(dx))
        def _():
            p_copy(dx, 0).start()
        for dy in (-1, 1):
            @pl.when(cross_both(dx, dy))
            def _():
                p_copy(dx, dy).start()
    lax.fori_loop(0, V, part(backward_x, range(R, R + CX)), 0)
    backward_y(R, 1)
    backward_y(2 * R, 1)
    for dx in (-1, 1):
        @pl.when(twin(dx))
        def _():
            p_pass(dx).wait_recv()
            p_buf[inner[dx]] = p_buf[inner[dx]] + tp_buf[...]
    for d in (-1, 1):
        @pl.when(has("by", d))
        def _():
            p_copy(0, d).start()
    red_own[1] = red_finish(0)
    red_start(1)
    def p_arrivals(nx, ny):
        rows = 128 * ny + (128 + 64 * ny) * (nx - 1)
        group(planes_of(rp_buf, rows), p_send.at[0], p_recv.at[0]).wait_recv()

    counted(p_arrivals)
    for s in range(2):
        xs, xe = slice(R + 8 * s, R + 8 * s + 8), edge[2 * s - 1]
        for h in range(2):
            ys, ye = slice(R + 8 * h, R + 8 * h + 8), edge[2 * h - 1]
            summed = p_buf[xs, ys] + rp_buf[xe, ys] + rp_buf[xs, ye] + rp_buf[xe, ye]
            out[8 * s:8 * s + 8, 8 * h:8 * h + 8, :] = e_buf[xs, ys, :] * summed
    def departures(nx, ny):
        group(planes_of(e_buf, 128 * (nx + ny) + 64 * nx * ny), e_send.at[0], e_recv.at[0]).wait_send()
        blocks = 2 * ny + nx * (1 + ny)
        group(e_buf.at[pl.ds(0, blocks), pl.ds(0, 24)], h_send.at[0], h_recv.at[0]).wait_send()
        tiles = e_buf.at[pl.ds(0, nx + ny + nx * ny), pl.ds(0, V)]
        group(tiles, w_send.at[0], w_recv.at[0]).wait_send()
        rows = 256 + 128 * ny + (128 + 64 * ny) * (nx - 1)
        group(planes_of(e_buf, rows), p_send.at[0], p_recv.at[0]).wait_send()

    counted(departures)
    for d in (-1, 1):
        @pl.when(has("bz", d))
        def _():
            face_copy(d).wait_send()
            share_copy(d).wait_send()
            for g in range(V // G):
                z_copy(g, d).wait_send()
    red_all(0).wait_send()
    red_all(1).wait_send()
    final = red_finish(1)
    scale = final[:, 0:1] / (final[:, CZ // 2:CZ // 2 + 1] * count_own[:, 0:1])
    out[...] = out[...] * scale.reshape(1, 1, 1)


def on_device(estimate, observed, coverage, psf_taps):
    dma = pltpu.SemaphoreType.DMA
    arrays = (estimate, observed, coverage.reshape(1, V), jnp.transpose(psf_taps, (1, 0, 2)))
    return pl.pallas_call(
        kernel,
        out_shape=jax.ShapeDtypeStruct((CX, CY, CZ), F32),
        in_specs=[pl.BlockSpec(memory_space=pltpu.HBM)] * 4,
        out_specs=pl.BlockSpec(memory_space=pltpu.VMEM),
        scratch_shapes=[
            pltpu.VMEM((EX, EY, CZ), F32),
            pltpu.VMEM((V, CX, CY, CZ), F32),
            pltpu.VMEM((V + 1, EX, CY, CZ), F32),
            pltpu.VMEM((V + 1, EX, CY, CZ), F32),
            pltpu.VMEM((V + 1, CX, CY, CZ), F32),
            pltpu.VMEM((V, CX, CY, CZ), F32),
            pltpu.VMEM((V, EX, 2 * CY, CZ), BF16),
            pltpu.VMEM((EX, EY, CZ), F32),
            pltpu.VMEM((EX, EY, CZ), F32),
            pltpu.VMEM((R, EY, CZ), F32),
            pltpu.VMEM((2, 2 * R, CZ), F32),
            pltpu.VMEM((3, V, CZ), F32),
            pltpu.VMEM((4, 3, 3 * R, CZ), F32),
            pltpu.VMEM((EX, EY, CZ), F32),
            pltpu.VMEM((V, 2 * R, CX * CY), F32),
            pltpu.VMEM((V, 2 * R, CX * CY), F32),
            pltpu.VMEM((3, 3, V, CZ), F32),
            pltpu.VMEM((1, V), jnp.int32),
            pltpu.VMEM((3, V, T), F32),
            pltpu.VMEM((3 + T, 2 * V, CZ), F32),
            pltpu.VMEM((2, 4 * R, CZ), F32),
            pltpu.VMEM((V, 256, 256), BF16),
            pltpu.VMEM((V, 384, 256), BF16),
            pltpu.VMEM((V, 192, 128), BF16),
            pltpu.VMEM((V, 2 * CY, 256), BF16),
            pltpu.VMEM((3, V, 2 * CY, 256), BF16),
            pltpu.VMEM((3, V, 128, 256), BF16),
            pltpu.VMEM((V + 1, CX, CY, CZ), F32),
            pltpu.VMEM((8, CZ), F32),
            pltpu.VMEM((2, 1, CZ), F32),
            pltpu.VMEM((2, 16, 1, CZ), F32),
            dma((4,)), dma((1,)), dma((3,)), dma((1,)), dma((2,)), dma((4,)), dma((4,)), dma((1,)), dma((2,)),
            dma((2, 2)), dma((2, 2)), dma((1,)), dma((2,)), dma((2,)), dma((2,)),
            pltpu.SemaphoreType.REGULAR((3,)),
        ],
        compiler_params=pltpu.CompilerParams(
            collective_id=0, has_side_effects=True, vmem_limit_bytes=48 * 1024 * 1024
        ),
    )(*[pltpu.with_memory_space_constraint(a, pltpu.HBM) for a in arrays])


def solution(mesh):
    block = P("bx", "by", "bz")
    views = P(None, "bx", "by", "bz")
    return jax.shard_map(
        on_device, mesh=mesh, in_specs=(block, views, views, P()), out_specs=block, check_vma=False
    )
```

```python
import functools

import jax
import jax.numpy as jnp
from jax import lax
from jax.experimental import pallas as pl
from jax.experimental.pallas import tpu as pltpu
from jax.sharding import PartitionSpec as P

MESH = pl.DeviceIdType.MESH
F32 = jnp.float32
BF16 = jnp.bfloat16
V, R, T = 8, 8, 17
CX, CY, CZ = 16, 16, 128
EX, EY = CX + 2 * R, CY + 2 * R
G = 4
LINES = (("bz", 4), ("by", 8), ("bx", 4))
STAGES = (8, 16)
SIDES = tuple((x, y) for x in (-1, 0, 1) for y in (-1, 0, 1) if x or y)
ROUNDS = (
    (("bz", 1), ("by", 1), ("bx", 1)),
    (("bz", 1), ("by", 1), ("bx", 1)),
    (("bz", 2), ("by", 2), ("bx", 2)),
    (("bz", 2), ("by", 4), ("bx", 2)),
)


def split(f):
    hi = f.astype(BF16)
    lo = (f - hi.astype(F32)).astype(BF16)
    return hi, lo


def dot(a, b):
    return jnp.dot(a, b, preferred_element_type=F32)


def stack4(f):
    hi, lo = split(f)
    return jnp.concatenate([hi, lo, hi, lo], axis=0)


def kernel(
    est, obs, cov, taps, out,
    e_buf, o_buf, y_buf, m_buf, g_buf, r_buf, x_buf, p_buf, rp_buf, tp_buf,
    zt_buf, share_buf, h_buf, ht_buf, sb_buf, hb_buf, w_buf, c_buf, k_buf, t_buf, l_buf,
    zf_mat, zm_mat, zh_mat, yf_mat, yw_mat, yb_mat, b_buf, seen_buf, red_own, red_in,
    load_sem, e_send, e_recv, w_send, w_recv, f_send, f_recv, h_send, h_recv,
    zb_send, zb_recv, p_send, p_recv, red_send, red_recv, met_sem,
):
    ids = {name: lax.axis_index(name) for name, _ in LINES}
    sizes = dict(LINES)

    def at(dx, dy, dz=0):
        return {
            name: lax.rem(ids[name] + d + sizes[name], sizes[name])
            for name, d in (("bx", dx), ("by", dy), ("bz", dz)) if d
        }

    barrier = pltpu.get_barrier_semaphore()

    def has(name, d):
        return ids[name] + d >= 0 if d < 0 else ids[name] + d < sizes[name]

    def meet(sem, steps):
        for name, size in steps:
            for d in (-size, size):
                @pl.when(has(name, d))
                def _():
                    pl.semaphore_signal(
                        sem, inc=1, device_id={name: ids[name] + d}, device_id_type=MESH
                    )

    def met(sem, steps, heard=0):
        for name, size in steps:
            for d in (-size, size):
                heard = heard + jnp.where(has(name, d), 1, 0)
        pl.semaphore_wait(sem, heard)

    def twin(dx):
        return lax.rem(ids["bx"], 2) == (1 - dx) // 2

    def cross(dx):
        return jnp.logical_and(has("bx", dx), jnp.logical_not(twin(dx)))

    def cross_both(dx, dy):
        return jnp.logical_and(cross(dx), has("by", dy))

    corners = [(dx, dy) for dx in (-1, 1) for dy in (-1, 1)]
    meet(barrier, ROUNDS[0])
    greeted = 0
    for dx, dy in corners:
        near_by = jnp.logical_and(has("bx", dx), has("by", dy))
        greeted = greeted + jnp.where(near_by, 1, 0)

        @pl.when(near_by)
        def _():
            pl.semaphore_signal(barrier, inc=1, device_id=at(dx, dy), device_id_type=MESH)
    load_e = pltpu.make_async_copy(est, e_buf.at[pl.ds(R, CX), pl.ds(R, CY)], load_sem.at[0])
    load_c = pltpu.make_async_copy(cov, c_buf, load_sem.at[1])
    load_t = pltpu.make_async_copy(taps, k_buf, load_sem.at[2])
    load_o = pltpu.make_async_copy(obs, o_buf, load_sem.at[3])
    for load in (load_e, load_c, load_t, load_o):
        load.start()

    def both(dx, dy):
        if dx and dy:
            return jnp.logical_and(has("bx", dx), has("by", dy))
        return has("bx", dx) if dx else has("by", dy)

    def remote(src, dst, send, recv, device):
        return pltpu.make_async_remote_copy(
            src_ref=src, dst_ref=dst, send_sem=send, recv_sem=recv,
            device_id=device, device_id_type=MESH,
        )

    own = pl.ds(R, CX)
    edge = {-1: pl.ds(0, R), 0: own, 1: pl.ds(EX - R, R)}
    inner = {-1: pl.ds(R, R), 0: own, 1: pl.ds(CX, R)}

    def counted(act):
        ends = [
            jnp.logical_and(has(name, -1), has(name, 1)) for name in ("bx", "by")
        ]
        for nx in (1, 2):
            for ny in (1, 2):
                hit = [e if n == 2 else jnp.logical_not(e) for e, n in zip(ends, (nx, ny))]

                @pl.when(jnp.logical_and(*hit))
                def _():
                    act(nx, ny)

    def planes_of(buf, rows):
        width = 32 if rows % 32 == 0 else 24
        return buf.at[pl.ds(0, rows // width), pl.ds(0, width)]

    def group(ref, send, recv):
        return remote(ref, ref, send, recv, at(0, 0, 1))

    def e_copy(dx, dy):
        return remote(
            e_buf.at[inner[dx], inner[dy]], e_buf.at[edge[-dx], edge[-dy]],
            e_send.at[0], e_recv.at[0 if dx else (3 - dy) // 2], at(dx, dy),
        )

    def e_pass(dx, dy):
        return remote(
            e_buf.at[inner[dx], edge[dy]], e_buf.at[edge[-dx], edge[dy]],
            e_send.at[0], e_recv.at[0], at(dx, 0),
        )

    def p_copy(dx, dy):
        return remote(
            p_buf.at[edge[dx], edge[dy]], rp_buf.at[edge[-dx], edge[-dy]],
            p_send.at[0], p_recv.at[0], at(dx, dy),
        )

    def p_pass(dx):
        return remote(p_buf.at[edge[dx]], tp_buf, p_send.at[0], p_recv.at[1], at(dx, 0))

    rows = {-1: pl.ds(R, R), 1: pl.ds(0, R)}
    to_rows = {-1: pl.ds(R, R), 1: pl.ds(0, R)}

    def face_copy(dz):
        return remote(
            zt_buf.at[:, rows[dz]], h_buf.at[pl.ds(1, 2), 1, to_rows[dz]],
            f_send.at[(1 + dz) // 2], f_recv.at[(1 - dz) // 2], at(0, 0, dz),
        )

    def share_copy(dz):
        return remote(
            share_buf.at[2], share_buf.at[(1 - dz) // 2],
            f_send.at[2 + (1 + dz) // 2], f_recv.at[2 + (1 - dz) // 2], at(0, 0, dz),
        )

    def h_copy(dx, dy):
        src = {-1: pl.ds(1, 1), 0: pl.ds(1, 2), 1: pl.ds(2, 1)}[dx]
        dst = {-1: pl.ds(3, 1), 0: pl.ds(1, 2), 1: pl.ds(0, 1)}[dx]
        return remote(
            h_buf.at[src, 1], h_buf.at[dst, 1 - dy],
            h_send.at[0], h_recv.at[1 if dx else 0], at(dx, dy),
        )

    def w_copy(dx, dy):
        return remote(
            w_buf.at[1, 1], w_buf.at[1 - dx, 1 - dy],
            w_send.at[0], w_recv.at[1 if dx else 0], at(dx, dy),
        )

    def z_copy(g, dz):
        views = pl.ds(G * g, G)
        bz, n = ids["bz"], sizes["bz"]
        place = 1 + (bz + 1) // n if dz > 0 else 2 * ((n - bz) // n)
        side = (dz + 1) // 2
        return remote(
            sb_buf.at[views, rows[dz]], hb_buf.at[views, pl.ds(pl.multiple_of(R * place, R), R)],
            zb_send.at[g, side], zb_recv.at[g, 1 - side], at(0, 0, dz),
        )

    part = functools.partial

    for d in (-1, 1):
        @pl.when(jnp.logical_not(has("by", d)))
        def _():
            e_buf[:, edge[d], :] = jnp.zeros((EX, R, CZ), F32)
            rp_buf[:, edge[d], :] = jnp.zeros((EX, R, CZ), F32)
            h_buf[:, 1 + d] = jnp.zeros((4, 3 * R, CZ), F32)
            w_buf[:, 1 + d] = jnp.zeros((3, V, CZ), F32)

        @pl.when(jnp.logical_not(has("bx", d)))
        def _():
            e_buf[edge[d]] = jnp.zeros((R, EY, CZ), F32)
            h_buf[3 * (1 + d) // 2] = jnp.zeros((3, 3 * R, CZ), F32)
            w_buf[1 + d] = jnp.zeros((3, V, CZ), F32)

        @pl.when(jnp.logical_not(cross(d)))
        def _():
            rp_buf[edge[d]] = jnp.zeros((R, EY, CZ), F32)

        @pl.when(jnp.logical_not(has("bz", d)))
        def _():
            hb_buf[:, rows[d], :] = jnp.zeros((V, R, CX * CY), F32)
            h_buf[1:3, 1, to_rows[-d], :] = jnp.zeros((2, R, CZ), F32)
            share_buf[(1 + d) // 2] = jnp.zeros((V, CZ), F32)

    row8 = lax.broadcasted_iota(jnp.int32, (V, CZ), 0)
    lane8 = lax.broadcasted_iota(jnp.int32, (V, CZ), 1)
    load_c.wait()
    flags = jnp.broadcast_to(c_buf[...].astype(F32), (V, V))
    picked = jnp.where(row8[:, :V] == lane8[:, :V], flags, 0.0)
    weight = jnp.broadcast_to(jnp.sum(picked, axis=1, keepdims=True), (V, CZ))
    w_buf[1, 1] = weight
    share_buf[2] = weight / jnp.sum(weight, axis=0, keepdims=True)
    load_e.wait()
    planes = e_buf[own, own].reshape(CX * CY, CZ)
    for h in range(2):
        flipped = planes[128 * h:128 * h + 128].T
        zt_buf[h, 0:R] = flipped[CZ - R:]
        zt_buf[h, R:2 * R] = flipped[:R]
    met(barrier, ROUNDS[0], greeted)
    meet(met_sem.at[0], ROUNDS[1])
    for d in (-1, 1):
        @pl.when(has("bz", d))
        def _():
            face_copy(d).start()
            share_copy(d).start()
    for dx, dy in SIDES:
        @pl.when(both(dx, dy))
        def _():
            w_copy(dx, dy).start()
    for d in (-1, 1):
        @pl.when(has("bx", d))
        def _():
            e_copy(d, 0).start()
    for d in (-1, 1):
        @pl.when(has("by", d))
        def _():
            e_copy(0, d).start()
    for dx, dy in corners:
        @pl.when(cross_both(dx, dy))
        def _():
            e_copy(dx, dy).start()

    load_t.wait()
    t_buf[...] = jnp.zeros_like(t_buf)
    for d in range(3):
        t_buf[d, 0:V, 0:T] = k_buf[d]
    taps_x, taps_y, taps_z = (
        t_buf[d, 0:V] / jnp.sum(t_buf[d, 0:V], axis=1, keepdims=True) for d in range(3)
    )
    for k, table in enumerate((taps_x, taps_y)):
        wide = jnp.concatenate(
            [jnp.broadcast_to(table[v:v + 1], (2 * R, CZ)) for v in range(V)], axis=0
        ).T
        l_buf[k] = wide[:4 * R]
    taps_y = taps_y + pltpu.roll(taps_y, 32, 1)
    taps_y = taps_y + pltpu.roll(taps_y, 64, 1)
    band = lax.broadcasted_iota(jnp.int32, (CY, 128), 1)
    bands = []
    for v in range(V):
        q = pltpu.roll(
            jnp.broadcast_to(taps_y[v:v + 1], (CY, 128)), 0, 1, stride=1, stride_axis=0
        )
        bands.append(q)
        q_hi, q_lo = split(q)
        zero = jnp.zeros_like(q_hi)
        for x in range(2):
            mine = (band // 32) % 2 == x
            yf_mat[v, x * CY:(x + 1) * CY, 0:128] = jnp.where(mine, q_hi, zero)
            yf_mat[v, x * CY:(x + 1) * CY, 128:256] = jnp.where(mine, q_lo, zero)
    for k in range(T):
        t_buf[3 + k, 0:V] = jnp.broadcast_to(taps_x[:, k:k + 1], (V, CZ))
        t_buf[3 + k, V:2 * V] = jnp.broadcast_to(l_buf[0, k:k + 1], (V, CZ))

    lane = lax.broadcasted_iota(jnp.int32, (128, 128), 1)
    row = lax.broadcasted_iota(jnp.int32, (128, 128), 0)
    near = jnp.abs(row - lane) <= R
    zf_mat[:, 128:256, :] = jnp.zeros((V, 128, 256), BF16)
    zh_mat[...] = jnp.zeros_like(zh_mat)
    for v in range(V):
        ring = pltpu.roll(
            jnp.broadcast_to(taps_z[v:v + 1], (128, 128)), 128 - R, 1, stride=1, stride_axis=0
        )
        ahead = ring.T
        m_hi, m_lo = split(jnp.where(near, ahead, 0.0))
        zf_mat[v, 0:128, 0:128] = m_hi
        zf_mat[v, 0:128, 128:256] = m_lo
        far = jnp.where(near, 0.0, ahead)
        f_hi, f_lo = split(jnp.concatenate([far[128 - R:128], far[0:R]], axis=0))
        top = 128 + 2 * R * v
        zf_mat[v, top:top + 2 * R, 0:128] = f_hi
        zf_mat[v, top:top + 2 * R, 128:256] = f_lo
        m_hi, m_lo = split(jnp.where(near, ring, 0.0))
        far = jnp.where(near, 0.0, ring)
        s_hi, s_lo = split(pltpu.roll(far, (2 * R * v + R) % 128, 1))
        for i in range(2):
            zm_mat[v, 128 * i:128 * i + 128, 0:128] = m_hi
            zm_mat[v, 128 * i:128 * i + 128, 128:256] = s_hi
        zm_mat[v, 256:384, 0:128] = m_lo
        zm_mat[v, 256:384, 128:256] = s_lo
        f_hi, f_lo = split(jnp.concatenate([far[0:R], far[128 - R:128]], axis=0))
        top = 2 * R * (v % G)
        zh_mat[v, top:top + 2 * R] = f_hi
        zh_mat[v, 64 + top:64 + top + 2 * R] = f_hi
        zh_mat[v, 128 + top:128 + top + 2 * R] = f_lo

    load_o.wait()
    seen = jnp.zeros((8, CZ), F32)
    for v in range(V):
        seen = seen + w_buf[1, 1, v:v + 1] * jnp.sum(o_buf[v].reshape(CX * CY // 8, 8, CZ), axis=0)
    count_own = jnp.sum(w_buf[1, 1], axis=0, keepdims=True)
    seen_buf[...] = seen / count_own

    for d in (-1, 1):
        @pl.when(has("bz", d))
        def _():
            face_copy(-d).wait_recv()
            share_copy(-d).wait_recv()
    for b in (1, 2):
        h_buf[b, 1, 2 * R:] = jnp.where(lane8 < CZ // 2, share_buf[0], share_buf[1])
    met(met_sem.at[0], ROUNDS[1])
    meet(met_sem.at[1], ROUNDS[2])
    for dx, dy in SIDES:
        @pl.when(both(dx, dy))
        def _():
            h_copy(dx, dy).start()
    for d in (-1, 1):
        @pl.when(has("by", d))
        def _():
            e_copy(0, -d).wait_recv()
            for dx in (-1, 1):
                @pl.when(twin(dx))
                def _():
                    e_pass(dx, d).start()

    def forward_y(x0, source=e_buf, mat=yf_mat, to=y_buf):
        data = jnp.concatenate(
            [stack4(source[pl.ds(x0 + 2 * h, 2)].reshape(2 * EY, CZ)) for h in range(2)], axis=1
        )
        full = dot(mat[...].reshape(V * 2 * CY, 256), data)
        for h in range(2):
            to[0:V, pl.ds(x0 + 2 * h, 2)] = full[:, h * CZ:(h + 1) * CZ].reshape(V, 2, CY, CZ)

    for x0 in range(R, R + CX, 4):
        forward_y(x0)

    def x_taps(v):
        return [jnp.broadcast_to(t_buf[3 + k, pl.ds(v, 1), :], (8, CZ)) for k in range(T)]

    def forward_x(inputs, first, y_buf, g_buf, v, carry):
        t = x_taps(v)
        for h in range(CY // 8):
            ys = pl.ds(8 * h, 8)
            acc = [None if first else g_buf[v, xo, ys, :] for xo in range(CX)]
            for xi in inputs:
                val = y_buf[v, xi, ys, :]
                for xo in range(max(0, xi - T + 1), min(CX, xi + 1)):
                    term = t[xi - xo] * val
                    acc[xo] = term if acc[xo] is None else acc[xo] + term
            for xo in range(CX):
                g_buf[v, xo, ys, :] = acc[xo]
        return carry

    y_spans = ((0, slice(R, CY), slice(0, R)), (1, slice(0, CY), slice(R, R + CY)),
               (2, slice(0, R), slice(R + CY, EY)))

    def halo_in(b):
        for yb, part_of, ys in y_spans:
            tile = jnp.concatenate([h_buf[b, yb, :2 * R]] * V, axis=0).T.reshape(R, CY, CZ)
            ht_buf[R * b:R * b + R, ys] = tile[:, part_of]

    def halo_share(b):
        for yb, _, ys in y_spans:
            tile = h_buf[b, yb, 2 * R:]
            before = jnp.broadcast_to(tile[:, 0:1], (V, CZ))
            after = jnp.broadcast_to(tile[:, CZ // 2:CZ // 2 + 1], (V, CZ))
            share = jnp.where(lane8 % (2 * R) < R, before, after)
            share = jnp.sum(jnp.where(lane8 // (2 * R) == row8, share, 0.0), axis=0, keepdims=True)
            at_x = slice(R * b, R * b + R)
            ht_buf[at_x, ys] = ht_buf[at_x, ys] * share

    def halo_y(b, to):
        t = [jnp.broadcast_to(l_buf[1, k:k + 1, :], (8, CZ)) for k in range(T)]
        for x in range(R * b, R * b + R):
            for h in range(2):
                acc = None
                for k in range(T):
                    term = t[k] * ht_buf[x, 8 * h + k:8 * h + k + 8, :]
                    acc = term if acc is None else acc + term
                to[V, x, 8 * h:8 * h + 8, :] = acc

    third = (band % 32)[:8]
    spans = ((0, R), (R, R + CX), (R + CX, EX))

    def mask(xb):
        xs = slice(*spans[xb])
        for yb in range(3):
            ys = slice(*spans[yb])
            count = jnp.maximum(jnp.sum(w_buf[xb, yb], axis=0, keepdims=True), 1.0)
            p_buf[xs, ys] = e_buf[xs, ys] * (1.0 / count)
        w = jnp.where(third < R, w_buf[xb, 0], jnp.where(third < R + CY, w_buf[xb, 1], w_buf[xb, 2]))
        for v in range(V):
            wide = jnp.broadcast_to(w[v:v + 1], (2 * CY, CZ)).astype(BF16)
            for i in range(2):
                cols = slice(128 * i, 128 * i + 128)
                yw_mat[xb, v, :, cols] = yf_mat[v, :, cols] * wide

    own_planes = range(R, R + CX)
    lax.fori_loop(0, V, part(forward_x, own_planes, True, y_buf, g_buf), 0)
    halo_planes = tuple(range(R)) + tuple(range(R + CX, EX))

    def masked_y(xb):
        mask(xb)
        for x0 in range(spans[xb][0], spans[xb][1], 4):
            forward_y(x0, p_buf, yw_mat.at[xb], m_buf)

    def w_arrivals(nx, ny):
        group(w_buf.at[0, pl.ds(0, ny)], w_send.at[0], w_recv.at[0]).wait_recv()

    counted(w_arrivals)
    masked_y(1)
    lax.fori_loop(0, V, part(forward_x, own_planes, True, m_buf, b_buf), 0)
    def x_arrivals(nx, ny):
        group(planes_of(e_buf, nx * (128 + 64 * ny)), e_send.at[0], e_recv.at[0]).wait_recv()
        tiles = w_buf.at[pl.ds(0, nx), pl.ds(0, 3)] if ny == 2 else w_buf.at[pl.ds(0, 2), pl.ds(0, nx)]
        group(tiles, w_send.at[0], w_recv.at[1]).wait_recv()

    counted(x_arrivals)
    for x0 in (0, 4, EX - 8, EX - 4):
        forward_y(x0)
    lax.fori_loop(0, V, part(forward_x, halo_planes, False, y_buf, g_buf), 0)
    masked_y(0)
    masked_y(2)
    lax.fori_loop(0, V, part(forward_x, halo_planes, False, m_buf, b_buf), 0)
    met(met_sem.at[1], ROUNDS[2])
    meet(met_sem.at[2], ROUNDS[3])

    def h_arrivals(nx, ny):
        group(h_buf.at[pl.ds(0, 2 * ny), 0], h_send.at[0], h_recv.at[0]).wait_recv()
        blocks = {2: pl.ds(0, nx), 1: pl.ds(0, 2 * nx)}[ny]
        cols = pl.ds(0, 3) if ny == 2 else 0
        group(h_buf.at[blocks, cols], h_send.at[0], h_recv.at[1]).wait_recv()

    counted(h_arrivals)
    for b in range(4):
        halo_in(b)
    for b in range(4):
        halo_y(b, y_buf)
    forward_x(range(EX), True, y_buf, g_buf, V, 0)

    def send_edges(fields, g):
        for v, f in zip(range(G * g, G * g + G), fields):
            for h in range(2):
                flipped = f[128 * h:128 * h + 128].T
                sb_buf[v, 0:R, 128 * h:128 * h + 128] = flipped[CZ - R:]
                sb_buf[v, R:2 * R, 128 * h:128 * h + 128] = flipped[:R]
        for d in (-1, 1):
            z_copy(g, d).start()

    def halo_rows(g):
        flat = hb_buf[G * g:G * g + G, 0:2 * R].reshape(G * 2 * R, CX * CY)
        hi = flat.astype(BF16).astype(F32)
        pair = jnp.concatenate([hi, flat - hi], axis=0)
        pair = jnp.concatenate([pair[:, :128].T, pair[:, 128:].T], axis=0).astype(BF16)
        return jnp.concatenate([pair, pair[:, :64]], axis=1)

    def z_apply(f, halo, mat, v):
        hi, lo = split(f)
        both = dot(jnp.concatenate([hi, halo[0]], axis=1), mat[v])
        rest = dot(jnp.concatenate([lo, halo[1]], axis=1), mat[v, :, 0:128])
        return both[:, :128] + both[:, 128:] + rest

    halo = split(g_buf[V].reshape(CX * CY, CZ))
    for g in range(V // G):
        ratios = []
        for v in range(G * g, G * g + G):
            blurred = z_apply(g_buf[v].reshape(CX * CY, CZ), halo, zf_mat, v)
            ratio = o_buf[v].reshape(CX * CY, CZ) / blurred
            r_buf[v] = ratio.reshape(CX, CY, CZ)
            ratios.append(ratio)
        send_edges(ratios, g)

    total = jnp.zeros((8, CZ), F32)
    outside = jnp.zeros((CX * CY, CZ), F32)
    for v in range(V):
        hi, lo = split(r_buf[v].reshape(CX * CY, CZ))
        f = dot(jnp.concatenate([hi, lo], axis=1), zm_mat[v, 0:256]) + dot(hi, zm_mat[v, 256:384])
        g_buf[v] = f[:, :128].reshape(CX, CY, CZ)
        outside = outside + f[:, 128:]
        weighed = f[:, :128] * b_buf[v].reshape(CX * CY, CZ)
        total = total + jnp.sum(weighed.reshape(CX * CY // 8, 8, CZ), axis=0)
    for b in range(4):
        halo_share(b)
    for b in range(4):
        halo_y(b, m_buf)
    forward_x(range(EX), True, m_buf, b_buf, V, 0)
    weighed = outside * b_buf[V].reshape(CX * CY, CZ)
    total = total + jnp.sum(weighed.reshape(CX * CY // 8, 8, CZ), axis=0)
    lane1 = lax.broadcasted_iota(jnp.int32, (1, CZ), 1)

    def summed(f):
        return jnp.sum(jnp.sum(f, axis=0, keepdims=True), axis=1, keepdims=True)

    red_own[0] = jnp.where(lane1 < CZ // 2, summed(seen_buf[...]), summed(total))

    by_hi, by_lo = lax.div(ids["by"], 4), lax.rem(ids["by"], 4)

    def red_peer(stage, d):
        if stage == 0:
            return {
                "bx": lax.rem(ids["bx"] + d % 4, 4),
                "by": lax.rem(by_hi + d // 4, 2) * 4 + by_lo,
            }
        return {
            "bz": lax.rem(ids["bz"] + d % 4, 4),
            "by": by_hi * 4 + lax.rem(by_lo + d // 4, 4),
        }

    def red_copy(stage, d):
        return pltpu.make_async_remote_copy(
            src_ref=red_own.at[stage], dst_ref=red_in.at[stage, d],
            send_sem=red_send.at[stage], recv_sem=red_recv.at[stage],
            device_id=red_peer(stage, d), device_id_type=MESH,
        )

    def red_start(stage):
        for d in range(1, STAGES[stage]):
            red_copy(stage, d).start()

    def red_all(stage):
        every = red_in.at[stage, pl.ds(1, STAGES[stage] - 1)]
        return pltpu.make_async_remote_copy(
            src_ref=every, dst_ref=every, send_sem=red_send.at[stage],
            recv_sem=red_recv.at[stage], device_id=red_peer(stage, 1), device_id_type=MESH,
        )

    def red_finish(stage):
        red_all(stage).wait_recv()
        total = red_own[stage]
        for d in range(1, STAGES[stage]):
            total = total + red_in[stage, d]
        return total

    met(met_sem.at[2], ROUNDS[3])
    red_start(0)
    for v in range(V):
        q4 = jnp.concatenate(
            [jnp.where(band // 32 == i // 2, bands[v], 0.0) for i in range(8)], axis=0
        ).T
        pair = split(q4)
        for xb in range(3):
            w = [jnp.broadcast_to(w_buf[xb, yb, v:v + 1], (8, CZ)) for yb in (0, 1, 1, 2)]
            w = jnp.concatenate(w * 4, axis=0).astype(BF16)
            for i in range(2):
                yb_mat[xb, v, :, 128 * i:128 * i + 128] = pair[i] * w

    def backward_x(outputs, v, carry):
        t = x_taps(v)
        for xo in outputs:
            accs = []
            for h in range(CY // 8):
                ys = pl.ds(8 * h, 8)
                acc = None
                for xi in range(max(0, xo - T + 1), min(CX, xo + 1)):
                    term = t[xo - xi] * g_buf[v, xi, ys, :]
                    acc = term if acc is None else acc + term
                accs.append(acc)
            hi, lo = split(jnp.concatenate(accs, axis=0))
            x_buf[v, xo, 0:CY, :] = hi
            x_buf[v, xo, CY:2 * CY, :] = lo
        return carry

    for g in range(V // G):
        for d in (-1, 1):
            z_copy(g, d).wait_recv()
        halo = halo_rows(g)
        for v in range(G * g, G * g + G):
            g_buf[v] = g_buf[v] + dot(halo, zh_mat[v]).reshape(CX, CY, CZ)

    lax.fori_loop(0, V, part(backward_x, halo_planes), 0)

    def backward_y(x0, xb):
        full = None
        for v in range(V):
            data = []
            for h in range(2):
                planes = x_buf[v, x0 + 4 * h:x0 + 4 * h + 4].reshape(128, CZ)
                data.append(jnp.concatenate([planes, planes], axis=0))
            term = dot(yb_mat[xb, v], jnp.concatenate(data, axis=1))
            full = term if full is None else full + term
        for h in range(2):
            p_buf[x0 + 4 * h:x0 + 4 * h + 4] = full[:, h * CZ:(h + 1) * CZ].reshape(4, EY, CZ)

    backward_y(0, 0)
    backward_y(EX - 8, 2)
    for dx in (-1, 1):
        @pl.when(twin(dx))
        def _():
            p_pass(dx).start()

        @pl.when(cross(dx))
        def _():
            p_copy(dx, 0).start()
        for dy in (-1, 1):
            @pl.when(cross_both(dx, dy))
            def _():
                p_copy(dx, dy).start()
    red_own[1] = red_finish(0)
    red_start(1)
    lax.fori_loop(0, V, part(backward_x, range(R, R + CX)), 0)
    backward_y(R, 1)
    backward_y(2 * R, 1)
    for dx in (-1, 1):
        @pl.when(twin(dx))
        def _():
            p_pass(dx).wait_recv()
            p_buf[inner[dx]] = p_buf[inner[dx]] + tp_buf[...]
    for d in (-1, 1):
        @pl.when(has("by", d))
        def _():
            p_copy(0, d).start()
    def p_arrivals(nx, ny):
        rows = 128 * ny + (128 + 64 * ny) * (nx - 1)
        group(planes_of(rp_buf, rows), p_send.at[0], p_recv.at[0]).wait_recv()

    counted(p_arrivals)
    for s in range(2):
        xs, xe = slice(R + 8 * s, R + 8 * s + 8), edge[2 * s - 1]
        for h in range(2):
            ys, ye = slice(R + 8 * h, R + 8 * h + 8), edge[2 * h - 1]
            summed = p_buf[xs, ys] + rp_buf[xe, ys] + rp_buf[xs, ye] + rp_buf[xe, ye]
            out[8 * s:8 * s + 8, 8 * h:8 * h + 8, :] = e_buf[xs, ys, :] * summed
    def departures(nx, ny):
        group(planes_of(e_buf, 128 * (nx + ny) + 64 * nx * ny), e_send.at[0], e_recv.at[0]).wait_send()
        blocks = 2 * ny + nx * (1 + ny)
        group(e_buf.at[pl.ds(0, blocks), pl.ds(0, 24)], h_send.at[0], h_recv.at[0]).wait_send()
        tiles = e_buf.at[pl.ds(0, nx + ny + nx * ny), pl.ds(0, V)]
        group(tiles, w_send.at[0], w_recv.at[0]).wait_send()
        rows = 256 + 128 * ny + (128 + 64 * ny) * (nx - 1)
        group(planes_of(e_buf, rows), p_send.at[0], p_recv.at[0]).wait_send()

    counted(departures)
    for d in (-1, 1):
        @pl.when(has("bz", d))
        def _():
            face_copy(d).wait_send()
            share_copy(d).wait_send()
    for g in range(V // G):
        for d in (-1, 1):
            z_copy(g, d).wait_send()
    red_all(0).wait_send()
    red_all(1).wait_send()
    final = red_finish(1)
    scale = final[:, 0:1] / (final[:, CZ // 2:CZ // 2 + 1] * count_own[:, 0:1])
    out[...] = out[...] * scale.reshape(1, 1, 1)


def on_device(estimate, observed, coverage, psf_taps):
    dma = pltpu.SemaphoreType.DMA
    arrays = (estimate, observed, coverage.reshape(1, V), jnp.transpose(psf_taps, (1, 0, 2)))
    return pl.pallas_call(
        kernel,
        out_shape=jax.ShapeDtypeStruct((CX, CY, CZ), F32),
        in_specs=[pl.BlockSpec(memory_space=pltpu.HBM)] * 4,
        out_specs=pl.BlockSpec(memory_space=pltpu.VMEM),
        scratch_shapes=[
            pltpu.VMEM((EX, EY, CZ), F32),
            pltpu.VMEM((V, CX, CY, CZ), F32),
            pltpu.VMEM((V + 1, EX, CY, CZ), F32),
            pltpu.VMEM((V + 1, EX, CY, CZ), F32),
            pltpu.VMEM((V + 1, CX, CY, CZ), F32),
            pltpu.VMEM((V, CX, CY, CZ), F32),
            pltpu.VMEM((V, EX, 2 * CY, CZ), BF16),
            pltpu.VMEM((EX, EY, CZ), F32),
            pltpu.VMEM((EX, EY, CZ), F32),
            pltpu.VMEM((R, EY, CZ), F32),
            pltpu.VMEM((2, 2 * R, CZ), F32),
            pltpu.VMEM((3, V, CZ), F32),
            pltpu.VMEM((4, 3, 3 * R, CZ), F32),
            pltpu.VMEM((EX, EY, CZ), F32),
            pltpu.VMEM((V, 2 * R, CX * CY), F32),
            pltpu.VMEM((V, 3 * R, CX * CY), F32),
            pltpu.VMEM((3, 3, V, CZ), F32),
            pltpu.VMEM((1, V), jnp.int32),
            pltpu.VMEM((3, V, T), F32),
            pltpu.VMEM((3 + T, 2 * V, CZ), F32),
            pltpu.VMEM((2, 4 * R, CZ), F32),
            pltpu.VMEM((V, 256, 256), BF16),
            pltpu.VMEM((V, 384, 256), BF16),
            pltpu.VMEM((V, 192, 128), BF16),
            pltpu.VMEM((V, 2 * CY, 256), BF16),
            pltpu.VMEM((3, V, 2 * CY, 256), BF16),
            pltpu.VMEM((3, V, 128, 256), BF16),
            pltpu.VMEM((V + 1, CX, CY, CZ), F32),
            pltpu.VMEM((8, CZ), F32),
            pltpu.VMEM((2, 1, CZ), F32),
            pltpu.VMEM((2, 16, 1, CZ), F32),
            dma((4,)), dma((1,)), dma((3,)), dma((1,)), dma((2,)), dma((4,)), dma((4,)), dma((1,)), dma((2,)),
            dma((2, 2)), dma((2, 2)), dma((1,)), dma((2,)), dma((2,)), dma((2,)),
            pltpu.SemaphoreType.REGULAR((3,)),
        ],
        compiler_params=pltpu.CompilerParams(
            collective_id=0, has_side_effects=True, vmem_limit_bytes=48 * 1024 * 1024
        ),
    )(*[pltpu.with_memory_space_constraint(a, pltpu.HBM) for a in arrays])


def solution(mesh):
    block = P("bx", "by", "bz")
    views = P(None, "bx", "by", "bz")
    return jax.shard_map(
        on_device, mesh=mesh, in_specs=(block, views, views, P()), out_specs=block, check_vma=False
    )
```

```python
import functools

import jax
import jax.numpy as jnp
from jax import lax
from jax.experimental import pallas as pl
from jax.experimental.pallas import tpu as pltpu
from jax.sharding import PartitionSpec as P

MESH = pl.DeviceIdType.MESH
F32 = jnp.float32
BF16 = jnp.bfloat16
V, R, T = 8, 8, 17
CX, CY, CZ = 16, 16, 128
EX, EY = CX + 2 * R, CY + 2 * R
G = 4
LINES = (("bz", 4), ("by", 8), ("bx", 4))
STAGES = (8, 16)
SIDES = tuple((x, y) for x in (-1, 0, 1) for y in (-1, 0, 1) if x or y)
ROUNDS = (
    (("bz", 1), ("by", 1), ("bx", 1)),
    (("bz", 1), ("by", 1), ("bx", 1)),
    (("bz", 2), ("by", 2), ("bx", 2)),
    (("bz", 2), ("by", 4), ("bx", 2)),
)


def split(f):
    hi = f.astype(BF16)
    lo = (f - hi.astype(F32)).astype(BF16)
    return hi, lo


def dot(a, b):
    return jnp.dot(a, b, preferred_element_type=F32)


def stack4(f):
    hi, lo = split(f)
    return jnp.concatenate([hi, lo, hi, lo], axis=0)


def kernel(
    est, obs, cov, taps, out,
    e_buf, o_buf, y_buf, m_buf, g_buf, r_buf, x_buf, p_buf, rp_buf, tp_buf,
    zt_buf, share_buf, h_buf, ht_buf, sb_buf, hb_buf, w_buf, c_buf, k_buf, t_buf, l_buf,
    zf_mat, zm_mat, zh_mat, xb_mat, xf_mat, yf_mat, yw_mat, yb_mat, b_buf, seen_buf, red_own, red_in,
    load_sem, e_send, e_recv, w_send, w_recv, f_send, f_recv, h_send, h_recv,
    zb_send, zb_recv, p_send, p_recv, red_send, red_recv, met_sem,
):
    ids = {name: lax.axis_index(name) for name, _ in LINES}
    sizes = dict(LINES)

    def at(dx, dy, dz=0):
        return {
            name: lax.rem(ids[name] + d + sizes[name], sizes[name])
            for name, d in (("bx", dx), ("by", dy), ("bz", dz)) if d
        }

    barrier = pltpu.get_barrier_semaphore()

    def has(name, d):
        return ids[name] + d >= 0 if d < 0 else ids[name] + d < sizes[name]

    def meet(sem, steps):
        for name, size in steps:
            for d in (-size, size):
                @pl.when(has(name, d))
                def _():
                    pl.semaphore_signal(
                        sem, inc=1, device_id={name: ids[name] + d}, device_id_type=MESH
                    )

    def met(sem, steps, heard=0):
        for name, size in steps:
            for d in (-size, size):
                heard = heard + jnp.where(has(name, d), 1, 0)
        pl.semaphore_wait(sem, heard)

    def twin(dx):
        return lax.rem(ids["bx"], 2) == (1 - dx) // 2

    def cross(dx):
        return jnp.logical_and(has("bx", dx), jnp.logical_not(twin(dx)))

    def cross_both(dx, dy):
        return jnp.logical_and(cross(dx), has("by", dy))

    corners = [(dx, dy) for dx in (-1, 1) for dy in (-1, 1)]
    meet(barrier, ROUNDS[0])
    greeted = 0
    for dx, dy in corners:
        near_by = jnp.logical_and(has("bx", dx), has("by", dy))
        greeted = greeted + jnp.where(near_by, 1, 0)

        @pl.when(near_by)
        def _():
            pl.semaphore_signal(barrier, inc=1, device_id=at(dx, dy), device_id_type=MESH)
    load_e = pltpu.make_async_copy(est, e_buf.at[pl.ds(R, CX), pl.ds(R, CY)], load_sem.at[0])
    load_c = pltpu.make_async_copy(cov, c_buf, load_sem.at[1])
    load_t = pltpu.make_async_copy(taps, k_buf, load_sem.at[2])
    load_o = pltpu.make_async_copy(obs, o_buf, load_sem.at[3])
    for load in (load_e, load_c, load_t, load_o):
        load.start()

    def both(dx, dy):
        if dx and dy:
            return jnp.logical_and(has("bx", dx), has("by", dy))
        return has("bx", dx) if dx else has("by", dy)

    def remote(src, dst, send, recv, device):
        return pltpu.make_async_remote_copy(
            src_ref=src, dst_ref=dst, send_sem=send, recv_sem=recv,
            device_id=device, device_id_type=MESH,
        )

    own = pl.ds(R, CX)
    edge = {-1: pl.ds(0, R), 0: own, 1: pl.ds(EX - R, R)}
    inner = {-1: pl.ds(R, R), 0: own, 1: pl.ds(CX, R)}

    def counted(act):
        ends = [
            jnp.logical_and(has(name, -1), has(name, 1)) for name in ("bx", "by")
        ]
        for nx in (1, 2):
            for ny in (1, 2):
                hit = [e if n == 2 else jnp.logical_not(e) for e, n in zip(ends, (nx, ny))]

                @pl.when(jnp.logical_and(*hit))
                def _():
                    act(nx, ny)

    def planes_of(buf, rows):
        width = 32 if rows % 32 == 0 else 24
        return buf.at[pl.ds(0, rows // width), pl.ds(0, width)]

    def group(ref, send, recv):
        return remote(ref, ref, send, recv, at(0, 0, 1))

    def e_copy(dx, dy):
        return remote(
            e_buf.at[inner[dx], inner[dy]], e_buf.at[edge[-dx], edge[-dy]],
            e_send.at[0], e_recv.at[0 if dx else (3 - dy) // 2], at(dx, dy),
        )

    def e_pass(dx, dy):
        return remote(
            e_buf.at[inner[dx], edge[dy]], e_buf.at[edge[-dx], edge[dy]],
            e_send.at[0], e_recv.at[0], at(dx, 0),
        )

    def p_copy(dx, dy):
        return remote(
            p_buf.at[edge[dx], edge[dy]], rp_buf.at[edge[-dx], edge[-dy]],
            p_send.at[0], p_recv.at[0], at(dx, dy),
        )

    def p_pass(dx):
        return remote(p_buf.at[edge[dx]], tp_buf, p_send.at[0], p_recv.at[1], at(dx, 0))

    rows = {-1: pl.ds(R, R), 1: pl.ds(0, R)}
    to_rows = {-1: pl.ds(R, R), 1: pl.ds(0, R)}

    def face_copy(dz):
        return remote(
            zt_buf.at[:, rows[dz]], h_buf.at[pl.ds(1, 2), 1, to_rows[dz]],
            f_send.at[(1 + dz) // 2], f_recv.at[(1 - dz) // 2], at(0, 0, dz),
        )

    def share_copy(dz):
        return remote(
            share_buf.at[2], share_buf.at[(1 - dz) // 2],
            f_send.at[2 + (1 + dz) // 2], f_recv.at[2 + (1 - dz) // 2], at(0, 0, dz),
        )

    def h_copy(dx, dy):
        src = {-1: pl.ds(1, 1), 0: pl.ds(1, 2), 1: pl.ds(2, 1)}[dx]
        dst = {-1: pl.ds(3, 1), 0: pl.ds(1, 2), 1: pl.ds(0, 1)}[dx]
        return remote(
            h_buf.at[src, 1], h_buf.at[dst, 1 - dy],
            h_send.at[0], h_recv.at[1 if dx else 0], at(dx, dy),
        )

    def w_copy(dx, dy):
        return remote(
            w_buf.at[1, 1], w_buf.at[1 - dx, 1 - dy],
            w_send.at[0], w_recv.at[1 if dx else 0], at(dx, dy),
        )

    def z_copy(g, dz):
        views = pl.ds(G * g, G)
        bz, n = ids["bz"], sizes["bz"]
        place = 1 + (bz + 1) // n if dz > 0 else 2 * ((n - bz) // n)
        side = (dz + 1) // 2
        return remote(
            sb_buf.at[views, rows[dz]], hb_buf.at[views, pl.ds(pl.multiple_of(R * place, R), R)],
            zb_send.at[g, side], zb_recv.at[g, 1 - side], at(0, 0, dz),
        )

    part = functools.partial

    for d in (-1, 1):
        @pl.when(jnp.logical_not(has("by", d)))
        def _():
            e_buf[:, edge[d], :] = jnp.zeros((EX, R, CZ), F32)
            rp_buf[:, edge[d], :] = jnp.zeros((EX, R, CZ), F32)
            h_buf[:, 1 + d] = jnp.zeros((4, 3 * R, CZ), F32)
            w_buf[:, 1 + d] = jnp.zeros((3, V, CZ), F32)

        @pl.when(jnp.logical_not(has("bx", d)))
        def _():
            e_buf[edge[d]] = jnp.zeros((R, EY, CZ), F32)
            h_buf[3 * (1 + d) // 2] = jnp.zeros((3, 3 * R, CZ), F32)
            w_buf[1 + d] = jnp.zeros((3, V, CZ), F32)

        @pl.when(jnp.logical_not(cross(d)))
        def _():
            rp_buf[edge[d]] = jnp.zeros((R, EY, CZ), F32)

        @pl.when(jnp.logical_not(has("bz", d)))
        def _():
            hb_buf[:, rows[d], :] = jnp.zeros((V, R, CX * CY), F32)
            h_buf[1:3, 1, to_rows[-d], :] = jnp.zeros((2, R, CZ), F32)
            share_buf[(1 + d) // 2] = jnp.zeros((V, CZ), F32)

    row8 = lax.broadcasted_iota(jnp.int32, (V, CZ), 0)
    lane8 = lax.broadcasted_iota(jnp.int32, (V, CZ), 1)
    load_c.wait()
    flags = jnp.broadcast_to(c_buf[...].astype(F32), (V, V))
    picked = jnp.where(row8[:, :V] == lane8[:, :V], flags, 0.0)
    weight = jnp.broadcast_to(jnp.sum(picked, axis=1, keepdims=True), (V, CZ))
    w_buf[1, 1] = weight
    share_buf[2] = weight / jnp.sum(weight, axis=0, keepdims=True)
    load_e.wait()
    planes = e_buf[own, own].reshape(CX * CY, CZ)
    for h in range(2):
        flipped = planes[128 * h:128 * h + 128].T
        zt_buf[h, 0:R] = flipped[CZ - R:]
        zt_buf[h, R:2 * R] = flipped[:R]
    met(barrier, ROUNDS[0], greeted)
    meet(met_sem.at[0], ROUNDS[1])
    for d in (-1, 1):
        @pl.when(has("bz", d))
        def _():
            face_copy(d).start()
            share_copy(d).start()
    for dx, dy in SIDES:
        @pl.when(both(dx, dy))
        def _():
            w_copy(dx, dy).start()
    for d in (-1, 1):
        @pl.when(has("bx", d))
        def _():
            e_copy(d, 0).start()
    for d in (-1, 1):
        @pl.when(has("by", d))
        def _():
            e_copy(0, d).start()
    for dx, dy in corners:
        @pl.when(cross_both(dx, dy))
        def _():
            e_copy(dx, dy).start()

    load_t.wait()
    t_buf[...] = jnp.zeros_like(t_buf)
    for d in range(3):
        t_buf[d, 0:V, 0:T] = k_buf[d]
    taps_x, taps_y, taps_z = (
        t_buf[d, 0:V] / jnp.sum(t_buf[d, 0:V], axis=1, keepdims=True) for d in range(3)
    )
    for k, table in enumerate((taps_x, taps_y)):
        wide = jnp.concatenate(
            [jnp.broadcast_to(table[v:v + 1], (2 * R, CZ)) for v in range(V)], axis=0
        ).T
        l_buf[k] = wide[:4 * R]
    taps_y = taps_y + pltpu.roll(taps_y, 32, 1)
    taps_y = taps_y + pltpu.roll(taps_y, 64, 1)
    band = lax.broadcasted_iota(jnp.int32, (CY, 128), 1)
    bands = []
    for v in range(V):
        q = pltpu.roll(
            jnp.broadcast_to(taps_y[v:v + 1], (CY, 128)), 0, 1, stride=1, stride_axis=0
        )
        bands.append(q)
        q_hi, q_lo = split(q)
        zero = jnp.zeros_like(q_hi)
        for x in range(2):
            mine = (band // 32) % 2 == x
            yf_mat[v, x * CY:(x + 1) * CY, 0:128] = jnp.where(mine, q_hi, zero)
            yf_mat[v, x * CY:(x + 1) * CY, 128:256] = jnp.where(mine, q_lo, zero)
    for k in range(T):
        t_buf[3 + k, 0:V] = jnp.broadcast_to(taps_x[:, k:k + 1], (V, CZ))
        t_buf[3 + k, V:2 * V] = jnp.broadcast_to(l_buf[0, k:k + 1], (V, CZ))

    lane = lax.broadcasted_iota(jnp.int32, (128, 128), 1)
    row = lax.broadcasted_iota(jnp.int32, (128, 128), 0)
    near = jnp.abs(row - lane) <= R
    zf_mat[:, 128:256, :] = jnp.zeros((V, 128, 256), BF16)
    zh_mat[...] = jnp.zeros_like(zh_mat)
    for v in range(V):
        ring = pltpu.roll(
            jnp.broadcast_to(taps_z[v:v + 1], (128, 128)), 128 - R, 1, stride=1, stride_axis=0
        )
        ahead = ring.T
        m_hi, m_lo = split(jnp.where(near, ahead, 0.0))
        zf_mat[v, 0:128, 0:128] = m_hi
        zf_mat[v, 0:128, 128:256] = m_lo
        far = jnp.where(near, 0.0, ahead)
        f_hi, f_lo = split(jnp.concatenate([far[128 - R:128], far[0:R]], axis=0))
        top = 128 + 2 * R * v
        zf_mat[v, top:top + 2 * R, 0:128] = f_hi
        zf_mat[v, top:top + 2 * R, 128:256] = f_lo
        m_hi, m_lo = split(jnp.where(near, ring, 0.0))
        far = jnp.where(near, 0.0, ring)
        s_hi, s_lo = split(pltpu.roll(far, (2 * R * v + R) % 128, 1))
        for i in range(2):
            zm_mat[v, 128 * i:128 * i + 128, 0:128] = m_hi
            zm_mat[v, 128 * i:128 * i + 128, 128:256] = s_hi
        zm_mat[v, 256:384, 0:128] = m_lo
        zm_mat[v, 256:384, 128:256] = s_lo
        f_hi, f_lo = split(jnp.concatenate([far[0:R], far[128 - R:128]], axis=0))
        top = 2 * R * (v % G)
        zh_mat[v, top:top + 2 * R] = f_hi
        zh_mat[v, 64 + top:64 + top + 2 * R] = f_hi
        zh_mat[v, 128 + top:128 + top + 2 * R] = f_lo

    sparse = jnp.zeros((V, CZ), F32)
    for k in range(T - 1):
        sparse = sparse + jnp.where(lane8 == 8 * k, t_buf[3 + k, 0:V], 0.0)
    for v in range(V):
        turned = pltpu.roll(jnp.broadcast_to(sparse[v:v + 1], (128, 128)), 0, 1, stride=1, stride_axis=0)
        last = jnp.broadcast_to(t_buf[2 + T, v:v + 1], (128, 128))
        low = jnp.where(lane >= row, turned, 0.0)
        high = jnp.where(lane < row, turned, jnp.where(lane == row, last, 0.0))
        for i, tile in enumerate((low, high)):
            k_hi, k_lo = split(tile.T)
            xb_mat[v, 128 * i:128 * i + 128, 0:128] = k_hi
            xb_mat[v, 128 * i:128 * i + 128, 128:256] = k_hi
            xb_mat[v, 128 * i:128 * i + 128, 256:384] = k_lo
        k_hi, k_lo = split(jnp.where(lane < 64, pltpu.roll(low, 64, 1), pltpu.roll(high, 64, 1)))
        xf_mat[v, :, 0:128] = k_hi
        xf_mat[v, :, 128:256] = k_hi
        xf_mat[v, :, 256:384] = k_lo

    load_o.wait()
    seen = jnp.zeros((8, CZ), F32)
    for v in range(V):
        seen = seen + w_buf[1, 1, v:v + 1] * jnp.sum(o_buf[v].reshape(CX * CY // 8, 8, CZ), axis=0)
    count_own = jnp.sum(w_buf[1, 1], axis=0, keepdims=True)
    seen_buf[...] = seen / count_own

    for d in (-1, 1):
        @pl.when(has("bz", d))
        def _():
            face_copy(-d).wait_recv()
            share_copy(-d).wait_recv()
    for b in (1, 2):
        h_buf[b, 1, 2 * R:] = jnp.where(lane8 < CZ // 2, share_buf[0], share_buf[1])
    met(met_sem.at[0], ROUNDS[1])
    meet(met_sem.at[1], ROUNDS[2])
    for dx, dy in SIDES:
        @pl.when(both(dx, dy))
        def _():
            h_copy(dx, dy).start()
    for d in (-1, 1):
        @pl.when(has("by", d))
        def _():
            e_copy(0, -d).wait_recv()
            for dx in (-1, 1):
                @pl.when(twin(dx))
                def _():
                    e_pass(dx, d).start()

    def forward_y(x0, source=e_buf, mat=yf_mat, to=y_buf):
        data = jnp.concatenate(
            [stack4(source[pl.ds(x0 + 2 * h, 2)].reshape(2 * EY, CZ)) for h in range(2)], axis=1
        )
        full = dot(mat[...].reshape(V * 2 * CY, 256), data)
        for h in range(2):
            to[0:V, pl.ds(x0 + 2 * h, 2)] = full[:, h * CZ:(h + 1) * CZ].reshape(V, 2, CY, CZ)

    for x0 in range(R, R + CX, 4):
        forward_y(x0)

    def x_taps(v):
        return [jnp.broadcast_to(t_buf[3 + k, pl.ds(v, 1), :], (8, CZ)) for k in range(T)]

    def forward_x(inputs, first, y_buf, g_buf, v, carry):
        t = x_taps(v)
        for h in range(CY // 8):
            ys = pl.ds(8 * h, 8)
            acc = [None if first else g_buf[v, xo, ys, :] for xo in range(CX)]
            for xi in inputs:
                val = y_buf[v, xi, ys, :]
                for xo in range(max(0, xi - T + 1), min(CX, xi + 1)):
                    term = t[xi - xo] * val
                    acc[xo] = term if acc[xo] is None else acc[xo] + term
            for xo in range(CX):
                g_buf[v, xo, ys, :] = acc[xo]
        return carry

    y_spans = ((0, slice(R, CY), slice(0, R)), (1, slice(0, CY), slice(R, R + CY)),
               (2, slice(0, R), slice(R + CY, EY)))

    def halo_in(b):
        for yb, part_of, ys in y_spans:
            tile = jnp.concatenate([h_buf[b, yb, :2 * R]] * V, axis=0).T.reshape(R, CY, CZ)
            ht_buf[R * b:R * b + R, ys] = tile[:, part_of]

    def halo_share(b):
        for yb, _, ys in y_spans:
            tile = h_buf[b, yb, 2 * R:]
            before = jnp.broadcast_to(tile[:, 0:1], (V, CZ))
            after = jnp.broadcast_to(tile[:, CZ // 2:CZ // 2 + 1], (V, CZ))
            share = jnp.where(lane8 % (2 * R) < R, before, after)
            share = jnp.sum(jnp.where(lane8 // (2 * R) == row8, share, 0.0), axis=0, keepdims=True)
            at_x = slice(R * b, R * b + R)
            ht_buf[at_x, ys] = ht_buf[at_x, ys] * share

    def halo_y(b, to):
        t = [jnp.broadcast_to(l_buf[1, k:k + 1, :], (8, CZ)) for k in range(T)]
        for x in range(R * b, R * b + R):
            for h in range(2):
                acc = None
                for k in range(T):
                    term = t[k] * ht_buf[x, 8 * h + k:8 * h + k + 8, :]
                    acc = term if acc is None else acc + term
                to[V, x, 8 * h:8 * h + 8, :] = acc

    third = (band % 32)[:8]
    spans = ((0, R), (R, R + CX), (R + CX, EX))

    def mask(xb):
        xs = slice(*spans[xb])
        for yb in range(3):
            ys = slice(*spans[yb])
            count = jnp.maximum(jnp.sum(w_buf[xb, yb], axis=0, keepdims=True), 1.0)
            p_buf[xs, ys] = e_buf[xs, ys] * (1.0 / count)
        w = jnp.where(third < R, w_buf[xb, 0], jnp.where(third < R + CY, w_buf[xb, 1], w_buf[xb, 2]))
        for v in range(V):
            wide = jnp.broadcast_to(w[v:v + 1], (2 * CY, CZ)).astype(BF16)
            for i in range(2):
                cols = slice(128 * i, 128 * i + 128)
                yw_mat[xb, v, :, cols] = yf_mat[v, :, cols] * wide


    def own_x(source, to):
        for v in range(V):
            pairs = [split(source[v, own, 8 * h:8 * h + 8, :].reshape(128, CZ)) for h in range(2)]
            data = jnp.concatenate([jnp.concatenate(p, axis=0) for p in pairs], axis=1)
            full = dot(xf_mat[v, :, 0:256], data) + dot(xf_mat[v, :, 256:384], data[0:128])
            for h in range(2):
                to[v, :, 8 * h:8 * h + 8, :] = full[:, h * CZ:(h + 1) * CZ].reshape(CX, 8, CZ)

    own_x(y_buf, g_buf)
    halo_planes = tuple(range(R)) + tuple(range(R + CX, EX))

    def masked_y(xb):
        mask(xb)
        for x0 in range(spans[xb][0], spans[xb][1], 4):
            forward_y(x0, p_buf, yw_mat.at[xb], m_buf)

    def w_arrivals(nx, ny):
        group(w_buf.at[0, pl.ds(0, ny)], w_send.at[0], w_recv.at[0]).wait_recv()

    counted(w_arrivals)
    masked_y(1)
    own_x(m_buf, b_buf)
    def x_arrivals(nx, ny):
        group(planes_of(e_buf, nx * (128 + 64 * ny)), e_send.at[0], e_recv.at[0]).wait_recv()
        tiles = w_buf.at[pl.ds(0, nx), pl.ds(0, 3)] if ny == 2 else w_buf.at[pl.ds(0, 2), pl.ds(0, nx)]
        group(tiles, w_send.at[0], w_recv.at[1]).wait_recv()

    counted(x_arrivals)
    for x0 in (0, 4, EX - 8, EX - 4):
        forward_y(x0)
    lax.fori_loop(0, V, part(forward_x, halo_planes, False, y_buf, g_buf), 0)
    masked_y(0)
    masked_y(2)
    lax.fori_loop(0, V, part(forward_x, halo_planes, False, m_buf, b_buf), 0)
    met(met_sem.at[1], ROUNDS[2])
    meet(met_sem.at[2], ROUNDS[3])

    def h_arrivals(nx, ny):
        group(h_buf.at[pl.ds(0, 2 * ny), 0], h_send.at[0], h_recv.at[0]).wait_recv()
        blocks = {2: pl.ds(0, nx), 1: pl.ds(0, 2 * nx)}[ny]
        cols = pl.ds(0, 3) if ny == 2 else 0
        group(h_buf.at[blocks, cols], h_send.at[0], h_recv.at[1]).wait_recv()

    counted(h_arrivals)
    for b in range(4):
        halo_in(b)
    for b in range(4):
        halo_y(b, y_buf)
    forward_x(range(EX), True, y_buf, g_buf, V, 0)

    def send_edges(fields, g):
        for v, f in zip(range(G * g, G * g + G), fields):
            for h in range(2):
                flipped = f[128 * h:128 * h + 128].T
                sb_buf[v, 0:R, 128 * h:128 * h + 128] = flipped[CZ - R:]
                sb_buf[v, R:2 * R, 128 * h:128 * h + 128] = flipped[:R]
        for d in (-1, 1):
            z_copy(g, d).start()

    def halo_rows(g):
        flat = hb_buf[G * g:G * g + G, 0:2 * R].reshape(G * 2 * R, CX * CY)
        hi = flat.astype(BF16).astype(F32)
        pair = jnp.concatenate([hi, flat - hi], axis=0)
        pair = jnp.concatenate([pair[:, :128].T, pair[:, 128:].T], axis=0).astype(BF16)
        return jnp.concatenate([pair, pair[:, :64]], axis=1)

    def z_apply(f, halo, mat, v):
        hi, lo = split(f)
        both = dot(jnp.concatenate([hi, halo[0]], axis=1), mat[v])
        rest = dot(jnp.concatenate([lo, halo[1]], axis=1), mat[v, :, 0:128])
        return both[:, :128] + both[:, 128:] + rest

    halo = split(g_buf[V].reshape(CX * CY, CZ))
    for g in range(V // G):
        ratios = []
        for v in range(G * g, G * g + G):
            blurred = z_apply(g_buf[v].reshape(CX * CY, CZ), halo, zf_mat, v)
            ratio = o_buf[v].reshape(CX * CY, CZ) / blurred
            r_buf[v] = ratio.reshape(CX, CY, CZ)
            ratios.append(ratio)
        send_edges(ratios, g)

    total = jnp.zeros((8, CZ), F32)
    outside = jnp.zeros((CX * CY, CZ), F32)
    for v in range(V):
        hi, lo = split(r_buf[v].reshape(CX * CY, CZ))
        f = dot(jnp.concatenate([hi, lo], axis=1), zm_mat[v, 0:256]) + dot(hi, zm_mat[v, 256:384])
        g_buf[v] = f[:, :128].reshape(CX, CY, CZ)
        outside = outside + f[:, 128:]
        weighed = f[:, :128] * b_buf[v].reshape(CX * CY, CZ)
        total = total + jnp.sum(weighed.reshape(CX * CY // 8, 8, CZ), axis=0)
    for b in range(4):
        halo_share(b)
    for b in range(4):
        halo_y(b, m_buf)
    forward_x(range(EX), True, m_buf, b_buf, V, 0)
    weighed = outside * b_buf[V].reshape(CX * CY, CZ)
    total = total + jnp.sum(weighed.reshape(CX * CY // 8, 8, CZ), axis=0)
    lane1 = lax.broadcasted_iota(jnp.int32, (1, CZ), 1)

    def summed(f):
        return jnp.sum(jnp.sum(f, axis=0, keepdims=True), axis=1, keepdims=True)

    red_own[0] = jnp.where(lane1 < CZ // 2, summed(seen_buf[...]), summed(total))

    by_hi, by_lo = lax.div(ids["by"], 4), lax.rem(ids["by"], 4)

    def red_peer(stage, d):
        if stage == 0:
            return {
                "bx": lax.rem(ids["bx"] + d % 4, 4),
                "by": lax.rem(by_hi + d // 4, 2) * 4 + by_lo,
            }
        return {
            "bz": lax.rem(ids["bz"] + d % 4, 4),
            "by": by_hi * 4 + lax.rem(by_lo + d // 4, 4),
        }

    def red_copy(stage, d):
        return pltpu.make_async_remote_copy(
            src_ref=red_own.at[stage], dst_ref=red_in.at[stage, d],
            send_sem=red_send.at[stage], recv_sem=red_recv.at[stage],
            device_id=red_peer(stage, d), device_id_type=MESH,
        )

    def red_start(stage):
        for d in range(1, STAGES[stage]):
            red_copy(stage, d).start()

    def red_all(stage):
        every = red_in.at[stage, pl.ds(1, STAGES[stage] - 1)]
        return pltpu.make_async_remote_copy(
            src_ref=every, dst_ref=every, send_sem=red_send.at[stage],
            recv_sem=red_recv.at[stage], device_id=red_peer(stage, 1), device_id_type=MESH,
        )

    def red_finish(stage):
        red_all(stage).wait_recv()
        total = red_own[stage]
        for d in range(1, STAGES[stage]):
            total = total + red_in[stage, d]
        return total

    met(met_sem.at[2], ROUNDS[3])
    red_start(0)
    for v in range(V):
        q4 = jnp.concatenate(
            [jnp.where(band // 32 == i // 2, bands[v], 0.0) for i in range(8)], axis=0
        ).T
        pair = split(q4)
        for xb in range(3):
            w = [jnp.broadcast_to(w_buf[xb, yb, v:v + 1], (8, CZ)) for yb in (0, 1, 1, 2)]
            w = jnp.concatenate(w * 4, axis=0).astype(BF16)
            for i in range(2):
                yb_mat[xb, v, :, 128 * i:128 * i + 128] = pair[i] * w

    def backward_x(v):
        pairs = [split(g_buf[v, :, 8 * h:8 * h + 8, :].reshape(128, CZ)) for h in range(2)]
        data = jnp.concatenate([jnp.concatenate(p, axis=0) for p in pairs], axis=1)
        full = dot(xb_mat[v, :, 0:256], data) + dot(xb_mat[v, :, 256:384], data[0:128])
        planes = jnp.concatenate(
            [full[:, h * CZ:(h + 1) * CZ].reshape(EX, 8, CZ) for h in range(2)], axis=1
        )
        hi, lo = split(planes)
        x_buf[v, :, 0:CY, :] = hi
        x_buf[v, :, CY:2 * CY, :] = lo

    for g in range(V // G):
        for d in (-1, 1):
            z_copy(g, d).wait_recv()
        halo = halo_rows(g)
        for v in range(G * g, G * g + G):
            g_buf[v] = g_buf[v] + dot(halo, zh_mat[v]).reshape(CX, CY, CZ)

    for v in range(V):
        backward_x(v)

    def backward_y(x0, xb):
        full = None
        for v in range(V):
            data = []
            for h in range(2):
                planes = x_buf[v, x0 + 4 * h:x0 + 4 * h + 4].reshape(128, CZ)
                data.append(jnp.concatenate([planes, planes], axis=0))
            term = dot(yb_mat[xb, v], jnp.concatenate(data, axis=1))
            full = term if full is None else full + term
        for h in range(2):
            p_buf[x0 + 4 * h:x0 + 4 * h + 4] = full[:, h * CZ:(h + 1) * CZ].reshape(4, EY, CZ)

    backward_y(0, 0)
    backward_y(EX - 8, 2)
    for dx in (-1, 1):
        @pl.when(twin(dx))
        def _():
            p_pass(dx).start()

        @pl.when(cross(dx))
        def _():
            p_copy(dx, 0).start()
        for dy in (-1, 1):
            @pl.when(cross_both(dx, dy))
            def _():
                p_copy(dx, dy).start()
    backward_y(R, 1)
    backward_y(2 * R, 1)
    red_own[1] = red_finish(0)
    red_start(1)
    for dx in (-1, 1):
        @pl.when(twin(dx))
        def _():
            p_pass(dx).wait_recv()
            p_buf[inner[dx]] = p_buf[inner[dx]] + tp_buf[...]
    for d in (-1, 1):
        @pl.when(has("by", d))
        def _():
            p_copy(0, d).start()
    def p_arrivals(nx, ny):
        rows = 128 * ny + (128 + 64 * ny) * (nx - 1)
        group(planes_of(rp_buf, rows), p_send.at[0], p_recv.at[0]).wait_recv()

    counted(p_arrivals)
    for s in range(2):
        xs, xe = slice(R + 8 * s, R + 8 * s + 8), edge[2 * s - 1]
        for h in range(2):
            ys, ye = slice(R + 8 * h, R + 8 * h + 8), edge[2 * h - 1]
            summed = p_buf[xs, ys] + rp_buf[xe, ys] + rp_buf[xs, ye] + rp_buf[xe, ye]
            out[8 * s:8 * s + 8, 8 * h:8 * h + 8, :] = e_buf[xs, ys, :] * summed
    def departures(nx, ny):
        group(planes_of(e_buf, 128 * (nx + ny) + 64 * nx * ny), e_send.at[0], e_recv.at[0]).wait_send()
        blocks = 2 * ny + nx * (1 + ny)
        group(e_buf.at[pl.ds(0, blocks), pl.ds(0, 24)], h_send.at[0], h_recv.at[0]).wait_send()
        tiles = e_buf.at[pl.ds(0, nx + ny + nx * ny), pl.ds(0, V)]
        group(tiles, w_send.at[0], w_recv.at[0]).wait_send()
        rows = 256 + 128 * ny + (128 + 64 * ny) * (nx - 1)
        group(planes_of(e_buf, rows), p_send.at[0], p_recv.at[0]).wait_send()

    counted(departures)
    for d in (-1, 1):
        @pl.when(has("bz", d))
        def _():
            face_copy(d).wait_send()
            share_copy(d).wait_send()
    for g in range(V // G):
        for d in (-1, 1):
            z_copy(g, d).wait_send()
    red_all(0).wait_send()
    red_all(1).wait_send()
    final = red_finish(1)
    scale = final[:, 0:1] / (final[:, CZ // 2:CZ // 2 + 1] * count_own[:, 0:1])
    out[...] = out[...] * scale.reshape(1, 1, 1)


def on_device(estimate, observed, coverage, psf_taps):
    dma = pltpu.SemaphoreType.DMA
    arrays = (estimate, observed, coverage.reshape(1, V), jnp.transpose(psf_taps, (1, 0, 2)))
    return pl.pallas_call(
        kernel,
        out_shape=jax.ShapeDtypeStruct((CX, CY, CZ), F32),
        in_specs=[pl.BlockSpec(memory_space=pltpu.HBM)] * 4,
        out_specs=pl.BlockSpec(memory_space=pltpu.VMEM),
        scratch_shapes=[
            pltpu.VMEM((EX, EY, CZ), F32),
            pltpu.VMEM((V, CX, CY, CZ), F32),
            pltpu.VMEM((V + 1, EX, CY, CZ), F32),
            pltpu.VMEM((V + 1, EX, CY, CZ), F32),
            pltpu.VMEM((V + 1, CX, CY, CZ), F32),
            pltpu.VMEM((V, CX, CY, CZ), F32),
            pltpu.VMEM((V, EX, 2 * CY, CZ), BF16),
            pltpu.VMEM((EX, EY, CZ), F32),
            pltpu.VMEM((EX, EY, CZ), F32),
            pltpu.VMEM((R, EY, CZ), F32),
            pltpu.VMEM((2, 2 * R, CZ), F32),
            pltpu.VMEM((3, V, CZ), F32),
            pltpu.VMEM((4, 3, 3 * R, CZ), F32),
            pltpu.VMEM((EX, EY, CZ), F32),
            pltpu.VMEM((V, 2 * R, CX * CY), F32),
            pltpu.VMEM((V, 3 * R, CX * CY), F32),
            pltpu.VMEM((3, 3, V, CZ), F32),
            pltpu.VMEM((1, V), jnp.int32),
            pltpu.VMEM((3, V, T), F32),
            pltpu.VMEM((3 + T, 2 * V, CZ), F32),
            pltpu.VMEM((2, 4 * R, CZ), F32),
            pltpu.VMEM((V, 256, 256), BF16),
            pltpu.VMEM((V, 384, 256), BF16),
            pltpu.VMEM((V, 192, 128), BF16),
            pltpu.VMEM((V, 256, 384), BF16),
            pltpu.VMEM((V, 128, 384), BF16),
            pltpu.VMEM((V, 2 * CY, 256), BF16),
            pltpu.VMEM((3, V, 2 * CY, 256), BF16),
            pltpu.VMEM((3, V, 128, 256), BF16),
            pltpu.VMEM((V + 1, CX, CY, CZ), F32),
            pltpu.VMEM((8, CZ), F32),
            pltpu.VMEM((2, 1, CZ), F32),
            pltpu.VMEM((2, 16, 1, CZ), F32),
            dma((4,)), dma((1,)), dma((3,)), dma((1,)), dma((2,)), dma((4,)), dma((4,)), dma((1,)), dma((2,)),
            dma((2, 2)), dma((2, 2)), dma((1,)), dma((2,)), dma((2,)), dma((2,)),
            pltpu.SemaphoreType.REGULAR((3,)),
        ],
        compiler_params=pltpu.CompilerParams(
            collective_id=0, has_side_effects=True, vmem_limit_bytes=48 * 1024 * 1024
        ),
    )(*[pltpu.with_memory_space_constraint(a, pltpu.HBM) for a in arrays])


def solution(mesh):
    block = P("bx", "by", "bz")
    views = P(None, "bx", "by", "bz")
    return jax.shard_map(
        on_device, mesh=mesh, in_specs=(block, views, views, P()), out_specs=block, check_vma=False
    )
```

```python
import functools

import jax
import jax.numpy as jnp
from jax import lax
from jax.experimental import pallas as pl
from jax.experimental.pallas import tpu as pltpu
from jax.sharding import PartitionSpec as P

MESH = pl.DeviceIdType.MESH
F32 = jnp.float32
BF16 = jnp.bfloat16
V, R, T = 8, 8, 17
CX, CY, CZ = 16, 16, 128
EX, EY = CX + 2 * R, CY + 2 * R
G = 4
LINES = (("bz", 4), ("by", 8), ("bx", 4))
STAGES = (8, 16)
SIDES = tuple((x, y) for x in (-1, 0, 1) for y in (-1, 0, 1) if x or y)
ROUNDS = (
    (("bz", 1), ("by", 1), ("bx", 1)),
    (("bz", 1), ("by", 1), ("bx", 1)),
    (("bz", 2), ("by", 2), ("bx", 2)),
    (("bz", 2), ("by", 4), ("bx", 2)),
)


def split(f):
    hi = f.astype(BF16)
    lo = (f - hi.astype(F32)).astype(BF16)
    return hi, lo


def dot(a, b):
    return jnp.dot(a, b, preferred_element_type=F32)


def stack4(f):
    hi, lo = split(f)
    return jnp.concatenate([hi, lo, hi, lo], axis=0)


def kernel(
    est, obs, cov, taps, out,
    e_buf, o_buf, y_buf, m_buf, g_buf, r_buf, x_buf, p_buf, rp_buf, tp_buf,
    zt_buf, share_buf, h_buf, ht_buf, sb_buf, hb_buf, w_buf, c_buf, k_buf, t_buf, l_buf,
    zf_mat, zm_mat, zh_mat, xb_mat, xf_mat, yf_mat, yw_mat, yb_mat, b_buf, seen_buf, red_own, red_in,
    load_sem, e_send, e_recv, w_send, w_recv, f_send, f_recv, h_send, h_recv,
    zb_send, zb_recv, p_send, p_recv, red_send, red_recv, met_sem,
):
    ids = {name: lax.axis_index(name) for name, _ in LINES}
    sizes = dict(LINES)

    def at(dx, dy, dz=0):
        return {
            name: lax.rem(ids[name] + d + sizes[name], sizes[name])
            for name, d in (("bx", dx), ("by", dy), ("bz", dz)) if d
        }

    barrier = pltpu.get_barrier_semaphore()

    def has(name, d):
        return ids[name] + d >= 0 if d < 0 else ids[name] + d < sizes[name]

    def meet(sem, steps):
        for name, size in steps:
            for d in (-size, size):
                @pl.when(has(name, d))
                def _():
                    pl.semaphore_signal(
                        sem, inc=1, device_id={name: ids[name] + d}, device_id_type=MESH
                    )

    def met(sem, steps, heard=0):
        for name, size in steps:
            for d in (-size, size):
                heard = heard + jnp.where(has(name, d), 1, 0)
        pl.semaphore_wait(sem, heard)

    def twin(dx):
        return lax.rem(ids["bx"], 2) == (1 - dx) // 2

    def cross(dx):
        return jnp.logical_and(has("bx", dx), jnp.logical_not(twin(dx)))

    def cross_both(dx, dy):
        return jnp.logical_and(cross(dx), has("by", dy))

    corners = [(dx, dy) for dx in (-1, 1) for dy in (-1, 1)]
    meet(barrier, ROUNDS[0])
    greeted = 0
    for dx, dy in corners:
        near_by = jnp.logical_and(has("bx", dx), has("by", dy))
        greeted = greeted + jnp.where(near_by, 1, 0)

        @pl.when(near_by)
        def _():
            pl.semaphore_signal(barrier, inc=1, device_id=at(dx, dy), device_id_type=MESH)
    load_e = pltpu.make_async_copy(est, e_buf.at[pl.ds(R, CX), pl.ds(R, CY)], load_sem.at[0])
    load_c = pltpu.make_async_copy(cov, c_buf, load_sem.at[1])
    load_t = pltpu.make_async_copy(taps, k_buf, load_sem.at[2])
    load_o = pltpu.make_async_copy(obs, o_buf, load_sem.at[3])
    for load in (load_e, load_c, load_t, load_o):
        load.start()

    def both(dx, dy):
        if dx and dy:
            return jnp.logical_and(has("bx", dx), has("by", dy))
        return has("bx", dx) if dx else has("by", dy)

    def remote(src, dst, send, recv, device):
        return pltpu.make_async_remote_copy(
            src_ref=src, dst_ref=dst, send_sem=send, recv_sem=recv,
            device_id=device, device_id_type=MESH,
        )

    own = pl.ds(R, CX)
    edge = {-1: pl.ds(0, R), 0: own, 1: pl.ds(EX - R, R)}
    inner = {-1: pl.ds(R, R), 0: own, 1: pl.ds(CX, R)}

    def counted(act):
        ends = [
            jnp.logical_and(has(name, -1), has(name, 1)) for name in ("bx", "by")
        ]
        for nx in (1, 2):
            for ny in (1, 2):
                hit = [e if n == 2 else jnp.logical_not(e) for e, n in zip(ends, (nx, ny))]

                @pl.when(jnp.logical_and(*hit))
                def _():
                    act(nx, ny)

    def planes_of(buf, rows):
        width = 32 if rows % 32 == 0 else 24
        return buf.at[pl.ds(0, rows // width), pl.ds(0, width)]

    def group(ref, send, recv):
        return remote(ref, ref, send, recv, at(0, 0, 1))

    def e_copy(dx, dy):
        return remote(
            e_buf.at[inner[dx], inner[dy]], e_buf.at[edge[-dx], edge[-dy]],
            e_send.at[0], e_recv.at[0 if dx else (3 - dy) // 2], at(dx, dy),
        )

    def e_pass(dx, dy):
        return remote(
            e_buf.at[inner[dx], edge[dy]], e_buf.at[edge[-dx], edge[dy]],
            e_send.at[0], e_recv.at[0], at(dx, 0),
        )

    def p_copy(dx, dy):
        return remote(
            p_buf.at[edge[dx], edge[dy]], rp_buf.at[edge[-dx], edge[-dy]],
            p_send.at[0], p_recv.at[0], at(dx, dy),
        )

    def p_pass(dx):
        return remote(p_buf.at[edge[dx]], tp_buf, p_send.at[0], p_recv.at[1], at(dx, 0))

    rows = {-1: pl.ds(R, R), 1: pl.ds(0, R)}
    to_rows = {-1: pl.ds(R, R), 1: pl.ds(0, R)}

    def face_copy(dz):
        return remote(
            zt_buf.at[:, rows[dz]], h_buf.at[pl.ds(1, 2), 1, to_rows[dz]],
            f_send.at[(1 + dz) // 2], f_recv.at[(1 - dz) // 2], at(0, 0, dz),
        )

    def share_copy(dz):
        return remote(
            share_buf.at[2], share_buf.at[(1 - dz) // 2],
            f_send.at[2 + (1 + dz) // 2], f_recv.at[2 + (1 - dz) // 2], at(0, 0, dz),
        )

    def h_copy(dx, dy):
        src = {-1: pl.ds(1, 1), 0: pl.ds(1, 2), 1: pl.ds(2, 1)}[dx]
        dst = {-1: pl.ds(3, 1), 0: pl.ds(1, 2), 1: pl.ds(0, 1)}[dx]
        return remote(
            h_buf.at[src, 1], h_buf.at[dst, 1 - dy],
            h_send.at[0], h_recv.at[1 if dx else 0], at(dx, dy),
        )

    def w_copy(dx, dy):
        return remote(
            w_buf.at[1, 1], w_buf.at[1 - dx, 1 - dy],
            w_send.at[0], w_recv.at[1 if dx else 0], at(dx, dy),
        )

    def z_copy(g, dz):
        views = pl.ds(G * g, G)
        bz, n = ids["bz"], sizes["bz"]
        place = 1 + (bz + 1) // n if dz > 0 else 2 * ((n - bz) // n)
        side = (dz + 1) // 2
        return remote(
            sb_buf.at[views, rows[dz]], hb_buf.at[views, pl.ds(pl.multiple_of(R * place, R), R)],
            zb_send.at[g, side], zb_recv.at[g, 1 - side], at(0, 0, dz),
        )

    part = functools.partial

    for d in (-1, 1):
        @pl.when(jnp.logical_not(has("by", d)))
        def _():
            e_buf[:, edge[d], :] = jnp.zeros((EX, R, CZ), F32)
            rp_buf[:, edge[d], :] = jnp.zeros((EX, R, CZ), F32)
            h_buf[:, 1 + d] = jnp.zeros((4, 3 * R, CZ), F32)
            w_buf[:, 1 + d] = jnp.zeros((3, V, CZ), F32)

        @pl.when(jnp.logical_not(has("bx", d)))
        def _():
            e_buf[edge[d]] = jnp.zeros((R, EY, CZ), F32)
            h_buf[3 * (1 + d) // 2] = jnp.zeros((3, 3 * R, CZ), F32)
            w_buf[1 + d] = jnp.zeros((3, V, CZ), F32)

        @pl.when(jnp.logical_not(cross(d)))
        def _():
            rp_buf[edge[d]] = jnp.zeros((R, EY, CZ), F32)

        @pl.when(jnp.logical_not(has("bz", d)))
        def _():
            hb_buf[:, rows[d], :] = jnp.zeros((V, R, CX * CY), F32)
            h_buf[1:3, 1, to_rows[-d], :] = jnp.zeros((2, R, CZ), F32)
            share_buf[(1 + d) // 2] = jnp.zeros((V, CZ), F32)

    row8 = lax.broadcasted_iota(jnp.int32, (V, CZ), 0)
    lane8 = lax.broadcasted_iota(jnp.int32, (V, CZ), 1)
    load_c.wait()
    flags = jnp.broadcast_to(c_buf[...].astype(F32), (V, V))
    picked = jnp.where(row8[:, :V] == lane8[:, :V], flags, 0.0)
    weight = jnp.broadcast_to(jnp.sum(picked, axis=1, keepdims=True), (V, CZ))
    w_buf[1, 1] = weight
    share_buf[2] = weight / jnp.sum(weight, axis=0, keepdims=True)
    load_e.wait()
    planes = e_buf[own, own].reshape(CX * CY, CZ)
    for h in range(2):
        flipped = planes[128 * h:128 * h + 128].T
        zt_buf[h, 0:R] = flipped[CZ - R:]
        zt_buf[h, R:2 * R] = flipped[:R]
    met(barrier, ROUNDS[0], greeted)
    meet(met_sem.at[0], ROUNDS[1])
    for d in (-1, 1):
        @pl.when(has("bz", d))
        def _():
            face_copy(d).start()
            share_copy(d).start()
    for dx, dy in SIDES:
        @pl.when(both(dx, dy))
        def _():
            w_copy(dx, dy).start()
    for d in (-1, 1):
        @pl.when(has("bx", d))
        def _():
            e_copy(d, 0).start()
    for d in (-1, 1):
        @pl.when(has("by", d))
        def _():
            e_copy(0, d).start()
    for dx, dy in corners:
        @pl.when(cross_both(dx, dy))
        def _():
            e_copy(dx, dy).start()

    load_t.wait()
    t_buf[...] = jnp.zeros_like(t_buf)
    for d in range(3):
        t_buf[d, 0:V, 0:T] = k_buf[d]
    taps_x, taps_y, taps_z = (
        t_buf[d, 0:V] / jnp.sum(t_buf[d, 0:V], axis=1, keepdims=True) for d in range(3)
    )
    for k, table in enumerate((taps_x, taps_y)):
        wide = jnp.concatenate(
            [jnp.broadcast_to(table[v:v + 1], (2 * R, CZ)) for v in range(V)], axis=0
        ).T
        l_buf[k] = wide[:4 * R]
    taps_y = taps_y + pltpu.roll(taps_y, 32, 1)
    taps_y = taps_y + pltpu.roll(taps_y, 64, 1)
    band = lax.broadcasted_iota(jnp.int32, (CY, 128), 1)
    bands = []
    for v in range(V):
        q = pltpu.roll(
            jnp.broadcast_to(taps_y[v:v + 1], (CY, 128)), 0, 1, stride=1, stride_axis=0
        )
        bands.append(q)
        q_hi, q_lo = split(q)
        zero = jnp.zeros_like(q_hi)
        for x in range(2):
            mine = (band // 32) % 2 == x
            yf_mat[v, x * CY:(x + 1) * CY, 0:128] = jnp.where(mine, q_hi, zero)
            yf_mat[v, x * CY:(x + 1) * CY, 128:256] = jnp.where(mine, q_lo, zero)
    for k in range(T):
        t_buf[3 + k, 0:V] = jnp.broadcast_to(taps_x[:, k:k + 1], (V, CZ))
        t_buf[3 + k, V:2 * V] = jnp.broadcast_to(l_buf[0, k:k + 1], (V, CZ))

    lane = lax.broadcasted_iota(jnp.int32, (128, 128), 1)
    row = lax.broadcasted_iota(jnp.int32, (128, 128), 0)
    near = jnp.abs(row - lane) <= R
    zf_mat[:, 128:256, :] = jnp.zeros((V, 128, 256), BF16)
    zh_mat[...] = jnp.zeros_like(zh_mat)
    for v in range(V):
        ring = pltpu.roll(
            jnp.broadcast_to(taps_z[v:v + 1], (128, 128)), 128 - R, 1, stride=1, stride_axis=0
        )
        ahead = ring.T
        m_hi, m_lo = split(jnp.where(near, ahead, 0.0))
        zf_mat[v, 0:128, 0:128] = m_hi
        zf_mat[v, 0:128, 128:256] = m_lo
        far = jnp.where(near, 0.0, ahead)
        f_hi, f_lo = split(jnp.concatenate([far[128 - R:128], far[0:R]], axis=0))
        top = 128 + 2 * R * v
        zf_mat[v, top:top + 2 * R, 0:128] = f_hi
        zf_mat[v, top:top + 2 * R, 128:256] = f_lo
        m_hi, m_lo = split(jnp.where(near, ring, 0.0))
        far = jnp.where(near, 0.0, ring)
        s_hi, s_lo = split(pltpu.roll(far, (2 * R * v + R) % 128, 1))
        for i in range(2):
            zm_mat[v, 128 * i:128 * i + 128, 0:128] = m_hi
            zm_mat[v, 128 * i:128 * i + 128, 128:256] = s_hi
        zm_mat[v, 256:384, 0:128] = m_lo
        zm_mat[v, 256:384, 128:256] = s_lo
        f_hi, f_lo = split(jnp.concatenate([far[0:R], far[128 - R:128]], axis=0))
        top = 2 * R * (v % G)
        zh_mat[v, top:top + 2 * R] = f_hi
        zh_mat[v, 64 + top:64 + top + 2 * R] = f_hi
        zh_mat[v, 128 + top:128 + top + 2 * R] = f_lo

    sparse = jnp.zeros((V, CZ), F32)
    for k in range(T - 1):
        sparse = sparse + jnp.where(lane8 == 8 * k, t_buf[3 + k, 0:V], 0.0)
    for v in range(V):
        turned = pltpu.roll(jnp.broadcast_to(sparse[v:v + 1], (128, 128)), 0, 1, stride=1, stride_axis=0)
        last = jnp.broadcast_to(t_buf[2 + T, v:v + 1], (128, 128))
        low = jnp.where(lane >= row, turned, 0.0)
        high = jnp.where(lane < row, turned, jnp.where(lane == row, last, 0.0))
        for i, tile in enumerate((low, high)):
            k_hi, k_lo = split(tile.T)
            xb_mat[v, 128 * i:128 * i + 128, 0:128] = k_hi
            xb_mat[v, 128 * i:128 * i + 128, 128:256] = k_hi
            xb_mat[v, 128 * i:128 * i + 128, 256:384] = k_lo
        k_hi, k_lo = split(jnp.where(lane < 64, pltpu.roll(low, 64, 1), pltpu.roll(high, 64, 1)))
        xf_mat[0, v, :, 0:128] = k_hi
        xf_mat[0, v, :, 128:256] = k_hi
        xf_mat[0, v, :, 256:384] = k_lo
        k_hi, k_lo = split(jnp.where(lane < 64, low, high))
        xf_mat[1, v, :, 0:128] = k_hi
        xf_mat[1, v, :, 128:256] = k_hi
        xf_mat[1, v, :, 256:384] = k_lo

    load_o.wait()
    seen = jnp.zeros((8, CZ), F32)
    for v in range(V):
        seen = seen + w_buf[1, 1, v:v + 1] * jnp.sum(o_buf[v].reshape(CX * CY // 8, 8, CZ), axis=0)
    count_own = jnp.sum(w_buf[1, 1], axis=0, keepdims=True)
    seen_buf[...] = seen / count_own

    for d in (-1, 1):
        @pl.when(has("bz", d))
        def _():
            face_copy(-d).wait_recv()
            share_copy(-d).wait_recv()
    for b in (1, 2):
        h_buf[b, 1, 2 * R:] = jnp.where(lane8 < CZ // 2, share_buf[0], share_buf[1])
    met(met_sem.at[0], ROUNDS[1])
    meet(met_sem.at[1], ROUNDS[2])
    for dx, dy in SIDES:
        @pl.when(both(dx, dy))
        def _():
            h_copy(dx, dy).start()
    for d in (-1, 1):
        @pl.when(has("by", d))
        def _():
            e_copy(0, -d).wait_recv()
            for dx in (-1, 1):
                @pl.when(twin(dx))
                def _():
                    e_pass(dx, d).start()

    def forward_y(x0, source=e_buf, mat=yf_mat, to=y_buf):
        data = jnp.concatenate(
            [stack4(source[pl.ds(x0 + 2 * h, 2)].reshape(2 * EY, CZ)) for h in range(2)], axis=1
        )
        full = dot(mat[...].reshape(V * 2 * CY, 256), data)
        for h in range(2):
            to[0:V, pl.ds(x0 + 2 * h, 2)] = full[:, h * CZ:(h + 1) * CZ].reshape(V, 2, CY, CZ)

    for x0 in range(R, R + CX, 4):
        forward_y(x0)

    def x_taps(v):
        return [jnp.broadcast_to(t_buf[3 + k, pl.ds(v, 1), :], (8, CZ)) for k in range(T)]

    def forward_x(inputs, first, y_buf, g_buf, v, carry):
        t = x_taps(v)
        for h in range(CY // 8):
            ys = pl.ds(8 * h, 8)
            acc = [None if first else g_buf[v, xo, ys, :] for xo in range(CX)]
            for xi in inputs:
                val = y_buf[v, xi, ys, :]
                for xo in range(max(0, xi - T + 1), min(CX, xi + 1)):
                    term = t[xi - xo] * val
                    acc[xo] = term if acc[xo] is None else acc[xo] + term
            for xo in range(CX):
                g_buf[v, xo, ys, :] = acc[xo]
        return carry

    y_spans = ((0, slice(R, CY), slice(0, R)), (1, slice(0, CY), slice(R, R + CY)),
               (2, slice(0, R), slice(R + CY, EY)))

    def halo_in(b):
        for yb, part_of, ys in y_spans:
            tile = jnp.concatenate([h_buf[b, yb, :2 * R]] * V, axis=0).T.reshape(R, CY, CZ)
            ht_buf[R * b:R * b + R, ys] = tile[:, part_of]

    def halo_share(b):
        for yb, _, ys in y_spans:
            tile = h_buf[b, yb, 2 * R:]
            before = jnp.broadcast_to(tile[:, 0:1], (V, CZ))
            after = jnp.broadcast_to(tile[:, CZ // 2:CZ // 2 + 1], (V, CZ))
            share = jnp.where(lane8 % (2 * R) < R, before, after)
            share = jnp.sum(jnp.where(lane8 // (2 * R) == row8, share, 0.0), axis=0, keepdims=True)
            at_x = slice(R * b, R * b + R)
            ht_buf[at_x, ys] = ht_buf[at_x, ys] * share

    def halo_y(b, to):
        t = [jnp.broadcast_to(l_buf[1, k:k + 1, :], (8, CZ)) for k in range(T)]
        for x in range(R * b, R * b + R):
            for h in range(2):
                acc = None
                for k in range(T):
                    term = t[k] * ht_buf[x, 8 * h + k:8 * h + k + 8, :]
                    acc = term if acc is None else acc + term
                to[V, x, 8 * h:8 * h + 8, :] = acc

    third = (band % 32)[:8]
    spans = ((0, R), (R, R + CX), (R + CX, EX))

    def mask(xb):
        xs = slice(*spans[xb])
        for yb in range(3):
            ys = slice(*spans[yb])
            count = jnp.maximum(jnp.sum(w_buf[xb, yb], axis=0, keepdims=True), 1.0)
            p_buf[xs, ys] = e_buf[xs, ys] * (1.0 / count)
        w = jnp.where(third < R, w_buf[xb, 0], jnp.where(third < R + CY, w_buf[xb, 1], w_buf[xb, 2]))
        for v in range(V):
            wide = jnp.broadcast_to(w[v:v + 1], (2 * CY, CZ)).astype(BF16)
            for i in range(2):
                cols = slice(128 * i, 128 * i + 128)
                yw_mat[xb, v, :, cols] = yf_mat[v, :, cols] * wide


    def planes_x(source, to, halo):
        for v in range(V):
            pairs = []
            for h in range(2):
                ys = slice(8 * h, 8 * h + 8)
                if halo:
                    f = jnp.concatenate([source[v, 0:R, ys], source[v, EX - R:EX, ys]], axis=0)
                else:
                    f = source[v, R:R + CX, ys]
                pairs.append(jnp.concatenate(split(f.reshape(128, CZ)), axis=0))
            data = jnp.concatenate(pairs, axis=1)
            mat = xf_mat.at[halo, v]
            full = dot(mat[:, 0:256], data) + dot(mat[:, 256:384], data[0:128])
            for h in range(2):
                ys = slice(8 * h, 8 * h + 8)
                f = full[:, h * CZ:(h + 1) * CZ].reshape(CX, 8, CZ)
                to[v, :, ys, :] = to[v, :, ys, :] + f if halo else f

    planes_x(y_buf, g_buf, 0)
    halo_planes = tuple(range(R)) + tuple(range(R + CX, EX))

    def masked_y(xb):
        mask(xb)
        for x0 in range(spans[xb][0], spans[xb][1], 4):
            forward_y(x0, p_buf, yw_mat.at[xb], m_buf)

    def w_arrivals(nx, ny):
        group(w_buf.at[0, pl.ds(0, ny)], w_send.at[0], w_recv.at[0]).wait_recv()

    counted(w_arrivals)
    masked_y(1)
    planes_x(m_buf, b_buf, 0)
    def x_arrivals(nx, ny):
        group(planes_of(e_buf, nx * (128 + 64 * ny)), e_send.at[0], e_recv.at[0]).wait_recv()
        tiles = w_buf.at[pl.ds(0, nx), pl.ds(0, 3)] if ny == 2 else w_buf.at[pl.ds(0, 2), pl.ds(0, nx)]
        group(tiles, w_send.at[0], w_recv.at[1]).wait_recv()

    counted(x_arrivals)
    for x0 in (0, 4, EX - 8, EX - 4):
        forward_y(x0)
    planes_x(y_buf, g_buf, 1)
    masked_y(0)
    masked_y(2)
    planes_x(m_buf, b_buf, 1)
    met(met_sem.at[1], ROUNDS[2])
    meet(met_sem.at[2], ROUNDS[3])

    def h_arrivals(nx, ny):
        group(h_buf.at[pl.ds(0, 2 * ny), 0], h_send.at[0], h_recv.at[0]).wait_recv()
        blocks = {2: pl.ds(0, nx), 1: pl.ds(0, 2 * nx)}[ny]
        cols = pl.ds(0, 3) if ny == 2 else 0
        group(h_buf.at[blocks, cols], h_send.at[0], h_recv.at[1]).wait_recv()

    counted(h_arrivals)
    for b in range(4):
        halo_in(b)
    for b in range(4):
        halo_y(b, y_buf)
    forward_x(range(EX), True, y_buf, g_buf, V, 0)

    def send_edges(fields, g):
        for v, f in zip(range(G * g, G * g + G), fields):
            for h in range(2):
                flipped = f[128 * h:128 * h + 128].T
                sb_buf[v, 0:R, 128 * h:128 * h + 128] = flipped[CZ - R:]
                sb_buf[v, R:2 * R, 128 * h:128 * h + 128] = flipped[:R]
        for d in (-1, 1):
            z_copy(g, d).start()

    def halo_rows(g):
        flat = hb_buf[G * g:G * g + G, 0:2 * R].reshape(G * 2 * R, CX * CY)
        hi = flat.astype(BF16).astype(F32)
        pair = jnp.concatenate([hi, flat - hi], axis=0)
        pair = jnp.concatenate([pair[:, :128].T, pair[:, 128:].T], axis=0).astype(BF16)
        return jnp.concatenate([pair, pair[:, :64]], axis=1)

    def z_apply(f, halo, mat, v):
        hi, lo = split(f)
        both = dot(jnp.concatenate([hi, halo[0]], axis=1), mat[v])
        rest = dot(jnp.concatenate([lo, halo[1]], axis=1), mat[v, :, 0:128])
        return both[:, :128] + both[:, 128:] + rest

    halo = split(g_buf[V].reshape(CX * CY, CZ))
    for g in range(V // G):
        ratios = []
        for v in range(G * g, G * g + G):
            blurred = z_apply(g_buf[v].reshape(CX * CY, CZ), halo, zf_mat, v)
            ratio = o_buf[v].reshape(CX * CY, CZ) / blurred
            r_buf[v] = ratio.reshape(CX, CY, CZ)
            ratios.append(ratio)
        send_edges(ratios, g)

    total = jnp.zeros((8, CZ), F32)
    outside = jnp.zeros((CX * CY, CZ), F32)
    for v in range(V):
        hi, lo = split(r_buf[v].reshape(CX * CY, CZ))
        f = dot(jnp.concatenate([hi, lo], axis=1), zm_mat[v, 0:256]) + dot(hi, zm_mat[v, 256:384])
        g_buf[v] = f[:, :128].reshape(CX, CY, CZ)
        outside = outside + f[:, 128:]
        weighed = f[:, :128] * b_buf[v].reshape(CX * CY, CZ)
        total = total + jnp.sum(weighed.reshape(CX * CY // 8, 8, CZ), axis=0)
    for b in range(4):
        halo_share(b)
    for b in range(4):
        halo_y(b, m_buf)
    forward_x(range(EX), True, m_buf, b_buf, V, 0)
    weighed = outside * b_buf[V].reshape(CX * CY, CZ)
    total = total + jnp.sum(weighed.reshape(CX * CY // 8, 8, CZ), axis=0)
    lane1 = lax.broadcasted_iota(jnp.int32, (1, CZ), 1)

    def summed(f):
        return jnp.sum(jnp.sum(f, axis=0, keepdims=True), axis=1, keepdims=True)

    red_own[0] = jnp.where(lane1 < CZ // 2, summed(seen_buf[...]), summed(total))

    by_hi, by_lo = lax.div(ids["by"], 4), lax.rem(ids["by"], 4)

    def red_peer(stage, d):
        if stage == 0:
            return {
                "bx": lax.rem(ids["bx"] + d % 4, 4),
                "by": lax.rem(by_hi + d // 4, 2) * 4 + by_lo,
            }
        return {
            "bz": lax.rem(ids["bz"] + d % 4, 4),
            "by": by_hi * 4 + lax.rem(by_lo + d // 4, 4),
        }

    def red_copy(stage, d):
        return pltpu.make_async_remote_copy(
            src_ref=red_own.at[stage], dst_ref=red_in.at[stage, d],
            send_sem=red_send.at[stage], recv_sem=red_recv.at[stage],
            device_id=red_peer(stage, d), device_id_type=MESH,
        )

    def red_start(stage):
        for d in range(1, STAGES[stage]):
            red_copy(stage, d).start()

    def red_all(stage):
        every = red_in.at[stage, pl.ds(1, STAGES[stage] - 1)]
        return pltpu.make_async_remote_copy(
            src_ref=every, dst_ref=every, send_sem=red_send.at[stage],
            recv_sem=red_recv.at[stage], device_id=red_peer(stage, 1), device_id_type=MESH,
        )

    def red_finish(stage):
        red_all(stage).wait_recv()
        total = red_own[stage]
        for d in range(1, STAGES[stage]):
            total = total + red_in[stage, d]
        return total

    met(met_sem.at[2], ROUNDS[3])
    red_start(0)
    for v in range(V):
        q4 = jnp.concatenate(
            [jnp.where(band // 32 == i // 2, bands[v], 0.0) for i in range(8)], axis=0
        ).T
        pair = split(q4)
        for xb in range(3):
            w = [jnp.broadcast_to(w_buf[xb, yb, v:v + 1], (8, CZ)) for yb in (0, 1, 1, 2)]
            w = jnp.concatenate(w * 4, axis=0).astype(BF16)
            for i in range(2):
                yb_mat[xb, v, :, 128 * i:128 * i + 128] = pair[i] * w

    def backward_x(v):
        pairs = [split(g_buf[v, :, 8 * h:8 * h + 8, :].reshape(128, CZ)) for h in range(2)]
        data = jnp.concatenate([jnp.concatenate(p, axis=0) for p in pairs], axis=1)
        full = dot(xb_mat[v, :, 0:256], data) + dot(xb_mat[v, :, 256:384], data[0:128])
        planes = jnp.concatenate(
            [full[:, h * CZ:(h + 1) * CZ].reshape(EX, 8, CZ) for h in range(2)], axis=1
        )
        hi, lo = split(planes)
        x_buf[v, :, 0:CY, :] = hi
        x_buf[v, :, CY:2 * CY, :] = lo

    for g in range(V // G):
        for d in (-1, 1):
            z_copy(g, d).wait_recv()
        halo = halo_rows(g)
        for v in range(G * g, G * g + G):
            g_buf[v] = g_buf[v] + dot(halo, zh_mat[v]).reshape(CX, CY, CZ)

    for v in range(V):
        backward_x(v)

    def backward_y(x0, xb):
        full = None
        for v in range(V):
            data = []
            for h in range(2):
                planes = x_buf[v, x0 + 4 * h:x0 + 4 * h + 4].reshape(128, CZ)
                data.append(jnp.concatenate([planes, planes], axis=0))
            term = dot(yb_mat[xb, v], jnp.concatenate(data, axis=1))
            full = term if full is None else full + term
        for h in range(2):
            p_buf[x0 + 4 * h:x0 + 4 * h + 4] = full[:, h * CZ:(h + 1) * CZ].reshape(4, EY, CZ)

    backward_y(0, 0)
    backward_y(EX - 8, 2)
    for dx in (-1, 1):
        @pl.when(twin(dx))
        def _():
            p_pass(dx).start()

        @pl.when(cross(dx))
        def _():
            p_copy(dx, 0).start()
        for dy in (-1, 1):
            @pl.when(cross_both(dx, dy))
            def _():
                p_copy(dx, dy).start()
    backward_y(R, 1)
    backward_y(2 * R, 1)
    red_own[1] = red_finish(0)
    red_start(1)
    for dx in (-1, 1):
        @pl.when(twin(dx))
        def _():
            p_pass(dx).wait_recv()
            p_buf[inner[dx]] = p_buf[inner[dx]] + tp_buf[...]
    for d in (-1, 1):
        @pl.when(has("by", d))
        def _():
            p_copy(0, d).start()
    def p_arrivals(nx, ny):
        rows = 128 * ny + (128 + 64 * ny) * (nx - 1)
        group(planes_of(rp_buf, rows), p_send.at[0], p_recv.at[0]).wait_recv()

    counted(p_arrivals)
    for s in range(2):
        xs, xe = slice(R + 8 * s, R + 8 * s + 8), edge[2 * s - 1]
        for h in range(2):
            ys, ye = slice(R + 8 * h, R + 8 * h + 8), edge[2 * h - 1]
            summed = p_buf[xs, ys] + rp_buf[xe, ys] + rp_buf[xs, ye] + rp_buf[xe, ye]
            out[8 * s:8 * s + 8, 8 * h:8 * h + 8, :] = e_buf[xs, ys, :] * summed
    def departures(nx, ny):
        group(planes_of(e_buf, 128 * (nx + ny) + 64 * nx * ny), e_send.at[0], e_recv.at[0]).wait_send()
        blocks = 2 * ny + nx * (1 + ny)
        group(e_buf.at[pl.ds(0, blocks), pl.ds(0, 24)], h_send.at[0], h_recv.at[0]).wait_send()
        tiles = e_buf.at[pl.ds(0, nx + ny + nx * ny), pl.ds(0, V)]
        group(tiles, w_send.at[0], w_recv.at[0]).wait_send()
        rows = 256 + 128 * ny + (128 + 64 * ny) * (nx - 1)
        group(planes_of(e_buf, rows), p_send.at[0], p_recv.at[0]).wait_send()

    counted(departures)
    for d in (-1, 1):
        @pl.when(has("bz", d))
        def _():
            face_copy(d).wait_send()
            share_copy(d).wait_send()
    for g in range(V // G):
        for d in (-1, 1):
            z_copy(g, d).wait_send()
    red_all(0).wait_send()
    red_all(1).wait_send()
    final = red_finish(1)
    scale = final[:, 0:1] / (final[:, CZ // 2:CZ // 2 + 1] * count_own[:, 0:1])
    out[...] = out[...] * scale.reshape(1, 1, 1)


def on_device(estimate, observed, coverage, psf_taps):
    dma = pltpu.SemaphoreType.DMA
    arrays = (estimate, observed, coverage.reshape(1, V), jnp.transpose(psf_taps, (1, 0, 2)))
    return pl.pallas_call(
        kernel,
        out_shape=jax.ShapeDtypeStruct((CX, CY, CZ), F32),
        in_specs=[pl.BlockSpec(memory_space=pltpu.HBM)] * 4,
        out_specs=pl.BlockSpec(memory_space=pltpu.VMEM),
        scratch_shapes=[
            pltpu.VMEM((EX, EY, CZ), F32),
            pltpu.VMEM((V, CX, CY, CZ), F32),
            pltpu.VMEM((V + 1, EX, CY, CZ), F32),
            pltpu.VMEM((V + 1, EX, CY, CZ), F32),
            pltpu.VMEM((V + 1, CX, CY, CZ), F32),
            pltpu.VMEM((V, CX, CY, CZ), F32),
            pltpu.VMEM((V, EX, 2 * CY, CZ), BF16),
            pltpu.VMEM((EX, EY, CZ), F32),
            pltpu.VMEM((EX, EY, CZ), F32),
            pltpu.VMEM((R, EY, CZ), F32),
            pltpu.VMEM((2, 2 * R, CZ), F32),
            pltpu.VMEM((3, V, CZ), F32),
            pltpu.VMEM((4, 3, 3 * R, CZ), F32),
            pltpu.VMEM((EX, EY, CZ), F32),
            pltpu.VMEM((V, 2 * R, CX * CY), F32),
            pltpu.VMEM((V, 3 * R, CX * CY), F32),
            pltpu.VMEM((3, 3, V, CZ), F32),
            pltpu.VMEM((1, V), jnp.int32),
            pltpu.VMEM((3, V, T), F32),
            pltpu.VMEM((3 + T, 2 * V, CZ), F32),
            pltpu.VMEM((2, 4 * R, CZ), F32),
            pltpu.VMEM((V, 256, 256), BF16),
            pltpu.VMEM((V, 384, 256), BF16),
            pltpu.VMEM((V, 192, 128), BF16),
            pltpu.VMEM((V, 256, 384), BF16),
            pltpu.VMEM((2, V, 128, 384), BF16),
            pltpu.VMEM((V, 2 * CY, 256), BF16),
            pltpu.VMEM((3, V, 2 * CY, 256), BF16),
            pltpu.VMEM((3, V, 128, 256), BF16),
            pltpu.VMEM((V + 1, CX, CY, CZ), F32),
            pltpu.VMEM((8, CZ), F32),
            pltpu.VMEM((2, 1, CZ), F32),
            pltpu.VMEM((2, 16, 1, CZ), F32),
            dma((4,)), dma((1,)), dma((3,)), dma((1,)), dma((2,)), dma((4,)), dma((4,)), dma((1,)), dma((2,)),
            dma((2, 2)), dma((2, 2)), dma((1,)), dma((2,)), dma((2,)), dma((2,)),
            pltpu.SemaphoreType.REGULAR((3,)),
        ],
        compiler_params=pltpu.CompilerParams(
            collective_id=0, has_side_effects=True, vmem_limit_bytes=48 * 1024 * 1024
        ),
    )(*[pltpu.with_memory_space_constraint(a, pltpu.HBM) for a in arrays])


def solution(mesh):
    block = P("bx", "by", "bz")
    views = P(None, "bx", "by", "bz")
    return jax.shard_map(
        on_device, mesh=mesh, in_specs=(block, views, views, P()), out_specs=block, check_vma=False
    )
```

```python
import functools

import jax
import jax.numpy as jnp
from jax import lax
from jax.experimental import pallas as pl
from jax.experimental.pallas import tpu as pltpu
from jax.sharding import PartitionSpec as P

MESH = pl.DeviceIdType.MESH
F32 = jnp.float32
BF16 = jnp.bfloat16
V, R, T = 8, 8, 17
CX, CY, CZ = 16, 16, 128
EX, EY = CX + 2 * R, CY + 2 * R
G = 4
LINES = (("bz", 4), ("by", 8), ("bx", 4))
STAGES = (8, 16)
SIDES = tuple((x, y) for x in (-1, 0, 1) for y in (-1, 0, 1) if x or y)
ROUNDS = (
    (("bz", 1), ("by", 1), ("bx", 1)),
    (("bz", 1), ("by", 1), ("bx", 1)),
    (("bz", 2), ("by", 2), ("bx", 2)),
    (("bz", 2), ("by", 4), ("bx", 2)),
)


def split(f):
    hi = f.astype(BF16)
    lo = (f - hi.astype(F32)).astype(BF16)
    return hi, lo


def dot(a, b):
    return jnp.dot(a, b, preferred_element_type=F32)


def stack4(f):
    hi, lo = split(f)
    return jnp.concatenate([hi, lo, hi, lo], axis=0)


def kernel(
    est, obs, cov, taps, out,
    e_buf, o_buf, y_buf, m_buf, g_buf, r_buf, x_buf, p_buf, rp_buf, tp_buf,
    zt_buf, share_buf, h_buf, ht_buf, sb_buf, hb_buf, w_buf, c_buf, k_buf, t_buf, l_buf,
    zf_mat, zm_mat, zh_mat, xb_mat, xf_mat, yf_mat, yw_mat, yb_mat, b_buf, seen_buf, red_own, red_in,
    load_sem, e_send, e_recv, w_send, w_recv, f_send, f_recv, h_send, h_recv,
    zb_send, zb_recv, p_send, p_recv, red_send, red_recv, met_sem,
):
    ids = {name: lax.axis_index(name) for name, _ in LINES}
    sizes = dict(LINES)

    def at(dx, dy, dz=0):
        return {
            name: lax.rem(ids[name] + d + sizes[name], sizes[name])
            for name, d in (("bx", dx), ("by", dy), ("bz", dz)) if d
        }

    barrier = pltpu.get_barrier_semaphore()

    def has(name, d):
        return ids[name] + d >= 0 if d < 0 else ids[name] + d < sizes[name]

    def meet(sem, steps):
        for name, size in steps:
            for d in (-size, size):
                @pl.when(has(name, d))
                def _():
                    pl.semaphore_signal(
                        sem, inc=1, device_id={name: ids[name] + d}, device_id_type=MESH
                    )

    def met(sem, steps, heard=0):
        for name, size in steps:
            for d in (-size, size):
                heard = heard + jnp.where(has(name, d), 1, 0)
        pl.semaphore_wait(sem, heard)

    def twin(dx):
        return lax.rem(ids["bx"], 2) == (1 - dx) // 2

    def cross(dx):
        return jnp.logical_and(has("bx", dx), jnp.logical_not(twin(dx)))

    def cross_both(dx, dy):
        return jnp.logical_and(cross(dx), has("by", dy))

    corners = [(dx, dy) for dx in (-1, 1) for dy in (-1, 1)]
    meet(barrier, ROUNDS[0])
    greeted = 0
    for dx, dy in corners:
        near_by = jnp.logical_and(has("bx", dx), has("by", dy))
        greeted = greeted + jnp.where(near_by, 1, 0)

        @pl.when(near_by)
        def _():
            pl.semaphore_signal(barrier, inc=1, device_id=at(dx, dy), device_id_type=MESH)
    load_e = pltpu.make_async_copy(est, e_buf.at[pl.ds(R, CX), pl.ds(R, CY)], load_sem.at[0])
    load_c = pltpu.make_async_copy(cov, c_buf, load_sem.at[1])
    load_t = pltpu.make_async_copy(taps, k_buf, load_sem.at[2])
    load_o = pltpu.make_async_copy(obs, o_buf, load_sem.at[3])
    for load in (load_e, load_c, load_t, load_o):
        load.start()

    def both(dx, dy):
        if dx and dy:
            return jnp.logical_and(has("bx", dx), has("by", dy))
        return has("bx", dx) if dx else has("by", dy)

    def remote(src, dst, send, recv, device):
        return pltpu.make_async_remote_copy(
            src_ref=src, dst_ref=dst, send_sem=send, recv_sem=recv,
            device_id=device, device_id_type=MESH,
        )

    own = pl.ds(R, CX)
    edge = {-1: pl.ds(0, R), 0: own, 1: pl.ds(EX - R, R)}
    inner = {-1: pl.ds(R, R), 0: own, 1: pl.ds(CX, R)}

    def counted(act):
        ends = [
            jnp.logical_and(has(name, -1), has(name, 1)) for name in ("bx", "by")
        ]
        for nx in (1, 2):
            for ny in (1, 2):
                hit = [e if n == 2 else jnp.logical_not(e) for e, n in zip(ends, (nx, ny))]

                @pl.when(jnp.logical_and(*hit))
                def _():
                    act(nx, ny)

    def planes_of(buf, rows):
        width = 32 if rows % 32 == 0 else 24
        return buf.at[pl.ds(0, rows // width), pl.ds(0, width)]

    def group(ref, send, recv):
        return remote(ref, ref, send, recv, at(0, 0, 1))

    def e_copy(dx, dy):
        return remote(
            e_buf.at[inner[dx], inner[dy]], e_buf.at[edge[-dx], edge[-dy]],
            e_send.at[0], e_recv.at[0 if dx else (3 - dy) // 2], at(dx, dy),
        )

    def e_pass(dx, dy):
        return remote(
            e_buf.at[inner[dx], edge[dy]], e_buf.at[edge[-dx], edge[dy]],
            e_send.at[0], e_recv.at[0], at(dx, 0),
        )

    def p_copy(dx, dy):
        return remote(
            p_buf.at[edge[dx], edge[dy]], rp_buf.at[edge[-dx], edge[-dy]],
            p_send.at[0], p_recv.at[0], at(dx, dy),
        )

    def p_pass(dx):
        return remote(p_buf.at[edge[dx]], tp_buf, p_send.at[0], p_recv.at[1], at(dx, 0))

    rows = {-1: pl.ds(R, R), 1: pl.ds(0, R)}
    to_rows = {-1: pl.ds(R, R), 1: pl.ds(0, R)}

    def face_copy(dz):
        return remote(
            zt_buf.at[:, rows[dz]], h_buf.at[pl.ds(1, 2), 1, to_rows[dz]],
            f_send.at[(1 + dz) // 2], f_recv.at[(1 - dz) // 2], at(0, 0, dz),
        )

    def share_copy(dz):
        return remote(
            share_buf.at[2], share_buf.at[(1 - dz) // 2],
            f_send.at[2 + (1 + dz) // 2], f_recv.at[2 + (1 - dz) // 2], at(0, 0, dz),
        )

    def h_copy(dx, dy):
        src = {-1: pl.ds(1, 1), 0: pl.ds(1, 2), 1: pl.ds(2, 1)}[dx]
        dst = {-1: pl.ds(3, 1), 0: pl.ds(1, 2), 1: pl.ds(0, 1)}[dx]
        return remote(
            h_buf.at[src, 1], h_buf.at[dst, 1 - dy],
            h_send.at[0], h_recv.at[1 if dx else 0], at(dx, dy),
        )

    def w_copy(dx, dy):
        return remote(
            w_buf.at[1, 1], w_buf.at[1 - dx, 1 - dy],
            w_send.at[0], w_recv.at[1 if dx else 0], at(dx, dy),
        )

    def z_copy(g, dz):
        views = pl.ds(G * g, G)
        bz, n = ids["bz"], sizes["bz"]
        place = 1 + (bz + 1) // n if dz > 0 else 2 * ((n - bz) // n)
        side = (dz + 1) // 2
        return remote(
            sb_buf.at[views, rows[dz]], hb_buf.at[views, pl.ds(pl.multiple_of(R * place, R), R)],
            zb_send.at[g, side], zb_recv.at[g, 1 - side], at(0, 0, dz),
        )

    part = functools.partial

    for d in (-1, 1):
        @pl.when(jnp.logical_not(has("by", d)))
        def _():
            e_buf[:, edge[d], :] = jnp.zeros((EX, R, CZ), F32)
            rp_buf[:, edge[d], :] = jnp.zeros((EX, R, CZ), F32)
            h_buf[:, 1 + d] = jnp.zeros((4, 3 * R, CZ), F32)
            w_buf[:, 1 + d] = jnp.zeros((3, V, CZ), F32)

        @pl.when(jnp.logical_not(has("bx", d)))
        def _():
            e_buf[edge[d]] = jnp.zeros((R, EY, CZ), F32)
            h_buf[3 * (1 + d) // 2] = jnp.zeros((3, 3 * R, CZ), F32)
            w_buf[1 + d] = jnp.zeros((3, V, CZ), F32)

        @pl.when(jnp.logical_not(cross(d)))
        def _():
            rp_buf[edge[d]] = jnp.zeros((R, EY, CZ), F32)

        @pl.when(jnp.logical_not(has("bz", d)))
        def _():
            hb_buf[:, rows[d], :] = jnp.zeros((V, R, CX * CY), F32)
            h_buf[1:3, 1, to_rows[-d], :] = jnp.zeros((2, R, CZ), F32)
            share_buf[(1 + d) // 2] = jnp.zeros((V, CZ), F32)

    row8 = lax.broadcasted_iota(jnp.int32, (V, CZ), 0)
    lane8 = lax.broadcasted_iota(jnp.int32, (V, CZ), 1)
    load_c.wait()
    flags = jnp.broadcast_to(c_buf[...].astype(F32), (V, V))
    picked = jnp.where(row8[:, :V] == lane8[:, :V], flags, 0.0)
    weight = jnp.broadcast_to(jnp.sum(picked, axis=1, keepdims=True), (V, CZ))
    w_buf[1, 1] = weight
    share_buf[2] = weight / jnp.sum(weight, axis=0, keepdims=True)
    load_e.wait()
    planes = e_buf[own, own].reshape(CX * CY, CZ)
    for h in range(2):
        flipped = planes[128 * h:128 * h + 128].T
        zt_buf[h, 0:R] = flipped[CZ - R:]
        zt_buf[h, R:2 * R] = flipped[:R]
    met(barrier, ROUNDS[0], greeted)
    meet(met_sem.at[0], ROUNDS[1])
    for d in (-1, 1):
        @pl.when(has("bz", d))
        def _():
            face_copy(d).start()
            share_copy(d).start()
    for dx, dy in SIDES:
        @pl.when(both(dx, dy))
        def _():
            w_copy(dx, dy).start()
    for d in (-1, 1):
        @pl.when(has("bx", d))
        def _():
            e_copy(d, 0).start()
    for d in (-1, 1):
        @pl.when(has("by", d))
        def _():
            e_copy(0, d).start()
    for dx, dy in corners:
        @pl.when(cross_both(dx, dy))
        def _():
            e_copy(dx, dy).start()

    load_t.wait()
    t_buf[...] = jnp.zeros_like(t_buf)
    for d in range(3):
        t_buf[d, 0:V, 0:T] = k_buf[d]
    taps_x, taps_y, taps_z = (
        t_buf[d, 0:V] / jnp.sum(t_buf[d, 0:V], axis=1, keepdims=True) for d in range(3)
    )
    for k, table in enumerate((taps_x, taps_y)):
        wide = jnp.concatenate(
            [jnp.broadcast_to(table[v:v + 1], (2 * R, CZ)) for v in range(V)], axis=0
        ).T
        l_buf[k] = wide[:4 * R]
    taps_y = taps_y + pltpu.roll(taps_y, 32, 1)
    taps_y = taps_y + pltpu.roll(taps_y, 64, 1)
    band = lax.broadcasted_iota(jnp.int32, (CY, 128), 1)
    bands = []
    for v in range(V):
        q = pltpu.roll(
            jnp.broadcast_to(taps_y[v:v + 1], (CY, 128)), 0, 1, stride=1, stride_axis=0
        )
        bands.append(q)
        q_hi, q_lo = split(q)
        zero = jnp.zeros_like(q_hi)
        for x in range(2):
            mine = (band // 32) % 2 == x
            yf_mat[v, x * CY:(x + 1) * CY, 0:128] = jnp.where(mine, q_hi, zero)
            yf_mat[v, x * CY:(x + 1) * CY, 128:256] = jnp.where(mine, q_lo, zero)
    for k in range(T):
        t_buf[3 + k, 0:V] = jnp.broadcast_to(taps_x[:, k:k + 1], (V, CZ))
        t_buf[3 + k, V:2 * V] = jnp.broadcast_to(l_buf[0, k:k + 1], (V, CZ))

    lane = lax.broadcasted_iota(jnp.int32, (128, 128), 1)
    row = lax.broadcasted_iota(jnp.int32, (128, 128), 0)
    near = jnp.abs(row - lane) <= R
    zf_mat[:, 128:256, :] = jnp.zeros((V, 128, 256), BF16)
    zh_mat[...] = jnp.zeros_like(zh_mat)
    for v in range(V):
        ring = pltpu.roll(
            jnp.broadcast_to(taps_z[v:v + 1], (128, 128)), 128 - R, 1, stride=1, stride_axis=0
        )
        ahead = ring.T
        m_hi, m_lo = split(jnp.where(near, ahead, 0.0))
        zf_mat[v, 0:128, 0:128] = m_hi
        zf_mat[v, 0:128, 128:256] = m_lo
        far = jnp.where(near, 0.0, ahead)
        f_hi, f_lo = split(jnp.concatenate([far[128 - R:128], far[0:R]], axis=0))
        top = 128 + 2 * R * v
        zf_mat[v, top:top + 2 * R, 0:128] = f_hi
        zf_mat[v, top:top + 2 * R, 128:256] = f_lo
        m_hi, m_lo = split(jnp.where(near, ring, 0.0))
        far = jnp.where(near, 0.0, ring)
        s_hi, s_lo = split(pltpu.roll(far, (2 * R * v + R) % 128, 1))
        for i in range(2):
            zm_mat[v, 128 * i:128 * i + 128, 0:128] = m_hi
            zm_mat[v, 128 * i:128 * i + 128, 128:256] = s_hi
        zm_mat[v, 256:384, 0:128] = m_lo
        zm_mat[v, 256:384, 128:256] = s_lo
        f_hi, f_lo = split(jnp.concatenate([far[0:R], far[128 - R:128]], axis=0))
        top = 2 * R * (v % G)
        zh_mat[v, top:top + 2 * R] = f_hi
        zh_mat[v, 64 + top:64 + top + 2 * R] = f_hi
        zh_mat[v, 128 + top:128 + top + 2 * R] = f_lo

    load_o.wait()
    seen = jnp.zeros((8, CZ), F32)
    for v in range(V):
        seen = seen + w_buf[1, 1, v:v + 1] * jnp.sum(o_buf[v].reshape(CX * CY // 8, 8, CZ), axis=0)
    count_own = jnp.sum(w_buf[1, 1], axis=0, keepdims=True)
    seen_buf[...] = seen / count_own

    for d in (-1, 1):
        @pl.when(has("bz", d))
        def _():
            face_copy(-d).wait_recv()
            share_copy(-d).wait_recv()
    for b in (1, 2):
        h_buf[b, 1, 2 * R:] = jnp.where(lane8 < CZ // 2, share_buf[0], share_buf[1])
    met(met_sem.at[0], ROUNDS[1])
    meet(met_sem.at[1], ROUNDS[2])
    for dx, dy in SIDES:
        @pl.when(both(dx, dy))
        def _():
            h_copy(dx, dy).start()
    sparse = jnp.zeros((V, CZ), F32)
    for k in range(T - 1):
        sparse = sparse + jnp.where(lane8 == 8 * k, t_buf[3 + k, 0:V], 0.0)
    for v in range(V):
        turned = pltpu.roll(jnp.broadcast_to(sparse[v:v + 1], (128, 128)), 0, 1, stride=1, stride_axis=0)
        last = jnp.broadcast_to(t_buf[2 + T, v:v + 1], (128, 128))
        low = jnp.where(lane >= row, turned, 0.0)
        high = jnp.where(lane < row, turned, jnp.where(lane == row, last, 0.0))
        for i, tile in enumerate((low, high)):
            k_hi, k_lo = split(tile.T)
            xb_mat[v, 128 * i:128 * i + 128, 0:128] = k_hi
            xb_mat[v, 128 * i:128 * i + 128, 128:256] = k_hi
            xb_mat[v, 128 * i:128 * i + 128, 256:384] = k_lo
        k_hi, k_lo = split(jnp.where(lane < 64, pltpu.roll(low, 64, 1), pltpu.roll(high, 64, 1)))
        xf_mat[0, v, :, 0:128] = k_hi
        xf_mat[0, v, :, 128:256] = k_hi
        xf_mat[0, v, :, 256:384] = k_lo
        k_hi, k_lo = split(jnp.where(lane < 64, low, high))
        xf_mat[1, v, :, 0:128] = k_hi
        xf_mat[1, v, :, 128:256] = k_hi
        xf_mat[1, v, :, 256:384] = k_lo

    for d in (-1, 1):
        @pl.when(has("by", d))
        def _():
            e_copy(0, -d).wait_recv()
            for dx in (-1, 1):
                @pl.when(twin(dx))
                def _():
                    e_pass(dx, d).start()

    def forward_y(x0, source=e_buf, mat=yf_mat, to=y_buf):
        data = jnp.concatenate(
            [stack4(source[pl.ds(x0 + 2 * h, 2)].reshape(2 * EY, CZ)) for h in range(2)], axis=1
        )
        full = dot(mat[...].reshape(V * 2 * CY, 256), data)
        for h in range(2):
            to[0:V, pl.ds(x0 + 2 * h, 2)] = full[:, h * CZ:(h + 1) * CZ].reshape(V, 2, CY, CZ)

    for x0 in range(R, R + CX, 4):
        forward_y(x0)

    def x_taps(v):
        return [jnp.broadcast_to(t_buf[3 + k, pl.ds(v, 1), :], (8, CZ)) for k in range(T)]

    def forward_x(inputs, first, y_buf, g_buf, v, carry):
        t = x_taps(v)
        for h in range(CY // 8):
            ys = pl.ds(8 * h, 8)
            acc = [None if first else g_buf[v, xo, ys, :] for xo in range(CX)]
            for xi in inputs:
                val = y_buf[v, xi, ys, :]
                for xo in range(max(0, xi - T + 1), min(CX, xi + 1)):
                    term = t[xi - xo] * val
                    acc[xo] = term if acc[xo] is None else acc[xo] + term
            for xo in range(CX):
                g_buf[v, xo, ys, :] = acc[xo]
        return carry

    y_spans = ((0, slice(R, CY), slice(0, R)), (1, slice(0, CY), slice(R, R + CY)),
               (2, slice(0, R), slice(R + CY, EY)))

    def halo_in(b):
        for yb, part_of, ys in y_spans:
            tile = jnp.concatenate([h_buf[b, yb, :2 * R]] * V, axis=0).T.reshape(R, CY, CZ)
            ht_buf[R * b:R * b + R, ys] = tile[:, part_of]

    def halo_share(b):
        for yb, _, ys in y_spans:
            tile = h_buf[b, yb, 2 * R:]
            before = jnp.broadcast_to(tile[:, 0:1], (V, CZ))
            after = jnp.broadcast_to(tile[:, CZ // 2:CZ // 2 + 1], (V, CZ))
            share = jnp.where(lane8 % (2 * R) < R, before, after)
            share = jnp.sum(jnp.where(lane8 // (2 * R) == row8, share, 0.0), axis=0, keepdims=True)
            at_x = slice(R * b, R * b + R)
            ht_buf[at_x, ys] = ht_buf[at_x, ys] * share

    def halo_y(b, to):
        t = [jnp.broadcast_to(l_buf[1, k:k + 1, :], (8, CZ)) for k in range(T)]
        for x in range(R * b, R * b + R):
            for h in range(2):
                acc = None
                for k in range(T):
                    term = t[k] * ht_buf[x, 8 * h + k:8 * h + k + 8, :]
                    acc = term if acc is None else acc + term
                to[V, x, 8 * h:8 * h + 8, :] = acc

    third = (band % 32)[:8]
    spans = ((0, R), (R, R + CX), (R + CX, EX))

    def mask(xb):
        xs = slice(*spans[xb])
        for yb in range(3):
            ys = slice(*spans[yb])
            count = jnp.maximum(jnp.sum(w_buf[xb, yb], axis=0, keepdims=True), 1.0)
            p_buf[xs, ys] = e_buf[xs, ys] * (1.0 / count)
        w = jnp.where(third < R, w_buf[xb, 0], jnp.where(third < R + CY, w_buf[xb, 1], w_buf[xb, 2]))
        for v in range(V):
            wide = jnp.broadcast_to(w[v:v + 1], (2 * CY, CZ)).astype(BF16)
            for i in range(2):
                cols = slice(128 * i, 128 * i + 128)
                yw_mat[xb, v, :, cols] = yf_mat[v, :, cols] * wide


    def planes_x(source, to, halo):
        for v in range(V):
            pairs = []
            for h in range(2):
                ys = slice(8 * h, 8 * h + 8)
                if halo:
                    f = jnp.concatenate([source[v, 0:R, ys], source[v, EX - R:EX, ys]], axis=0)
                else:
                    f = source[v, R:R + CX, ys]
                pairs.append(jnp.concatenate(split(f.reshape(128, CZ)), axis=0))
            data = jnp.concatenate(pairs, axis=1)
            mat = xf_mat.at[halo, v]
            full = dot(mat[:, 0:256], data) + dot(mat[:, 256:384], data[0:128])
            for h in range(2):
                ys = slice(8 * h, 8 * h + 8)
                f = full[:, h * CZ:(h + 1) * CZ].reshape(CX, 8, CZ)
                to[v, :, ys, :] = to[v, :, ys, :] + f if halo else f

    planes_x(y_buf, g_buf, 0)
    halo_planes = tuple(range(R)) + tuple(range(R + CX, EX))

    def masked_y(xb):
        mask(xb)
        for x0 in range(spans[xb][0], spans[xb][1], 4):
            forward_y(x0, p_buf, yw_mat.at[xb], m_buf)

    def w_arrivals(nx, ny):
        group(w_buf.at[0, pl.ds(0, ny)], w_send.at[0], w_recv.at[0]).wait_recv()

    counted(w_arrivals)
    masked_y(1)
    planes_x(m_buf, b_buf, 0)
    def x_arrivals(nx, ny):
        group(planes_of(e_buf, nx * (128 + 64 * ny)), e_send.at[0], e_recv.at[0]).wait_recv()
        tiles = w_buf.at[pl.ds(0, nx), pl.ds(0, 3)] if ny == 2 else w_buf.at[pl.ds(0, 2), pl.ds(0, nx)]
        group(tiles, w_send.at[0], w_recv.at[1]).wait_recv()

    counted(x_arrivals)
    for x0 in (0, 4, EX - 8, EX - 4):
        forward_y(x0)
    planes_x(y_buf, g_buf, 1)
    masked_y(0)
    masked_y(2)
    planes_x(m_buf, b_buf, 1)
    met(met_sem.at[1], ROUNDS[2])
    meet(met_sem.at[2], ROUNDS[3])

    def h_arrivals(nx, ny):
        group(h_buf.at[pl.ds(0, 2 * ny), 0], h_send.at[0], h_recv.at[0]).wait_recv()
        blocks = {2: pl.ds(0, nx), 1: pl.ds(0, 2 * nx)}[ny]
        cols = pl.ds(0, 3) if ny == 2 else 0
        group(h_buf.at[blocks, cols], h_send.at[0], h_recv.at[1]).wait_recv()

    counted(h_arrivals)
    for b in range(4):
        halo_in(b)
    for b in range(4):
        halo_y(b, y_buf)
    forward_x(range(EX), True, y_buf, g_buf, V, 0)

    def send_edges(fields, g):
        for v, f in zip(range(G * g, G * g + G), fields):
            for h in range(2):
                flipped = f[128 * h:128 * h + 128].T
                sb_buf[v, 0:R, 128 * h:128 * h + 128] = flipped[CZ - R:]
                sb_buf[v, R:2 * R, 128 * h:128 * h + 128] = flipped[:R]
        for d in (-1, 1):
            z_copy(g, d).start()

    def halo_rows(g):
        flat = hb_buf[G * g:G * g + G, 0:2 * R].reshape(G * 2 * R, CX * CY)
        hi = flat.astype(BF16).astype(F32)
        pair = jnp.concatenate([hi, flat - hi], axis=0)
        pair = jnp.concatenate([pair[:, :128].T, pair[:, 128:].T], axis=0).astype(BF16)
        return jnp.concatenate([pair, pair[:, :64]], axis=1)

    def z_apply(f, halo, mat, v):
        hi, lo = split(f)
        both = dot(jnp.concatenate([hi, halo[0]], axis=1), mat[v])
        rest = dot(jnp.concatenate([lo, halo[1]], axis=1), mat[v, :, 0:128])
        return both[:, :128] + both[:, 128:] + rest

    halo = split(g_buf[V].reshape(CX * CY, CZ))
    for g in range(V // G):
        ratios = []
        for v in range(G * g, G * g + G):
            blurred = z_apply(g_buf[v].reshape(CX * CY, CZ), halo, zf_mat, v)
            ratio = o_buf[v].reshape(CX * CY, CZ) / blurred
            r_buf[v] = ratio.reshape(CX, CY, CZ)
            ratios.append(ratio)
        send_edges(ratios, g)

    total = jnp.zeros((8, CZ), F32)
    outside = jnp.zeros((CX * CY, CZ), F32)
    for v in range(V):
        hi, lo = split(r_buf[v].reshape(CX * CY, CZ))
        f = dot(jnp.concatenate([hi, lo], axis=1), zm_mat[v, 0:256]) + dot(hi, zm_mat[v, 256:384])
        g_buf[v] = f[:, :128].reshape(CX, CY, CZ)
        outside = outside + f[:, 128:]
        weighed = f[:, :128] * b_buf[v].reshape(CX * CY, CZ)
        total = total + jnp.sum(weighed.reshape(CX * CY // 8, 8, CZ), axis=0)
    for b in range(4):
        halo_share(b)
    for b in range(4):
        halo_y(b, m_buf)
    forward_x(range(EX), True, m_buf, b_buf, V, 0)
    weighed = outside * b_buf[V].reshape(CX * CY, CZ)
    total = total + jnp.sum(weighed.reshape(CX * CY // 8, 8, CZ), axis=0)
    lane1 = lax.broadcasted_iota(jnp.int32, (1, CZ), 1)

    def summed(f):
        return jnp.sum(jnp.sum(f, axis=0, keepdims=True), axis=1, keepdims=True)

    red_own[0] = jnp.where(lane1 < CZ // 2, summed(seen_buf[...]), summed(total))

    by_hi, by_lo = lax.div(ids["by"], 4), lax.rem(ids["by"], 4)

    def red_peer(stage, d):
        if stage == 0:
            return {
                "bx": lax.rem(ids["bx"] + d % 4, 4),
                "by": lax.rem(by_hi + d // 4, 2) * 4 + by_lo,
            }
        return {
            "bz": lax.rem(ids["bz"] + d % 4, 4),
            "by": by_hi * 4 + lax.rem(by_lo + d // 4, 4),
        }

    def red_copy(stage, d):
        return pltpu.make_async_remote_copy(
            src_ref=red_own.at[stage], dst_ref=red_in.at[stage, d],
            send_sem=red_send.at[stage], recv_sem=red_recv.at[stage],
            device_id=red_peer(stage, d), device_id_type=MESH,
        )

    def red_start(stage):
        for d in range(1, STAGES[stage]):
            red_copy(stage, d).start()

    def red_all(stage):
        every = red_in.at[stage, pl.ds(1, STAGES[stage] - 1)]
        return pltpu.make_async_remote_copy(
            src_ref=every, dst_ref=every, send_sem=red_send.at[stage],
            recv_sem=red_recv.at[stage], device_id=red_peer(stage, 1), device_id_type=MESH,
        )

    def red_finish(stage):
        red_all(stage).wait_recv()
        total = red_own[stage]
        for d in range(1, STAGES[stage]):
            total = total + red_in[stage, d]
        return total

    met(met_sem.at[2], ROUNDS[3])
    red_start(0)
    for v in range(V):
        q4 = jnp.concatenate(
            [jnp.where(band // 32 == i // 2, bands[v], 0.0) for i in range(8)], axis=0
        ).T
        pair = split(q4)
        for xb in range(3):
            w = [jnp.broadcast_to(w_buf[xb, yb, v:v + 1], (8, CZ)) for yb in (0, 1, 1, 2)]
            w = jnp.concatenate(w * 4, axis=0).astype(BF16)
            for i in range(2):
                yb_mat[xb, v, :, 128 * i:128 * i + 128] = pair[i] * w

    def backward_x(v):
        pairs = [split(g_buf[v, :, 8 * h:8 * h + 8, :].reshape(128, CZ)) for h in range(2)]
        data = jnp.concatenate([jnp.concatenate(p, axis=0) for p in pairs], axis=1)
        full = dot(xb_mat[v, :, 0:256], data) + dot(xb_mat[v, :, 256:384], data[0:128])
        planes = jnp.concatenate(
            [full[:, h * CZ:(h + 1) * CZ].reshape(EX, 8, CZ) for h in range(2)], axis=1
        )
        hi, lo = split(planes)
        x_buf[v, :, 0:CY, :] = hi
        x_buf[v, :, CY:2 * CY, :] = lo

    for g in range(V // G):
        for d in (-1, 1):
            z_copy(g, d).wait_recv()
        halo = halo_rows(g)
        for v in range(G * g, G * g + G):
            g_buf[v] = g_buf[v] + dot(halo, zh_mat[v]).reshape(CX, CY, CZ)

    for v in range(V):
        backward_x(v)

    def backward_y(x0, xb):
        full = None
        for v in range(V):
            data = []
            for h in range(2):
                planes = x_buf[v, x0 + 4 * h:x0 + 4 * h + 4].reshape(128, CZ)
                data.append(jnp.concatenate([planes, planes], axis=0))
            term = dot(yb_mat[xb, v], jnp.concatenate(data, axis=1))
            full = term if full is None else full + term
        for h in range(2):
            p_buf[x0 + 4 * h:x0 + 4 * h + 4] = full[:, h * CZ:(h + 1) * CZ].reshape(4, EY, CZ)

    backward_y(0, 0)
    backward_y(EX - 8, 2)
    for dx in (-1, 1):
        @pl.when(twin(dx))
        def _():
            p_pass(dx).start()

        @pl.when(cross(dx))
        def _():
            p_copy(dx, 0).start()
        for dy in (-1, 1):
            @pl.when(cross_both(dx, dy))
            def _():
                p_copy(dx, dy).start()
    backward_y(R, 1)
    backward_y(2 * R, 1)
    red_own[1] = red_finish(0)
    red_start(1)
    for dx in (-1, 1):
        @pl.when(twin(dx))
        def _():
            p_pass(dx).wait_recv()
            p_buf[inner[dx]] = p_buf[inner[dx]] + tp_buf[...]
    for d in (-1, 1):
        @pl.when(has("by", d))
        def _():
            p_copy(0, d).start()
    def p_arrivals(nx, ny):
        rows = 128 * ny + (128 + 64 * ny) * (nx - 1)
        group(planes_of(rp_buf, rows), p_send.at[0], p_recv.at[0]).wait_recv()

    counted(p_arrivals)
    for s in range(2):
        xs, xe = slice(R + 8 * s, R + 8 * s + 8), edge[2 * s - 1]
        for h in range(2):
            ys, ye = slice(R + 8 * h, R + 8 * h + 8), edge[2 * h - 1]
            summed = p_buf[xs, ys] + rp_buf[xe, ys] + rp_buf[xs, ye] + rp_buf[xe, ye]
            out[8 * s:8 * s + 8, 8 * h:8 * h + 8, :] = e_buf[xs, ys, :] * summed
    def departures(nx, ny):
        group(planes_of(e_buf, 128 * (nx + ny) + 64 * nx * ny), e_send.at[0], e_recv.at[0]).wait_send()
        blocks = 2 * ny + nx * (1 + ny)
        group(e_buf.at[pl.ds(0, blocks), pl.ds(0, 24)], h_send.at[0], h_recv.at[0]).wait_send()
        tiles = e_buf.at[pl.ds(0, nx + ny + nx * ny), pl.ds(0, V)]
        group(tiles, w_send.at[0], w_recv.at[0]).wait_send()
        rows = 256 + 128 * ny + (128 + 64 * ny) * (nx - 1)
        group(planes_of(e_buf, rows), p_send.at[0], p_recv.at[0]).wait_send()

    counted(departures)
    for d in (-1, 1):
        @pl.when(has("bz", d))
        def _():
            face_copy(d).wait_send()
            share_copy(d).wait_send()
    for g in range(V // G):
        for d in (-1, 1):
            z_copy(g, d).wait_send()
    red_all(0).wait_send()
    red_all(1).wait_send()
    final = red_finish(1)
    scale = final[:, 0:1] / (final[:, CZ // 2:CZ // 2 + 1] * count_own[:, 0:1])
    out[...] = out[...] * scale.reshape(1, 1, 1)


def on_device(estimate, observed, coverage, psf_taps):
    dma = pltpu.SemaphoreType.DMA
    arrays = (estimate, observed, coverage.reshape(1, V), jnp.transpose(psf_taps, (1, 0, 2)))
    return pl.pallas_call(
        kernel,
        out_shape=jax.ShapeDtypeStruct((CX, CY, CZ), F32),
        in_specs=[pl.BlockSpec(memory_space=pltpu.HBM)] * 4,
        out_specs=pl.BlockSpec(memory_space=pltpu.VMEM),
        scratch_shapes=[
            pltpu.VMEM((EX, EY, CZ), F32),
            pltpu.VMEM((V, CX, CY, CZ), F32),
            pltpu.VMEM((V + 1, EX, CY, CZ), F32),
            pltpu.VMEM((V + 1, EX, CY, CZ), F32),
            pltpu.VMEM((V + 1, CX, CY, CZ), F32),
            pltpu.VMEM((V, CX, CY, CZ), F32),
            pltpu.VMEM((V, EX, 2 * CY, CZ), BF16),
            pltpu.VMEM((EX, EY, CZ), F32),
            pltpu.VMEM((EX, EY, CZ), F32),
            pltpu.VMEM((R, EY, CZ), F32),
            pltpu.VMEM((2, 2 * R, CZ), F32),
            pltpu.VMEM((3, V, CZ), F32),
            pltpu.VMEM((4, 3, 3 * R, CZ), F32),
            pltpu.VMEM((EX, EY, CZ), F32),
            pltpu.VMEM((V, 2 * R, CX * CY), F32),
            pltpu.VMEM((V, 3 * R, CX * CY), F32),
            pltpu.VMEM((3, 3, V, CZ), F32),
            pltpu.VMEM((1, V), jnp.int32),
            pltpu.VMEM((3, V, T), F32),
            pltpu.VMEM((3 + T, 2 * V, CZ), F32),
            pltpu.VMEM((2, 4 * R, CZ), F32),
            pltpu.VMEM((V, 256, 256), BF16),
            pltpu.VMEM((V, 384, 256), BF16),
            pltpu.VMEM((V, 192, 128), BF16),
            pltpu.VMEM((V, 256, 384), BF16),
            pltpu.VMEM((2, V, 128, 384), BF16),
            pltpu.VMEM((V, 2 * CY, 256), BF16),
            pltpu.VMEM((3, V, 2 * CY, 256), BF16),
            pltpu.VMEM((3, V, 128, 256), BF16),
            pltpu.VMEM((V + 1, CX, CY, CZ), F32),
            pltpu.VMEM((8, CZ), F32),
            pltpu.VMEM((2, 1, CZ), F32),
            pltpu.VMEM((2, 16, 1, CZ), F32),
            dma((4,)), dma((1,)), dma((3,)), dma((1,)), dma((2,)), dma((4,)), dma((4,)), dma((1,)), dma((2,)),
            dma((2, 2)), dma((2, 2)), dma((1,)), dma((2,)), dma((2,)), dma((2,)),
            pltpu.SemaphoreType.REGULAR((3,)),
        ],
        compiler_params=pltpu.CompilerParams(
            collective_id=0, has_side_effects=True, vmem_limit_bytes=48 * 1024 * 1024
        ),
    )(*[pltpu.with_memory_space_constraint(a, pltpu.HBM) for a in arrays])


def solution(mesh):
    block = P("bx", "by", "bz")
    views = P(None, "bx", "by", "bz")
    return jax.shard_map(
        on_device, mesh=mesh, in_specs=(block, views, views, P()), out_specs=block, check_vma=False
    )
```
